32 devices in a mesh: data: 32 (over z, y, x, core).
Axes of the slice: x: 2, y: 2, z: 4, core: 2. Of those that a mesh axis runs over, the one named last changes fastest.
Arguments:
- h_a: bfloat16 [16384, 512], P('data')
- h_b: bfloat16 [16384, 512], P('data')
- w_one: bfloat16 [512, 2048], replicated
- w_two: bfloat16 [2048, 2048], replicated
- w_three: bfloat16 [2048, 2048], replicated
- gain_one: float32 [2048], replicated
- bias_one: float32 [2048], replicated
- gain_two: float32 [2048], replicated
- bias_two: float32 [2048], replicated
Outputs:
- output 1: float32 [], replicated
- output 2: float32 [512, 2048], replicated
- output 3: float32 [2048, 2048], replicated
- output 4: float32 [2048, 2048], replicated
- output 5: float32 [2048], replicated
- output 6: float32 [2048], replicated
- output 7: float32 [2048], replicated
- output 8: float32 [2048], replicated
All inputs are finite; a program needn't handle non-finite values.
Results may differ from the reference program's by a relative error of at most 0.00114.
Values are sent between devices in bfloat16 or wider.
A program may use at most 1 GiB of HBM per device.

```python
import jax
import jax.numpy as jnp
from jax import lax

GROUP_DEVS = 32
ROWS_DEV = 512
FEAT_DIM = 512
PROJ_DIM = 2048

ALL_ROWS = GROUP_DEVS * ROWS_DEV
BN_EPS = 1e-5
STD_EPS = 1e-4
INV_WEIGHT = 2.0
VAR_WEIGHT = 1.0
COV_WEIGHT = 2.0


def setup_inputs(seed: int = 0) -> dict:
    key_list = jax.random.split(jax.random.key(seed), 11)
    shard_shape = (GROUP_DEVS, ROWS_DEV, FEAT_DIM)
    stat_shape = (GROUP_DEVS, 1, FEAT_DIM)
    base_a = jax.random.normal(key_list[0], shard_shape, jnp.float32)
    base_b = 0.8 * base_a + 0.6 * jax.random.normal(key_list[1], shard_shape, jnp.float32)
    shard_off = 0.6 * jax.random.normal(key_list[2], stat_shape, jnp.float32)
    shard_scale = jnp.exp(0.3 * jax.random.normal(key_list[3], stat_shape, jnp.float32))
    h_a = ((base_a + shard_off) * shard_scale).reshape(ALL_ROWS, FEAT_DIM).astype(jnp.bfloat16)
    h_b = ((base_b + shard_off) * shard_scale).reshape(ALL_ROWS, FEAT_DIM).astype(jnp.bfloat16)
    w_one = (jax.random.normal(key_list[4], (FEAT_DIM, PROJ_DIM), jnp.float32) * FEAT_DIM ** -0.5).astype(jnp.bfloat16)
    w_two = (jax.random.normal(key_list[5], (PROJ_DIM, PROJ_DIM), jnp.float32) * PROJ_DIM ** -0.5).astype(jnp.bfloat16)
    w_three = (jax.random.normal(key_list[6], (PROJ_DIM, PROJ_DIM), jnp.float32) * (0.7 * PROJ_DIM ** -0.5)).astype(jnp.bfloat16)
    gain_one = 1.0 + 0.3 * jax.random.normal(key_list[7], (PROJ_DIM,), jnp.float32)
    bias_one = 0.3 * jax.random.normal(key_list[8], (PROJ_DIM,), jnp.float32)
    gain_two = 1.0 + 0.3 * jax.random.normal(key_list[9], (PROJ_DIM,), jnp.float32)
    bias_two = 0.3 * jax.random.normal(key_list[10], (PROJ_DIM,), jnp.float32)
    return {'h_a': h_a, 'h_b': h_b, 'w_one': w_one, 'w_two': w_two, 'w_three': w_three,
            'gain_one': gain_one, 'bias_one': bias_one, 'gain_two': gain_two, 'bias_two': bias_two}


def layer_forward(x_in, weight, gain_vec, bias_vec):
    pre_act = jnp.dot(x_in, weight, preferred_element_type=jnp.float32)
    centered = pre_act - jnp.mean(pre_act, axis=0)
    inv_std = lax.rsqrt(jnp.mean(centered * centered, axis=0) + BN_EPS)
    normed = centered * inv_std
    act_val = gain_vec * normed + bias_vec
    return jnp.maximum(act_val, 0.0).astype(jnp.bfloat16), normed, act_val, inv_std


def layer_backward(d_out, normed, act_val, inv_std, gain_vec):
    d_act = jnp.where(act_val > 0.0, d_out, 0.0)
    sum_d = jnp.sum(d_act, axis=0)
    sum_dn = jnp.sum(d_act * normed, axis=0)
    d_pre = inv_std * gain_vec * (d_act - sum_d / ALL_ROWS - normed * (sum_dn / ALL_ROWS))
    return d_pre.astype(jnp.bfloat16), sum_dn, sum_d


def view_forward(view_feats, w_one, w_two, w_three, gain_one, bias_one, gain_two, bias_two):
    hidden_one, normed_one, act_one, inv_one = layer_forward(view_feats, w_one, gain_one, bias_one)
    hidden_two, normed_two, act_two, inv_two = layer_forward(hidden_one, w_two, gain_two, bias_two)
    z_view = jnp.dot(hidden_two, w_three, preferred_element_type=jnp.float32).astype(jnp.bfloat16)
    return z_view, (hidden_one, normed_one, act_one, inv_one, hidden_two, normed_two, act_two, inv_two)


def branch_terms(z_view):
    z_float = z_view.astype(jnp.float32)
    centered = z_float - jnp.mean(z_float, axis=0)
    cov_mat = jnp.dot(centered.T, centered) / (ALL_ROWS - 1)
    diag_var = jnp.diagonal(cov_mat)
    std_vec = jnp.sqrt(diag_var + STD_EPS)
    off_diag = cov_mat - jnp.diag(diag_var)
    hinge_on = (std_vec < 1.0).astype(jnp.float32)
    term_val = VAR_WEIGHT * jnp.sum(jnp.maximum(1.0 - std_vec, 0.0)) + COV_WEIGHT * jnp.sum(off_diag * off_diag)
    grad_cov = 2.0 * COV_WEIGHT * off_diag - jnp.diag(VAR_WEIGHT * hinge_on / (2.0 * std_vec))
    grad_hat = grad_cov.astype(jnp.bfloat16).astype(jnp.float32)
    grad_z = (2.0 / (ALL_ROWS - 1)) * jnp.dot(centered, grad_hat)
    return term_val, grad_z


def view_backward(view_feats, d_z, saved, w_two, w_three, gain_one, gain_two):
    hidden_one, normed_one, act_one, inv_one, hidden_two, normed_two, act_two, inv_two = saved
    grad_three = jnp.dot(hidden_two.T, d_z, preferred_element_type=jnp.float32)
    d_hidden_two = jnp.dot(d_z, w_three.T, preferred_element_type=jnp.float32)
    d_pre_two, gain_grad_two, bias_grad_two = layer_backward(d_hidden_two, normed_two, act_two, inv_two, gain_two)
    grad_two = jnp.dot(hidden_one.T, d_pre_two, preferred_element_type=jnp.float32)
    d_hidden_one = jnp.dot(d_pre_two, w_two.T, preferred_element_type=jnp.float32)
    d_pre_one, gain_grad_one, bias_grad_one = layer_backward(d_hidden_one, normed_one, act_one, inv_one, gain_one)
    grad_one = jnp.dot(view_feats.T, d_pre_one, preferred_element_type=jnp.float32)
    return grad_one, grad_two, grad_three, gain_grad_one, bias_grad_one, gain_grad_two, bias_grad_two


def reference(h_a, h_b, w_one, w_two, w_three, gain_one, bias_one, gain_two, bias_two):
    z_a, saved_a = view_forward(h_a, w_one, w_two, w_three, gain_one, bias_one, gain_two, bias_two)
    z_b, saved_b = view_forward(h_b, w_one, w_two, w_three, gain_one, bias_one, gain_two, bias_two)
    term_a, grad_za = branch_terms(z_a)
    term_b, grad_zb = branch_terms(z_b)
    z_diff = z_a.astype(jnp.float32) - z_b.astype(jnp.float32)
    loss_val = INV_WEIGHT * jnp.sum(z_diff * z_diff) / ALL_ROWS + term_a + term_b
    d_inv = (2.0 * INV_WEIGHT / ALL_ROWS) * z_diff
    d_za = (grad_za + d_inv).astype(jnp.bfloat16)
    d_zb = (grad_zb - d_inv).astype(jnp.bfloat16)
    back_a = view_backward(h_a, d_za, saved_a, w_two, w_three, gain_one, gain_two)
    back_b = view_backward(h_b, d_zb, saved_b, w_two, w_three, gain_one, gain_two)
    summed = [part_a + part_b for part_a, part_b in zip(back_a, back_b)]
    return (loss_val, summed[0], summed[1], summed[2], summed[3], summed[4], summed[5], summed[6])
```

```python
import functools

import jax
import jax.numpy as jnp
from jax import lax
from jax.experimental import pallas as pl
from jax.experimental.pallas import tpu as pltpu
from jax.sharding import PartitionSpec as P

BN_EPS = 1e-5
STD_EPS = 1e-4
INV_WEIGHT = 2.0
VAR_WEIGHT = 1.0
COV_WEIGHT = 2.0

F32 = jnp.float32
BF16 = jnp.bfloat16
MESH = pl.DeviceIdType.MESH
VMEM_LIMIT = 67043328

ROWS = 1024
HALF = 512
FEAT = 512
DIM = 2048
NB = 8
BLK = 256
LAG = 2
RING = 4
ALL_ROWS = 16384


def sds(shape, dtype):
    return jax.ShapeDtypeStruct(shape, dtype)


ANY = pl.BlockSpec(memory_space=pl.ANY)
INV = pl.BlockSpec(memory_space=pltpu.VMEM)


class Place:
    def __init__(self):
        i = lax.axis_index('data')
        self.c = lax.rem(i, 2)
        x = lax.rem(i // 2, 2)
        y = lax.rem(i // 4, 2)
        z = i // 8
        zl = lax.rem(z, 2)
        zh = z // 2
        self.pc = i + 1 - 2 * self.c
        px = i + 2 - 4 * x
        py = i + 4 - 8 * y
        p1 = i + 8 - 16 * zl
        p2 = i + 16 - 32 * zh
        self.ring = (px, py, p1, p2)
        self.bits = ((x, zl, y, zh), (y, zl, x, zh))
        self.peers = ((px, p1, py, p2), (py, p1, px, p2))
        self.keep = []
        self.send = []
        for k in range(2):
            keep = [0]
            send = [None]
            for s in range(1, 5):
                n = BLK >> s
                bit = self.bits[k][s - 1]
                send.append(keep[-1] + (1 - bit) * n)
                keep.append(keep[-1] + bit * n)
            self.keep.append(keep)
            self.send.append(send)

    def barrier(self):
        sem = pltpu.get_barrier_semaphore()
        for p in (self.pc,) + self.ring:
            pl.semaphore_signal(sem, inc=1, device_id=(p,), device_id_type=MESH)
        pl.semaphore_wait(sem, 5)


def rcopy(src, dst, ssem, rsem, dev):
    return pltpu.make_async_remote_copy(src_ref=src, dst_ref=dst, send_sem=ssem, recv_sem=rsem,
                                        device_id=(dev,), device_id_type=MESH)


def rows_at(off, n):
    return pl.ds(pl.multiple_of(off, n), n)


def nn(a, b):
    return jnp.dot(a, b, preferred_element_type=F32)


def nt(a, b):
    return lax.dot_general(a, b, (((1,), (1,)), ((), ())), preferred_element_type=F32)


def tn(a, b):
    return lax.dot_general(a, b, (((0,), (0,)), ((), ())), preferred_element_type=F32)


def cols(j):
    return pl.ds(pl.multiple_of(j * BLK, BLK), BLK)


class Scatter:
    def __init__(self, place, part, lands, ssem, rsem, n_units, slots):
        self.pl, self.part, self.lands = place, part, lands
        self.ssem, self.rsem, self.n, self.slots = ssem, rsem, n_units, slots

    def copy(self, u, s, k):
        n = BLK >> s
        r = lax.rem(u, RING)
        return rcopy(self.part.at[lax.rem(u, self.slots), k, rows_at(self.pl.send[k][s], n)],
                     self.lands[s - 1].at[r, k], self.ssem.at[s - 1, k, r], self.rsem.at[s - 1, k, r],
                     self.pl.peers[k][s - 1])

    def begin(self, u):
        for k in range(2):
            self.copy(u, 1, k).start()

    def advance(self, t, final):
        for s in (4, 3, 2, 1):
            u = t - LAG * s

            @pl.when((u >= 0) & (u < self.n))
            def _(s=s, u=u):
                n = BLK >> s
                p, r = lax.rem(u, self.slots), lax.rem(u, RING)
                for k in range(2):
                    cp = self.copy(u, s, k)
                    cp.wait_send()
                    cp.wait_recv()
                    rr = rows_at(self.pl.keep[k][s], n)
                    self.part[p, k, rr] = self.part[p, k, rr] + self.lands[s - 1][r, k]
                    if s < 4:
                        self.copy(u, s + 1, k).start()
                if s == 4:
                    final(u)


def scatter_scratch(slots):
    return [pltpu.VMEM((slots, 2, BLK, BLK), F32)] + \
        [pltpu.VMEM((RING, 2, BLK >> s, BLK), F32) for s in range(1, 5)] + \
        [pltpu.SemaphoreType.DMA((4, 2, RING)), pltpu.SemaphoreType.DMA((4, 2, RING))]


class SmallReduce:
    def __init__(self, place, val, land, ssem, rsem):
        self.pl, self.val, self.land, self.ssem, self.rsem = place, val, land, ssem, rsem

    def copy(self, k):
        return rcopy(self.val, self.land.at[k], self.ssem.at[k], self.rsem.at[k], self.pl.ring[k])

    def start(self, k):
        self.copy(k).start()

    def finish(self, k):
        self.copy(k).wait()
        self.val[...] = self.val[...] + self.land[k]

    def run(self):
        for k in range(4):
            self.start(k)
            self.finish(k)


def small_scratch(n):
    return [pltpu.VMEM((n, BLK), F32), pltpu.VMEM((4, n, BLK), F32),
            pltpu.SemaphoreType.DMA((4,)), pltpu.SemaphoreType.DMA((4,))]


def forward_kernel(ha, hb, w1, w2, w3, gb, n1_o, n2_o, x1_o, x2_o, z_o, r_o, h_o,
                   h, w1v, w2v, w3v, u1, u2, x1, x2, z, s1, l1, a1, b1, s2, l2, a2, b2, hsem, wsem, osem):
    me = Place()
    loads = [pltpu.make_async_copy(w1, w1v, wsem.at[0]), pltpu.make_async_copy(w2, w2v, wsem.at[1]),
             pltpu.make_async_copy(w3, w3v, wsem.at[2])]
    mine = pl.ds(pl.multiple_of(me.c * HALF, HALF), HALF)
    for c, own in ((0, ha), (1, hb)):
        @pl.when(me.c == c)
        def _(own=own):
            pltpu.make_async_copy(own, h.at[mine], hsem.at[0]).start()
    loads[0].start()
    me.barrier()

    def exchange(src):
        return rcopy(src, h.at[mine], hsem.at[1], hsem.at[2], me.pc)
    for c, other in ((0, hb), (1, ha)):
        @pl.when(me.c == c)
        def _(other=other):
            exchange(other).start()
    loads[1].start()
    loads[2].start()
    loads[0].wait()
    pltpu.make_async_copy(ha, h.at[mine], hsem.at[0]).wait()
    exchange(ha).wait()
    out = []

    def save(src, dst):
        cp = pltpu.make_async_copy(src, dst, osem.at[len(out)])
        cp.start()
        out.append(cp)

    save(h, h_o)

    def matmul(src, w, dst, st):
        def step(j, carry):
            res = nn(src[...], w[:, cols(j)])
            dst[:, cols(j)] = res
            st[pl.ds(j, 1)] = jnp.sum(res, axis=0, keepdims=True)
            st[pl.ds(NB + j, 1)] = jnp.sum(res * res, axis=0, keepdims=True)
            return carry
        lax.fori_loop(0, NB, step, 0)

    def norm(u, x, st, layer):
        mean = st[0:NB] * (1.0 / ALL_ROWS)
        var = st[NB:2 * NB] * (1.0 / ALL_ROWS) - mean * mean
        st[0:NB] = mean
        st[NB:2 * NB] = lax.rsqrt(var + BN_EPS)

        def step(j, carry):
            nrm = (u[:, cols(j)] - st[pl.ds(j, 1)]) * st[pl.ds(NB + j, 1)]
            act = gb[pl.ds(2 * NB * layer + j, 1)] * nrm + gb[pl.ds(2 * NB * layer + NB + j, 1)]
            u[:, cols(j)] = nrm
            x[:, cols(j)] = jnp.maximum(act, 0.0).astype(BF16)
            return carry
        lax.fori_loop(0, NB, step, 0)

    matmul(h, w1v, u1, s1)
    SmallReduce(me, s1, l1, a1, b1).run()
    norm(u1, x1, s1, 0)
    save(u1, n1_o)
    save(x1, x1_o)
    loads[1].wait()
    matmul(x1, w2v, u2, s2)
    SmallReduce(me, s2, l2, a2, b2).run()
    norm(u2, x2, s2, 1)
    save(u2, n2_o)
    save(x2, x2_o)
    r_o[0:NB] = s1[NB:2 * NB]
    r_o[NB:2 * NB] = s2[NB:2 * NB]
    loads[2].wait()

    def step(j, carry):
        z[:, cols(j)] = nn(x2[...], w3v[:, cols(j)]).astype(BF16)
        return carry
    lax.fori_loop(0, NB, step, 0)
    save(z, z_o)
    for cp in out:
        cp.wait()


def forward(ha, hb, w1, w2, w3, gb):
    return pl.pallas_call(
        forward_kernel,
        out_shape=(sds((ROWS, DIM), F32), sds((ROWS, DIM), F32), sds((ROWS, DIM), BF16), sds((ROWS, DIM), BF16),
                   sds((ROWS, DIM), BF16), sds((2 * NB, BLK), F32), sds((ROWS, FEAT), BF16)),
        in_specs=[ANY] * 5 + [INV],
        out_specs=(ANY,) * 5 + (INV, ANY),
        scratch_shapes=[pltpu.VMEM((ROWS, FEAT), BF16), pltpu.VMEM((FEAT, DIM), BF16), pltpu.VMEM((DIM, DIM), BF16),
                        pltpu.VMEM((DIM, DIM), BF16), pltpu.VMEM((ROWS, DIM), F32), pltpu.VMEM((ROWS, DIM), F32),
                        pltpu.VMEM((ROWS, DIM), BF16), pltpu.VMEM((ROWS, DIM), BF16), pltpu.VMEM((ROWS, DIM), BF16)]
        + small_scratch(2 * NB) + small_scratch(2 * NB)
        + [pltpu.SemaphoreType.DMA((3,)), pltpu.SemaphoreType.DMA((3,)), pltpu.SemaphoreType.DMA((6,))],
        compiler_params=pltpu.CompilerParams(collective_id=0, has_side_effects=True, vmem_limit_bytes=VMEM_LIMIT),
        name='forward',
    )(ha, hb, w1, w2, w3, gb)


GRAM_UNITS = 18
GRAM_SLOTS = 4 * LAG + 2


def block_of(q):
    p, r = q // 9, lax.rem(q, 9)
    first = r < NB - p
    return jnp.where(first, p, NB - 1 - p), jnp.where(first, p + r, r - 1)


def gram_kernel(z_i, dz_o, loss_o, z, zo, part, r1, r2, r3, r4, ssem, rsem, gh, gfull, mut, dz,
                sv, sl, sa, sb, asem, bsem, csem):
    me = Place()
    load = pltpu.make_async_copy(z_i, z.at[pl.ds(0, ROWS)], csem.at[0])
    load.start()
    me.barrier()
    swap = rcopy(z_i, zo, csem.at[1], csem.at[2], me.pc)
    swap.start()
    load.wait()
    loss_o[...] = jnp.zeros_like(loss_o)

    def col_sum(j, carry):
        sv[pl.ds(j, 1)] = jnp.sum(z[0:ROWS, cols(j)].astype(F32), axis=0, keepdims=True)
        return carry
    lax.fori_loop(0, NB, col_sum, 0)
    red = SmallReduce(me, sv, sl, sa, sb)
    sc = Scatter(me, part, (r1, r2, r3, r4), ssem, rsem, GRAM_UNITS, GRAM_SLOTS)

    def compute(u):
        for k in range(2):
            i, j = block_of(2 * u + k)
            part[lax.rem(u, GRAM_SLOTS), k] = tn(z[0:ROWS, cols(i)], z[0:ROWS, cols(j)])

    def spread(u, s, k):
        rr = rows_at(me.keep[k][s], BLK >> s)
        r = lax.rem(u, RING)
        buf = gh.at[2 * u + k, rr]
        return rcopy(buf, buf, asem.at[s - 1, k, r], bsem.at[s - 1, k, r], me.peers[k][s - 1])

    def final(u):
        for k in range(2):
            i, j = block_of(2 * u + k)
            rr = rows_at(me.keep[k][4], 16)
            gram = part[lax.rem(u, GRAM_SLOTS), k, rr]
            mu_r = mut[pl.ds(pl.multiple_of(i * BLK + me.keep[k][4], 16), 16)]
            mu_c = sv[pl.ds(j, 1)]
            cov = (gram - ALL_ROWS * jnp.concatenate([mu_r, mu_r], axis=1) * mu_c) * (1.0 / (ALL_ROWS - 1))
            row = lax.broadcasted_iota(jnp.int32, (16, BLK), 0) + (i * BLK + me.keep[k][4])
            col = lax.broadcasted_iota(jnp.int32, (16, BLK), 1) + j * BLK
            diag = row == col
            std = jnp.sqrt(jnp.where(diag, cov, 1.0) + STD_EPS)
            hinge = jnp.where(std < 1.0, VAR_WEIGHT / (2.0 * std), 0.0)
            weight = jnp.where(i == j, COV_WEIGHT, 2.0 * COV_WEIGHT)
            term = jnp.where(diag, VAR_WEIGHT * jnp.maximum(1.0 - std, 0.0), weight * cov * cov)
            loss_o[...] = loss_o[...] + term[0:8] + term[8:16]
            gh[2 * u + k, rr] = jnp.where(diag, -hinge, (2.0 * COV_WEIGHT) * cov).astype(BF16)
            spread(u, 4, k).start()

    compute(0)

    def slot(t, carry):
        for s in range(4):
            @pl.when(t == s + 1)
            def _(s=s):
                red.finish(s)

            @pl.when(t == s)
            def _(s=s):
                red.start(s)

        @pl.when(t == 5)
        def _():
            mean = sv[...] * (1.0 / ALL_ROWS)
            sv[...] = mean
            hi = mean.astype(BF16)
            mid = (mean - hi.astype(F32)).astype(BF16)
            low = (mean - hi.astype(F32) - mid.astype(F32)).astype(BF16)
            for j in range(NB):
                for h in range(2):
                    lanes = slice(128 * h, 128 * h + 128)
                    dst = slice(j * BLK + 128 * h, j * BLK + 128 * h + 128)
                    mut[dst] = jnp.broadcast_to(mean[j:j + 1, lanes], (128, 128)).T
                z[ROWS:ROWS + 16, j * BLK:(j + 1) * BLK] = jnp.concatenate(
                    [hi[j:j + 1], mid[j:j + 1], low[j:j + 1], jnp.zeros((13, BLK), BF16)], axis=0)

        for s in (1, 2, 3, 4):
            u = t - LAG * (9 - s)

            @pl.when((u >= 0) & (u < GRAM_UNITS))
            def _(s=s, u=u):
                for k in range(2):
                    cp = spread(u, s, k)
                    cp.wait_send()
                    cp.wait_recv()
                    if s > 1:
                        spread(u, s - 1, k).start()
                if s == 1:
                    for k in range(2):
                        i, j = block_of(2 * u + k)
                        blk = gh[2 * u + k]
                        gfull[rows_at(i * BLK, BLK), cols(j)] = blk

                        @pl.when(i != j)
                        def _():
                            gfull[rows_at(j * BLK, BLK), cols(i)] = blk.T

        sc.advance(t, final)

        @pl.when(t < GRAM_UNITS)
        def _():
            sc.begin(t)

        @pl.when(t + 1 < GRAM_UNITS)
        def _():
            compute(t + 1)
        return carry
    lax.fori_loop(0, GRAM_UNITS + 8 * LAG, slot, 0)
    swap.wait()
    pull = 2.0 * INV_WEIGHT / ALL_ROWS

    def dz_block(j, carry):
        acc = nn(z[...], gfull[:, cols(j)])
        mean = acc[ROWS:ROWS + 1] + acc[ROWS + 1:ROWS + 2] + acc[ROWS + 2:ROWS + 3]
        diff = z[0:ROWS, cols(j)].astype(F32) - zo[:, cols(j)].astype(F32)
        sq = jnp.sum((diff * diff).reshape(ROWS // 8, 8, BLK), axis=0)
        loss_o[...] = loss_o[...] + (0.5 * INV_WEIGHT / ALL_ROWS) * sq
        dz[:, cols(j)] = (pull * diff + (2.0 / (ALL_ROWS - 1)) * (acc[0:ROWS] - mean)).astype(BF16)
        return carry
    lax.fori_loop(0, NB, dz_block, 0)
    store = pltpu.make_async_copy(dz, dz_o, csem.at[0])
    store.start()
    store.wait()


def gram(z):
    return pl.pallas_call(
        gram_kernel,
        out_shape=(sds((ROWS, DIM), BF16), sds((8, BLK), F32)),
        in_specs=[ANY],
        out_specs=(ANY, INV),
        scratch_shapes=[pltpu.VMEM((ROWS + 16, DIM), BF16), pltpu.VMEM((ROWS, DIM), BF16)]
        + scatter_scratch(GRAM_SLOTS)
        + [pltpu.VMEM((2 * GRAM_UNITS, BLK, BLK), BF16), pltpu.VMEM((DIM, DIM), BF16), pltpu.VMEM((DIM, 128), F32),
           pltpu.VMEM((ROWS, DIM), BF16)]
        + small_scratch(NB)
        + [pltpu.SemaphoreType.DMA((4, 2, RING)), pltpu.SemaphoreType.DMA((4, 2, RING)), pltpu.SemaphoreType.DMA((3,))],
        compiler_params=pltpu.CompilerParams(collective_id=1, has_side_effects=True, vmem_limit_bytes=VMEM_LIMIT),
        name='gram',
    )(z)


GRAD_UNITS = 36
GRAD_SLOTS = 5 * LAG + 2


def grad_kernel(dz_i, x2_i, x1_i, h_i, n2_i, n1_i, w3, w2, gb, rs_i, loss_i, g_o, st2_o, st1_o,
                dz, dzo, du2, du2o, x2h, x2o, x1h, x1o, hh, ho, wv, nv, da,
                part, r1, r2, r3, r4, ssem, rsem, s2, l2, a2, b2, s1, l1, a1, b1, e2, e1,
                asem, bsem, lsem, csem, dsem, esem):
    me = Place()
    c = me.c
    half = pl.ds(pl.multiple_of(c * 1024, 1024), 1024)
    ohalf = pl.ds(pl.multiple_of((1 - c) * 1024, 1024), 1024)
    hhalf = pl.ds(pl.multiple_of(c * 256, 256), 256)
    hohalf = pl.ds(pl.multiple_of((1 - c) * 256, 256), 256)
    loads = [pltpu.make_async_copy(dz_i, dz, csem.at[0]), pltpu.make_async_copy(x2_i.at[:, half], x2h, csem.at[1]),
             pltpu.make_async_copy(w3, wv, csem.at[2]), pltpu.make_async_copy(n2_i, nv, csem.at[3]),
             pltpu.make_async_copy(x1_i.at[:, half], x1h, csem.at[4]),
             pltpu.make_async_copy(h_i.at[:, hhalf], hh, csem.at[5])]
    load_w2 = pltpu.make_async_copy(w2, wv, csem.at[6])
    load_n1 = pltpu.make_async_copy(n1_i, nv, csem.at[7])
    swaps = [rcopy(dz_i, dzo, dsem.at[0], esem.at[0], me.pc),
             rcopy(x2_i.at[:, ohalf], x2o, dsem.at[1], esem.at[1], me.pc),
             rcopy(x1_i.at[:, ohalf], x1o, dsem.at[2], esem.at[2], me.pc),
             rcopy(h_i.at[:, hohalf], ho, dsem.at[3], esem.at[3], me.pc)]
    swap_du2 = rcopy(du2, du2o, dsem.at[4], esem.at[4], me.pc)
    swap_du1 = rcopy(dz, dzo, dsem.at[5], esem.at[5], me.pc)
    swap_s2 = rcopy(s2, e2, dsem.at[6], esem.at[6], me.pc)
    swap_s1 = rcopy(s1, e1, dsem.at[7], esem.at[7], me.pc)
    for cp in loads[:2]:
        cp.start()
    me.barrier()
    for cp in swaps[:2]:
        cp.start()
    for cp in loads[2:]:
        cp.start()
    for cp in swaps[2:]:
        cp.start()
    for cp in loads:
        cp.wait()
    for cp in swaps:
        cp.wait()
    s2[2 * NB:3 * NB] = loss_i[...]
    red2 = SmallReduce(me, s2, l2, a2, b2)
    red1 = SmallReduce(me, s1, l1, a1, b1)
    sc = Scatter(me, part, (r1, r2, r3, r4), ssem, rsem, GRAD_UNITS, GRAD_SLOTS)

    def compute(u):
        p = lax.rem(u, GRAD_SLOTS)
        v = lax.rem(u, 16)
        rb, cb = cols(v // 4), pl.ds(pl.multiple_of(lax.rem(v, 4) * 512, 512), 512)
        for w, (la, lb, ra, rb_) in enumerate(((x2h, x2o, dz, dzo), (x1h, x1o, du2, du2o), (hh, ho, dz, dzo))):
            @pl.when(u // 16 == w)
            def _(w=w, la=la, lb=lb, ra=ra, rb_=rb_):
                lc = slice(None) if w == 2 else rb
                res = tn(la[:, lc], ra[:, cb]) + tn(lb[:, lc], rb_[:, cb])
                part[p, 0] = res[:, 0:BLK]
                part[p, 1] = res[:, BLK:2 * BLK]

    def base(u):
        w, v = u // 16, lax.rem(u, 16)
        own = jnp.where(w == 2, 256, 1024)
        return w * 2048 + c * own + (v // 4) * 256, lax.rem(v, 4) * 512

    def region(u, k, off, n):
        r0, c0 = base(u)
        return g_o.at[rows_at(r0 + off, n), pl.ds(pl.multiple_of(c0 + k * BLK, BLK), BLK)]

    def keep_copy(u, k):
        return pltpu.make_async_copy(part.at[lax.rem(u, GRAD_SLOTS), k, rows_at(me.keep[k][4], 16)],
                                     region(u, k, me.keep[k][4], 16), lsem.at[k, lax.rem(u, RING)])

    def spread(u, s, k):
        n = BLK >> s
        r = lax.rem(u, RING)
        dst = region(u, k, me.keep[k][s], n)
        src = part.at[lax.rem(u, GRAD_SLOTS), k, rows_at(me.keep[k][4], 16)] if s == 4 else dst
        return rcopy(src, dst, asem.at[s, k, r], bsem.at[s, k, r], me.peers[k][s - 1])

    def cross(u):
        r = lax.rem(u, RING)
        r0, c0 = base(u)
        reg = g_o.at[rows_at(r0, BLK), pl.ds(pl.multiple_of(c0, 512), 512)]
        return rcopy(reg, reg, asem.at[0, 0, r], bsem.at[0, 0, r], me.pc)

    def final(u):
        for k in range(2):
            spread(u, 4, k).start()
            keep_copy(u, k).start()

    def back_block(j, grad, st, layer):
        dx = nt(grad[...], wv[cols(j)])
        nrm = nv[:, cols(j)]
        act = gb[pl.ds(2 * NB * layer + j, 1)] * nrm + gb[pl.ds(2 * NB * layer + NB + j, 1)]
        d_act = jnp.where(act > 0.0, dx, 0.0)
        da[:, cols(j)] = d_act
        st[pl.ds(j, 1)] = jnp.sum(d_act, axis=0, keepdims=True)
        st[pl.ds(NB + j, 1)] = jnp.sum(d_act * nrm, axis=0, keepdims=True)

    def back_pre(dst, st, layer):
        def step(j, carry):
            scale = gb[pl.ds(2 * NB * layer + j, 1)] * rs_i[pl.ds(NB * layer + j, 1)]
            m0 = st[pl.ds(j, 1)] * (1.0 / ALL_ROWS)
            m1 = st[pl.ds(NB + j, 1)] * (1.0 / ALL_ROWS)
            dst[:, cols(j)] = (scale * (da[:, cols(j)] - m0 - nv[:, cols(j)] * m1)).astype(BF16)
            return carry
        lax.fori_loop(0, NB, step, 0)

    compute(0)

    def slot(t, carry):
        u = t - LAG * 9

        @pl.when((u >= 0) & (u < GRAD_UNITS))
        def _(u=u):
            cross(u).wait()

        for s in (1, 2, 3, 4):
            u = t - LAG * (9 - s)

            @pl.when((u >= 0) & (u < GRAD_UNITS))
            def _(s=s, u=u):
                for k in range(2):
                    cp = spread(u, s, k)
                    cp.wait_send()
                    cp.wait_recv()
                    if s == 4:
                        keep_copy(u, k).wait()
                    if s > 1:
                        spread(u, s - 1, k).start()
                if s == 1:
                    cross(u).start()

        sc.advance(t, final)

        @pl.when(t < GRAD_UNITS)
        def _():
            sc.begin(t)

        for first, grad, st, layer, red, dst, swap_d, swap_s, nxt in (
                (0, dz, s2, 1, red2, du2, swap_du2, swap_s2, load_n1),
                (13, du2, s1, 0, red1, dz, swap_du1, swap_s1, None)):
            @pl.when((t >= first) & (t < first + NB))
            def _(first=first, grad=grad, st=st, layer=layer):
                back_block(t - first, grad, st, layer)

            if nxt is not None:
                @pl.when(t == first + NB - 1)
                def _():
                    load_w2.start()
            for k in range(4):
                @pl.when(t == first + NB + k + 1)
                def _(red=red, k=k):
                    red.finish(k)

                @pl.when(t == first + NB + k)
                def _(red=red, k=k):
                    red.start(k)

            @pl.when(t == first + NB + 4)
            def _(st=st, layer=layer, dst=dst, swap_d=swap_d, swap_s=swap_s, nxt=nxt):
                back_pre(dst, st, layer)
                swap_d.start()
                swap_s.start()
                if nxt is not None:
                    nxt.start()
                    load_w2.wait()
                    nxt.wait()

        @pl.when(t == 15)
        def _():
            swap_du2.wait()

        @pl.when(t == 31)
        def _():
            swap_du1.wait()

        @pl.when(t + 1 < GRAD_UNITS)
        def _():
            compute(t + 1)
        return carry
    lax.fori_loop(0, GRAD_UNITS + 9 * LAG, slot, 0)
    swap_s2.wait()
    swap_s1.wait()
    st2_o[...] = s2[...] + e2[...]
    st1_o[...] = s1[...] + e1[...]


def gradients(dz, x2, x1, h, n2, n1, w3, w2, gb, rs, loss):
    act = pltpu.VMEM((ROWS, DIM), BF16)
    part = pltpu.VMEM((ROWS, 1024), BF16)
    dma = pltpu.SemaphoreType.DMA
    return pl.pallas_call(
        grad_kernel,
        out_shape=(sds((2 * DIM + FEAT, DIM), F32), sds((3 * NB, BLK), F32), sds((2 * NB, BLK), F32)),
        in_specs=[ANY] * 8 + [INV] * 3,
        out_specs=(ANY, INV, INV),
        scratch_shapes=[act, act, act, act, part, part, part, part, pltpu.VMEM((ROWS, 256), BF16),
                        pltpu.VMEM((ROWS, 256), BF16), pltpu.VMEM((DIM, DIM), BF16), pltpu.VMEM((ROWS, DIM), F32),
                        pltpu.VMEM((ROWS, DIM), F32)]
        + scatter_scratch(GRAD_SLOTS) + small_scratch(3 * NB) + small_scratch(2 * NB)
        + [pltpu.VMEM((3 * NB, BLK), F32), pltpu.VMEM((2 * NB, BLK), F32),
           dma((5, 2, RING)), dma((5, 2, RING)), dma((2, RING)), dma((8,)), dma((8,)), dma((8,))],
        compiler_params=pltpu.CompilerParams(collective_id=2, has_side_effects=True, vmem_limit_bytes=VMEM_LIMIT),
        name='gradients',
    )(dz, x2, x1, h, n2, n1, w3, w2, gb, rs, loss)


def solution(mesh):
    def local_step(h_a, h_b, w_one, w_two, w_three, gain_one, bias_one, gain_two, bias_two):
        gb = jnp.stack([gain_one, bias_one, gain_two, bias_two]).reshape(4 * NB, BLK)
        n1, n2, x1, x2, z, rs, h = forward(h_a, h_b, w_one, w_two, w_three, gb)
        dz, loss_part = gram(z)
        grads, st2, st1 = gradients(dz, x2, x1, h, n2, n1, w_three, w_two, gb, rs, loss_part)
        loss = jnp.sum(st2[2 * NB:])
        return (loss, grads[2 * DIM:], grads[DIM:2 * DIM], grads[:DIM],
                st1[NB:2 * NB].reshape(DIM), st1[:NB].reshape(DIM),
                st2[NB:2 * NB].reshape(DIM), st2[:NB].reshape(DIM))

    row_spec = P('data', None)
    return jax.shard_map(local_step, mesh=mesh,
                         in_specs=(row_spec, row_spec, P(), P(), P(), P(), P(), P(), P()),
                         out_specs=(P(), P(), P(), P(), P(), P(), P(), P()),
                         check_vma=False)
```

```python
import functools

import jax
import jax.numpy as jnp
from jax import lax
from jax.experimental import pallas as pl
from jax.experimental.pallas import tpu as pltpu
from jax.sharding import PartitionSpec as P

BN_EPS = 1e-5
STD_EPS = 1e-4
INV_WEIGHT = 2.0
VAR_WEIGHT = 1.0
COV_WEIGHT = 2.0

F32 = jnp.float32
BF16 = jnp.bfloat16
MESH = pl.DeviceIdType.MESH
VMEM_LIMIT = 67043328

ROWS = 1024
HALF = 512
FEAT = 512
DIM = 2048
NB = 8
BLK = 256
LAG = 2
RING = 4
ALL_ROWS = 16384


def sds(shape, dtype):
    return jax.ShapeDtypeStruct(shape, dtype)


ANY = pl.BlockSpec(memory_space=pl.ANY)
INV = pl.BlockSpec(memory_space=pltpu.VMEM)


class Place:
    def __init__(self):
        i = lax.axis_index('data')
        self.c = lax.rem(i, 2)
        x = lax.rem(i // 2, 2)
        y = lax.rem(i // 4, 2)
        z = i // 8
        zl = lax.rem(z, 2)
        zh = z // 2
        self.pc = i + 1 - 2 * self.c
        px = i + 2 - 4 * x
        py = i + 4 - 8 * y
        p1 = i + 8 - 16 * zl
        p2 = i + 16 - 32 * zh
        self.ring = (px, py, p1, p2)
        self.bits = ((x, zl, y, zh), (y, zl, x, zh))
        self.peers = ((px, p1, py, p2), (py, p1, px, p2))
        self.keep = []
        self.send = []
        for k in range(2):
            keep = [0]
            send = [None]
            for s in range(1, 5):
                n = BLK >> s
                bit = self.bits[k][s - 1]
                send.append(keep[-1] + (1 - bit) * n)
                keep.append(keep[-1] + bit * n)
            self.keep.append(keep)
            self.send.append(send)

    def barrier(self):
        sem = pltpu.get_barrier_semaphore()
        for p in (self.pc,) + self.ring:
            pl.semaphore_signal(sem, inc=1, device_id=(p,), device_id_type=MESH)
        pl.semaphore_wait(sem, 5)


def rcopy(src, dst, ssem, rsem, dev):
    return pltpu.make_async_remote_copy(src_ref=src, dst_ref=dst, send_sem=ssem, recv_sem=rsem,
                                        device_id=(dev,), device_id_type=MESH)


def rows_at(off, n):
    return pl.ds(pl.multiple_of(off, n), n)


def nn(a, b):
    return jnp.dot(a, b, preferred_element_type=F32)


def nt(a, b):
    return lax.dot_general(a, b, (((1,), (1,)), ((), ())), preferred_element_type=F32)


def tn(a, b):
    return lax.dot_general(a, b, (((0,), (0,)), ((), ())), preferred_element_type=F32)


def cols(j):
    return pl.ds(pl.multiple_of(j * BLK, BLK), BLK)


class Scatter:
    def __init__(self, place, part, lands, ssem, rsem):
        self.pl, self.part, self.lands, self.ssem, self.rsem = place, part, lands, ssem, rsem

    def copy(self, u, s, k):
        n = BLK >> s
        r = lax.rem(u, RING)
        return rcopy(self.part.at[lax.rem(u, SLOTS), k, rows_at(self.pl.send[k][s], n)],
                     self.lands[s - 1].at[r, k], self.ssem.at[s - 1, k, r], self.rsem.at[s - 1, k, r],
                     self.pl.peers[k][s - 1])

    def begin(self, u):
        for k in range(2):
            self.copy(u, 1, k).start()

    def advance(self, t, final):
        for s in (4, 3, 2, 1):
            u, ok = unit_at(t - LAG * s)

            @pl.when(ok)
            def _(s=s, u=u):
                n = BLK >> s
                p, r = lax.rem(u, SLOTS), lax.rem(u, RING)
                for k in range(2):
                    cp = self.copy(u, s, k)
                    cp.wait_send()
                    cp.wait_recv()
                    rr = rows_at(self.pl.keep[k][s], n)
                    self.part[p, k, rr] = self.part[p, k, rr] + self.lands[s - 1][r, k]
                    if s < 4:
                        self.copy(u, s + 1, k).start()
                if s == 4:
                    final(u)


def scatter_scratch(slots):
    return [pltpu.VMEM((slots, 2, BLK, BLK), F32)] + \
        [pltpu.VMEM((RING, 2, BLK >> s, BLK), F32) for s in range(1, 5)] + \
        [pltpu.SemaphoreType.DMA((4, 2, RING)), pltpu.SemaphoreType.DMA((4, 2, RING))]


class SmallReduce:
    def __init__(self, place, val, land, ssem, rsem):
        self.pl, self.val, self.land, self.ssem, self.rsem = place, val, land, ssem, rsem

    def copy(self, k):
        return rcopy(self.val, self.land.at[k], self.ssem.at[k], self.rsem.at[k], self.pl.ring[k])

    def start(self, k):
        self.copy(k).start()

    def finish(self, k):
        self.copy(k).wait()
        self.val[...] = self.val[...] + self.land[k]

    def run(self):
        for k in range(4):
            self.start(k)
            self.finish(k)


def small_scratch(n):
    return [pltpu.VMEM((n, BLK), F32), pltpu.VMEM((4, n, BLK), F32),
            pltpu.SemaphoreType.DMA((4,)), pltpu.SemaphoreType.DMA((4,))]


def forward_kernel(ha, hb, w1, w2, w3, gb, n1_o, n2_o, x1_o, x2_o, z_o, r_o, h_o,
                   h, w1v, w2v, w3v, u1, u2, x1, x2, z, s1, l1, a1, b1, s2, l2, a2, b2, hsem, wsem, osem):
    me = Place()
    loads = [pltpu.make_async_copy(w1, w1v, wsem.at[0]), pltpu.make_async_copy(w2, w2v, wsem.at[1]),
             pltpu.make_async_copy(w3, w3v, wsem.at[2])]
    mine = pl.ds(pl.multiple_of(me.c * HALF, HALF), HALF)
    for c, own in ((0, ha), (1, hb)):
        @pl.when(me.c == c)
        def _(own=own):
            pltpu.make_async_copy(own, h.at[mine], hsem.at[0]).start()
    loads[0].start()
    me.barrier()

    def exchange(src):
        return rcopy(src, h.at[mine], hsem.at[1], hsem.at[2], me.pc)
    for c, other in ((0, hb), (1, ha)):
        @pl.when(me.c == c)
        def _(other=other):
            exchange(other).start()
    loads[1].start()
    loads[2].start()
    loads[0].wait()
    pltpu.make_async_copy(ha, h.at[mine], hsem.at[0]).wait()
    exchange(ha).wait()
    out = []

    def save(src, dst):
        cp = pltpu.make_async_copy(src, dst, osem.at[len(out)])
        cp.start()
        out.append(cp)

    save(h, h_o)

    def matmul(src, w, dst, st):
        def step(j, carry):
            res = nn(src[...], w[:, cols(j)])
            dst[:, cols(j)] = res
            st[pl.ds(j, 1)] = jnp.sum(res, axis=0, keepdims=True)
            st[pl.ds(NB + j, 1)] = jnp.sum(res * res, axis=0, keepdims=True)
            return carry
        lax.fori_loop(0, NB, step, 0)

    def norm(u, x, st, layer):
        mean = st[0:NB] * (1.0 / ALL_ROWS)
        var = st[NB:2 * NB] * (1.0 / ALL_ROWS) - mean * mean
        st[0:NB] = mean
        st[NB:2 * NB] = lax.rsqrt(var + BN_EPS)

        def step(j, carry):
            nrm = (u[:, cols(j)] - st[pl.ds(j, 1)]) * st[pl.ds(NB + j, 1)]
            act = gb[pl.ds(2 * NB * layer + j, 1)] * nrm + gb[pl.ds(2 * NB * layer + NB + j, 1)]
            u[:, cols(j)] = nrm
            x[:, cols(j)] = jnp.maximum(act, 0.0).astype(BF16)
            return carry
        lax.fori_loop(0, NB, step, 0)

    matmul(h, w1v, u1, s1)
    SmallReduce(me, s1, l1, a1, b1).run()
    norm(u1, x1, s1, 0)
    save(u1, n1_o)
    save(x1, x1_o)
    loads[1].wait()
    matmul(x1, w2v, u2, s2)
    SmallReduce(me, s2, l2, a2, b2).run()
    norm(u2, x2, s2, 1)
    save(u2, n2_o)
    save(x2, x2_o)
    r_o[0:NB] = s1[NB:2 * NB]
    r_o[NB:2 * NB] = s2[NB:2 * NB]
    loads[2].wait()

    def step(j, carry):
        z[:, cols(j)] = nn(x2[...], w3v[:, cols(j)]).astype(BF16)
        return carry
    lax.fori_loop(0, NB, step, 0)
    save(z, z_o)
    for cp in out:
        cp.wait()


def forward(ha, hb, w1, w2, w3, gb):
    return pl.pallas_call(
        forward_kernel,
        out_shape=(sds((ROWS, DIM), F32), sds((ROWS, DIM), F32), sds((ROWS, DIM), BF16), sds((ROWS, DIM), BF16),
                   sds((ROWS, DIM), BF16), sds((2 * NB, BLK), F32), sds((ROWS, FEAT), BF16)),
        in_specs=[ANY] * 5 + [INV],
        out_specs=(ANY,) * 5 + (INV, ANY),
        scratch_shapes=[pltpu.VMEM((ROWS, FEAT), BF16), pltpu.VMEM((FEAT, DIM), BF16), pltpu.VMEM((DIM, DIM), BF16),
                        pltpu.VMEM((DIM, DIM), BF16), pltpu.VMEM((ROWS, DIM), F32), pltpu.VMEM((ROWS, DIM), F32),
                        pltpu.VMEM((ROWS, DIM), BF16), pltpu.VMEM((ROWS, DIM), BF16), pltpu.VMEM((ROWS, DIM), BF16)]
        + small_scratch(2 * NB) + small_scratch(2 * NB)
        + [pltpu.SemaphoreType.DMA((3,)), pltpu.SemaphoreType.DMA((3,)), pltpu.SemaphoreType.DMA((6,))],
        compiler_params=pltpu.CompilerParams(collective_id=0, has_side_effects=True, vmem_limit_bytes=VMEM_LIMIT),
        name='forward',
    )(ha, hb, w1, w2, w3, gb)


GRAM_UNITS = 18
UNITS = 54
SLOTS = 5 * LAG + 2
START_3 = 26
START_2 = 46
END = START_2 + 20 + 9 * LAG
DZ_SLOTS = (23, 28, 32, 34)
PASS_2 = 35
PASS_1 = 45


def block_of(q):
    i = jnp.int32(0)
    for first in (8, 15, 21, 26, 30, 33, 35):
        i = i + jnp.where(q >= first, 1, 0)
    return i, i + q - (17 * i - i * i) // 2


def unit_at(t):
    u = jnp.where(t < START_3, t, jnp.where(t < START_2, t - (START_3 - 18), t - (START_2 - 34)))
    ok = ((t >= 0) & (t < 18)) | ((t >= START_3) & (t < START_3 + 16)) | ((t >= START_2) & (t < START_2 + 20))
    return jnp.where(ok, u, 0), ok


def back_kernel(z_i, x2_i, x1_i, h_i, n2_i, n1_i, w3, w2, gb, rs_i, g_o, st2_o, st1_o,
                zd, zod, dz, dzo, gw, x2h, x2o, x1h, x1o, hh, ho, nv, da, mut, lacc,
                part, r1, r2, r3, r4, ssem, rsem, sv, sl, sa, sb, s2, l2, a2, b2, s1, l1, a1, b1, e2, e1,
                gasem, gbsem, asem, bsem, lsem, csem, dsem, esem):
    me = Place()
    c = me.c
    half = pl.ds(pl.multiple_of(c * 1024, 1024), 1024)
    ohalf = pl.ds(pl.multiple_of((1 - c) * 1024, 1024), 1024)
    hhalf = pl.ds(pl.multiple_of(c * 256, 256), 256)
    hohalf = pl.ds(pl.multiple_of((1 - c) * 256, 256), 256)
    body = pl.ds(0, ROWS)
    load_z = pltpu.make_async_copy(z_i, zd.at[body], csem.at[0])
    loads = [pltpu.make_async_copy(x2_i.at[:, half], x2h, csem.at[1]),
             pltpu.make_async_copy(n2_i, nv, csem.at[2]),
             pltpu.make_async_copy(x1_i.at[:, half], x1h, csem.at[3]),
             pltpu.make_async_copy(h_i.at[:, hhalf], hh, csem.at[4])]
    load_w3 = pltpu.make_async_copy(w3, gw, csem.at[5])
    load_w2 = pltpu.make_async_copy(w2, gw, csem.at[6])
    load_n1 = pltpu.make_async_copy(n1_i, nv, csem.at[7])
    swap_z = rcopy(z_i, zod, dsem.at[0], esem.at[0], me.pc)
    swaps = [rcopy(x2_i.at[:, ohalf], x2o, dsem.at[1], esem.at[1], me.pc),
             rcopy(x1_i.at[:, ohalf], x1o, dsem.at[2], esem.at[2], me.pc),
             rcopy(h_i.at[:, hohalf], ho, dsem.at[3], esem.at[3], me.pc)]
    swap_du2 = rcopy(zd.at[body], zod, dsem.at[4], esem.at[4], me.pc)
    swap_du1 = rcopy(dz, dzo, dsem.at[5], esem.at[5], me.pc)
    swap_s2 = rcopy(s2, e2, dsem.at[6], esem.at[6], me.pc)
    swap_s1 = rcopy(s1, e1, dsem.at[7], esem.at[7], me.pc)

    def swap_dz(p):
        part_cols = pl.ds(512 * p, 512)
        return rcopy(dz.at[:, part_cols], dzo.at[:, part_cols], dsem.at[8 + p], esem.at[8 + p], me.pc)

    load_z.start()
    me.barrier()
    swap_z.start()
    load_z.wait()
    for cp in swaps + loads:
        cp.start()
    lacc[...] = jnp.zeros_like(lacc)

    def col_sum(j, carry):
        sv[pl.ds(j, 1)] = jnp.sum(zd[0:ROWS, cols(j)].astype(F32), axis=0, keepdims=True)
        return carry
    lax.fori_loop(0, NB, col_sum, 0)
    red0 = SmallReduce(me, sv, sl, sa, sb)
    red2 = SmallReduce(me, s2, l2, a2, b2)
    red1 = SmallReduce(me, s1, l1, a1, b1)
    sc = Scatter(me, part, (r1, r2, r3, r4), ssem, rsem)

    def compute(u):
        p = lax.rem(u, SLOTS)

        @pl.when(u < GRAM_UNITS)
        def _():
            for k in range(2):
                i, j = block_of(2 * u + k)
                part[p, k] = tn(zd[0:ROWS, cols(i)], zd[0:ROWS, cols(j)])

        w, rb, cb = grad_unit(u)
        for w_, la, lb, ra, rb_ in ((0, x2h, x2o, dz, dzo), (1, x1h, x1o, zd, zod), (2, hh, ho, dz, dzo)):
            @pl.when((u >= GRAM_UNITS) & (w == w_))
            def _(w_=w_, la=la, lb=lb, ra=ra, rb_=rb_):
                lc = slice(None) if w_ == 2 else cols(rb)
                rc = pl.ds(pl.multiple_of(cb * 512, 512), 512)
                res = tn(la[:, lc], ra[0:ROWS, rc]) + tn(lb[:, lc], rb_[:, rc])
                part[p, 0] = res[:, 0:BLK]
                part[p, 1] = res[:, BLK:2 * BLK]

    def grad_unit(u):
        v = u - GRAM_UNITS
        w = v // 16
        q = lax.rem(v, 16)
        return w, jnp.where(w == 2, 0, lax.rem(q, 4)), jnp.where(w == 2, q, q // 4)

    def base(u):
        w, rb, cb = grad_unit(u)
        return w * 2048 + c * jnp.where(w == 2, 256, 1024) + rb * 256, cb * 512

    def region(u, k, off, n):
        r0, c0 = base(u)
        return g_o.at[rows_at(r0 + off, n), pl.ds(pl.multiple_of(c0 + k * BLK, BLK), BLK)]

    def keep_copy(u, k):
        return pltpu.make_async_copy(part.at[lax.rem(u, SLOTS), k, rows_at(me.keep[k][4], 16)],
                                     region(u, k, me.keep[k][4], 16), lsem.at[k, lax.rem(u, RING)])

    def spread(u, s, k):
        r = lax.rem(u, RING)
        dst = region(u, k, me.keep[k][s], BLK >> s)
        src = part.at[lax.rem(u, SLOTS), k, rows_at(me.keep[k][4], 16)] if s == 4 else dst
        return rcopy(src, dst, asem.at[s, k, r], bsem.at[s, k, r], me.peers[k][s - 1])

    def cross(u):
        r = lax.rem(u, RING)
        r0, c0 = base(u)
        reg = g_o.at[rows_at(r0, BLK), pl.ds(pl.multiple_of(c0, 512), 512)]
        return rcopy(reg, reg, asem.at[0, 0, r], bsem.at[0, 0, r], me.pc)

    def spread_gram(u, s, k):
        i, j = block_of(2 * u + k)
        r = lax.rem(u, RING)
        buf = gw.at[rows_at(i * BLK + me.keep[k][s], BLK >> s), cols(j)]
        return rcopy(buf, buf, gasem.at[s - 1, k, r], gbsem.at[s - 1, k, r], me.peers[k][s - 1])

    def final(u):
        @pl.when(u >= GRAM_UNITS)
        def _():
            for k in range(2):
                spread(u, 4, k).start()
                keep_copy(u, k).start()

        @pl.when(u < GRAM_UNITS)
        def _():
            for k in range(2):
                i, j = block_of(2 * u + k)
                own = rows_at(me.keep[k][4], 16)
                row0 = rows_at(i * BLK + me.keep[k][4], 16)
                mu_r = mut[row0]
                mu_c = sv[pl.ds(j, 1)]
                mm = ALL_ROWS * jnp.concatenate([mu_r, mu_r], axis=1) * mu_c
                cov = (part[lax.rem(u, SLOTS), k, own] - mm) * (1.0 / (ALL_ROWS - 1))
                row = lax.broadcasted_iota(jnp.int32, (16, BLK), 0) + (i * BLK + me.keep[k][4])
                col = lax.broadcasted_iota(jnp.int32, (16, BLK), 1) + j * BLK
                diag = row == col
                std = jnp.sqrt(jnp.where(diag, cov, 1.0) + STD_EPS)
                hinge = jnp.where(std < 1.0, VAR_WEIGHT / (2.0 * std), 0.0)
                weight = jnp.where(i == j, COV_WEIGHT, 2.0 * COV_WEIGHT)
                term = jnp.where(diag, VAR_WEIGHT * jnp.maximum(1.0 - std, 0.0), weight * cov * cov)
                lacc[...] = lacc[...] + term[0:8] + term[8:16]
                gw[row0, cols(j)] = jnp.where(diag, -hinge, (2.0 * COV_WEIGHT) * cov).astype(BF16)
                spread_gram(u, 4, k).start()

    def dz_block(j):
        acc = nn(zd[...], gw[:, cols(j)])
        mean = acc[ROWS:ROWS + 1] + acc[ROWS + 1:ROWS + 2] + acc[ROWS + 2:ROWS + 3]
        diff = zd[0:ROWS, cols(j)].astype(F32) - zod[:, cols(j)].astype(F32)
        sq = jnp.sum((diff * diff).reshape(ROWS // 8, 8, BLK), axis=0)
        lacc[...] = lacc[...] + (0.5 * INV_WEIGHT / ALL_ROWS) * sq
        dz[:, cols(j)] = ((2.0 * INV_WEIGHT / ALL_ROWS) * diff
                          + (2.0 / (ALL_ROWS - 1)) * (acc[0:ROWS] - mean)).astype(BF16)

    def back_block(j, grad, st, layer):
        dx = nt(grad[0:ROWS, :], gw[cols(j)])
        nrm = nv[:, cols(j)]
        act = gb[pl.ds(2 * NB * layer + j, 1)] * nrm + gb[pl.ds(2 * NB * layer + NB + j, 1)]
        d_act = jnp.where(act > 0.0, dx, 0.0)
        da[:, cols(j)] = d_act
        st[pl.ds(j, 1)] = jnp.sum(d_act, axis=0, keepdims=True)
        st[pl.ds(NB + j, 1)] = jnp.sum(d_act * nrm, axis=0, keepdims=True)

    def back_pre(dst, st, layer):
        def step(j, carry):
            scale = gb[pl.ds(2 * NB * layer + j, 1)] * rs_i[pl.ds(NB * layer + j, 1)]
            m0 = st[pl.ds(j, 1)] * (1.0 / ALL_ROWS)
            m1 = st[pl.ds(NB + j, 1)] * (1.0 / ALL_ROWS)
            dst[0:ROWS, cols(j)] = (scale * (da[:, cols(j)] - m0 - nv[:, cols(j)] * m1)).astype(BF16)
            return carry
        lax.fori_loop(0, NB, step, 0)

    compute(jnp.int32(0))

    def slot(t, carry):
        u, ok = unit_at(t - 9 * LAG)

        @pl.when(ok & (u >= GRAM_UNITS))
        def _(u=u):
            cross(u).wait()

        for s in (1, 2, 3, 4):
            u, ok = unit_at(t - LAG * (9 - s))

            @pl.when(ok & (u >= GRAM_UNITS))
            def _(s=s, u=u):
                for k in range(2):
                    cp = spread(u, s, k)
                    cp.wait_send()
                    cp.wait_recv()
                    if s == 4:
                        keep_copy(u, k).wait()
                    if s > 1:
                        spread(u, s - 1, k).start()
                if s == 1:
                    cross(u).start()

            @pl.when(ok & (u < GRAM_UNITS))
            def _(s=s, u=u):
                for k in range(2):
                    cp = spread_gram(u, s, k)
                    cp.wait_send()
                    cp.wait_recv()
                    if s > 1:
                        spread_gram(u, s - 1, k).start()
                if s == 1:
                    for k in range(2):
                        i, j = block_of(2 * u + k)

                        @pl.when(i != j)
                        def _():
                            gw[rows_at(j * BLK, BLK), cols(i)] = gw[rows_at(i * BLK, BLK), cols(j)].T

        sc.advance(t, final)
        u, ok = unit_at(t)

        @pl.when(ok)
        def _(u=u):
            sc.begin(u)

        for first, red in ((0, red0), (PASS_2 + 4, red2), (PASS_1 + 4, red1)):
            for k in range(4):
                @pl.when(t == first + k + 1)
                def _(red=red, k=k):
                    red.finish(k)

                @pl.when(t == first + k)
                def _(red=red, k=k):
                    red.start(k)

        @pl.when(t == 5)
        def _():
            mean = sv[...] * (1.0 / ALL_ROWS)
            sv[...] = mean
            hi = mean.astype(BF16)
            mid = (mean - hi.astype(F32)).astype(BF16)
            low = (mean - hi.astype(F32) - mid.astype(F32)).astype(BF16)
            for j in range(NB):
                for h in range(2):
                    lanes = slice(128 * h, 128 * h + 128)
                    dst = slice(j * BLK + 128 * h, j * BLK + 128 * h + 128)
                    mut[dst] = jnp.broadcast_to(mean[j:j + 1, lanes], (128, 128)).T
                zd[ROWS:ROWS + 16, j * BLK:(j + 1) * BLK] = jnp.concatenate(
                    [hi[j:j + 1], mid[j:j + 1], low[j:j + 1], jnp.zeros((13, BLK), BF16)], axis=0)

        @pl.when(t == DZ_SLOTS[0] - 1)
        def _():
            swap_z.wait()
            for cp in swaps + loads:
                cp.wait()

        for p, first in enumerate(DZ_SLOTS):
            @pl.when(t == first + 1)
            def _(p=p):
                swap_dz(p).wait()

            @pl.when(t == first)
            def _(p=p):
                def step(j, carry):
                    dz_block(2 * p + j)
                    return carry
                lax.fori_loop(0, 2, step, 0)
                swap_dz(p).start()

        @pl.when(t == DZ_SLOTS[3])
        def _():
            load_w3.start()

        @pl.when(t == PASS_2)
        def _():
            s2[2 * NB:3 * NB] = lacc[...]
            load_w3.wait()

        @pl.when(t == PASS_1)
        def _():
            load_w2.wait()
            load_n1.wait()
            swap_du2.wait()

        @pl.when(t == START_2 + 14)
        def _():
            swap_du1.wait()

        for first, grad, st, layer, dst in ((PASS_2, dz, s2, 1, zd), (PASS_1, zd, s1, 0, dz)):
            @pl.when((t >= first) & (t < first + 4))
            def _(first=first, grad=grad, st=st, layer=layer):
                def step(j, carry):
                    back_block(2 * (t - first) + j, grad, st, layer)
                    return carry
                lax.fori_loop(0, 2, step, 0)

            @pl.when(t == first + 8)
            def _(st=st, layer=layer, dst=dst):
                back_pre(dst, st, layer)

        @pl.when(t == PASS_2 + 4)
        def _():
            load_w2.start()

        @pl.when(t == PASS_2 + 8)
        def _():
            load_n1.start()
            swap_du2.start()
            swap_s2.start()

        @pl.when(t == PASS_1 + 8)
        def _():
            swap_du1.start()
            swap_s1.start()

        u, ok = unit_at(t + 1)

        @pl.when(ok)
        def _(u=u):
            compute(u)
        return carry
    lax.fori_loop(0, END, slot, 0)
    swap_s2.wait()
    swap_s1.wait()
    st2_o[...] = s2[...] + e2[...]
    st1_o[...] = s1[...] + e1[...]


def backward(z, x2, x1, h, n2, n1, w3, w2, gb, rs):
    act = pltpu.VMEM((ROWS, DIM), BF16)
    piece = pltpu.VMEM((ROWS, 1024), BF16)
    feat = pltpu.VMEM((ROWS, 256), BF16)
    wide = pltpu.VMEM((ROWS, DIM), F32)
    dma = pltpu.SemaphoreType.DMA
    return pl.pallas_call(
        back_kernel,
        out_shape=(sds((2 * DIM + FEAT, DIM), F32), sds((3 * NB, BLK), F32), sds((2 * NB, BLK), F32)),
        in_specs=[ANY] * 8 + [INV] * 2,
        out_specs=(ANY, INV, INV),
        scratch_shapes=[pltpu.VMEM((ROWS + 16, DIM), BF16), act, act, act, pltpu.VMEM((DIM, DIM), BF16),
                        piece, piece, piece, piece, feat, feat, wide, wide, pltpu.VMEM((DIM, 128), F32),
                        pltpu.VMEM((NB, BLK), F32)]
        + scatter_scratch(SLOTS) + small_scratch(NB) + small_scratch(3 * NB) + small_scratch(2 * NB)
        + [pltpu.VMEM((3 * NB, BLK), F32), pltpu.VMEM((2 * NB, BLK), F32),
           dma((4, 2, RING)), dma((4, 2, RING)), dma((5, 2, RING)), dma((5, 2, RING)), dma((2, RING)),
           dma((8,)), dma((12,)), dma((12,))],
        compiler_params=pltpu.CompilerParams(collective_id=1, has_side_effects=True, vmem_limit_bytes=VMEM_LIMIT),
        name='backward',
    )(z, x2, x1, h, n2, n1, w3, w2, gb, rs)


def solution(mesh):
    def local_step(h_a, h_b, w_one, w_two, w_three, gain_one, bias_one, gain_two, bias_two):
        gb = jnp.stack([gain_one, bias_one, gain_two, bias_two]).reshape(4 * NB, BLK)
        n1, n2, x1, x2, z, rs, h = forward(h_a, h_b, w_one, w_two, w_three, gb)
        grads, st2, st1 = backward(z, x2, x1, h, n2, n1, w_three, w_two, gb, rs)
        loss = jnp.sum(st2[2 * NB:])
        return (loss, grads[2 * DIM:], grads[DIM:2 * DIM], grads[:DIM],
                st1[NB:2 * NB].reshape(DIM), st1[:NB].reshape(DIM),
                st2[NB:2 * NB].reshape(DIM), st2[:NB].reshape(DIM))

    row_spec = P('data', None)
    return jax.shard_map(local_step, mesh=mesh,
                         in_specs=(row_spec, row_spec, P(), P(), P(), P(), P(), P(), P()),
                         out_specs=(P(), P(), P(), P(), P(), P(), P(), P()),
                         check_vma=False)
```

```python
import functools

import jax
import jax.numpy as jnp
from jax import lax
from jax.experimental import pallas as pl
from jax.experimental.pallas import tpu as pltpu
from jax.sharding import PartitionSpec as P

BN_EPS = 1e-5
STD_EPS = 1e-4
INV_WEIGHT = 2.0
VAR_WEIGHT = 1.0
COV_WEIGHT = 2.0

F32 = jnp.float32
BF16 = jnp.bfloat16
MESH = pl.DeviceIdType.MESH
VMEM_LIMIT = 67043328

ROWS = 1024
HALF = 512
FEAT = 512
DIM = 2048
NB = 8
BLK = 256
LAG = 2
RING = 4
ALL_ROWS = 16384


def sds(shape, dtype):
    return jax.ShapeDtypeStruct(shape, dtype)


ANY = pl.BlockSpec(memory_space=pl.ANY)
INV = pl.BlockSpec(memory_space=pltpu.VMEM)


class Place:
    def __init__(self):
        i = lax.axis_index('data')
        self.c = lax.rem(i, 2)
        x = lax.rem(i // 2, 2)
        y = lax.rem(i // 4, 2)
        z = i // 8
        zl = lax.rem(z, 2)
        zh = z // 2
        self.pc = i + 1 - 2 * self.c
        px = i + 2 - 4 * x
        py = i + 4 - 8 * y
        p1 = i + 8 - 16 * zl
        p2 = i + 16 - 32 * zh
        pd = px + py - i
        p3 = p1 + p2 - i
        self.phases = ((px, py, pd), (p1, p2, p3))
        self.bits = ((x, zl, y, zh), (y, zl, x, zh))
        self.peers = ((px, p1, py, p2), (py, p1, px, p2))
        self.keep = []
        self.send = []
        for k in range(2):
            keep = [0]
            send = [None]
            for s in range(1, 5):
                n = BLK >> s
                bit = self.bits[k][s - 1]
                send.append(keep[-1] + (1 - bit) * n)
                keep.append(keep[-1] + bit * n)
            self.keep.append(keep)
            self.send.append(send)

    def barrier(self):
        sem = pltpu.get_barrier_semaphore()
        for p in (self.pc,) + self.phases[0] + self.phases[1]:
            pl.semaphore_signal(sem, inc=1, device_id=(p,), device_id_type=MESH)
        pl.semaphore_wait(sem, 7)


def rcopy(src, dst, ssem, rsem, dev):
    return pltpu.make_async_remote_copy(src_ref=src, dst_ref=dst, send_sem=ssem, recv_sem=rsem,
                                        device_id=(dev,), device_id_type=MESH)


def rows_at(off, n):
    return pl.ds(pl.multiple_of(off, n), n)


def nn(a, b):
    return jnp.dot(a, b, preferred_element_type=F32)


def nt(a, b):
    return lax.dot_general(a, b, (((1,), (1,)), ((), ())), preferred_element_type=F32)


def tn(a, b):
    return lax.dot_general(a, b, (((0,), (0,)), ((), ())), preferred_element_type=F32)


def cols(j):
    return pl.ds(pl.multiple_of(j * BLK, BLK), BLK)


class Scatter:
    def __init__(self, place, part, lands, ssem, rsem):
        self.pl, self.part, self.lands, self.ssem, self.rsem = place, part, lands, ssem, rsem

    def copy(self, u, s, k):
        n = BLK >> s
        r = lax.rem(u, RING)
        return rcopy(self.part.at[lax.rem(u, SLOTS), k, rows_at(self.pl.send[k][s], n)],
                     self.lands[s - 1].at[r, k], self.ssem.at[s - 1, k, r], self.rsem.at[s - 1, k, r],
                     self.pl.peers[k][s - 1])

    def begin(self, u):
        for k in range(2):
            self.copy(u, 1, k).start()

    def advance(self, t, final):
        for s in (4, 3, 2, 1):
            u, ok = unit_at(t - LAG * s)

            @pl.when(ok)
            def _(s=s, u=u):
                n = BLK >> s
                p, r = lax.rem(u, SLOTS), lax.rem(u, RING)
                for k in range(2):
                    cp = self.copy(u, s, k)
                    cp.wait_send()
                    cp.wait_recv()
                    rr = rows_at(self.pl.keep[k][s], n)
                    self.part[p, k, rr] = self.part[p, k, rr] + self.lands[s - 1][r, k]
                    if s < 4:
                        self.copy(u, s + 1, k).start()
                if s == 4:
                    final(u)


def scatter_scratch(slots):
    return [pltpu.VMEM((slots, 2, BLK, BLK), F32)] + \
        [pltpu.VMEM((RING, 2, BLK >> s, BLK), F32) for s in range(1, 5)] + \
        [pltpu.SemaphoreType.DMA((4, 2, RING)), pltpu.SemaphoreType.DMA((4, 2, RING))]


class SmallReduce:
    def __init__(self, place, val, land, ssem, rsem):
        self.pl, self.val, self.land, self.ssem, self.rsem = place, val, land, ssem, rsem

    def copies(self, ph):
        return [rcopy(self.val, self.land.at[ph, k], self.ssem.at[ph, k], self.rsem.at[ph, k], p)
                for k, p in enumerate(self.pl.phases[ph])]

    def start(self, ph):
        for cp in self.copies(ph):
            cp.start()

    def finish(self, ph):
        for cp in self.copies(ph):
            cp.wait()
        self.val[...] = (self.val[...] + self.land[ph, 0]) + (self.land[ph, 1] + self.land[ph, 2])

    def run(self):
        for ph in range(2):
            self.start(ph)
            self.finish(ph)


def small_scratch(n):
    return [pltpu.VMEM((n, BLK), F32), pltpu.VMEM((2, 3, n, BLK), F32),
            pltpu.SemaphoreType.DMA((2, 3)), pltpu.SemaphoreType.DMA((2, 3))]


GRAM_UNITS = 18
UNITS = 54
SLOTS = 5 * LAG + 2
START_3 = 26
START_2 = 42
END = START_2 + 20 + 9 * LAG
DZ_SLOTS = (23, 28, 32, 34)
PASS_2 = 35
PASS_1 = 43


def block_of(q):
    i = jnp.int32(0)
    for first in (8, 15, 21, 26, 30, 33, 35):
        i = i + jnp.where(q >= first, 1, 0)
    return i, i + q - (17 * i - i * i) // 2


def unit_at(t):
    u = jnp.where(t < START_3, t, jnp.where(t < START_2, t - (START_3 - 18), t - (START_2 - 34)))
    ok = ((t >= 0) & (t < 18)) | ((t >= START_3) & (t < START_3 + 16)) | ((t >= START_2) & (t < START_2 + 20))
    return jnp.where(ok, u, 0), ok


def step_kernel(ha, hb, w1, w2, w3, gb, g_o, n1_o, st2_o, st1_o,
                zd, zod, dz, dzo, gw, x2h, x2o, x1h, x1o, hv, ho, nv, da, mut, lacc, rs,
                part, r1, r2, r3, r4, ssem, rsem, sv, sl, sa, sb, f1, fl1, fa1, fb1, f2, fl2, fa2, fb2,
                s2, l2, a2, b2, s1, l1, a1, b1, e2, e1,
                gasem, gbsem, asem, bsem, lsem, csem, dsem, esem):
    me = Place()
    c = me.c
    half = pl.ds(pl.multiple_of(c * 1024, 1024), 1024)
    ohalf = pl.ds(pl.multiple_of((1 - c) * 1024, 1024), 1024)
    hhalf = pl.ds(pl.multiple_of(c * 256, 256), 256)
    hohalf = pl.ds(pl.multiple_of((1 - c) * 256, 256), 256)
    mine = pl.ds(pl.multiple_of(c * HALF, HALF), HALF)
    body = pl.ds(0, ROWS)
    w1v = zod.at[pl.ds(0, FEAT)]
    load_w1 = pltpu.make_async_copy(w1, w1v, csem.at[0])
    load_w2a = pltpu.make_async_copy(w2, gw, csem.at[1])
    load_w3a = pltpu.make_async_copy(w3, gw, csem.at[2])
    load_w3 = pltpu.make_async_copy(w3, gw, csem.at[5])
    load_w2 = pltpu.make_async_copy(w2, gw, csem.at[6])
    load_n1 = pltpu.make_async_copy(n1_o, nv, csem.at[7])
    save_n1 = pltpu.make_async_copy(da, n1_o, csem.at[8])
    keep_x1 = pltpu.make_async_copy(dzo.at[:, half], x1h, csem.at[3])
    keep_x2 = pltpu.make_async_copy(dz.at[:, half], x2h, csem.at[4])
    swap_z = rcopy(zd.at[body], zod, dsem.at[0], esem.at[0], me.pc)
    swap_x2 = rcopy(dz.at[:, ohalf], x2o, dsem.at[1], esem.at[1], me.pc)
    swap_x1 = rcopy(dzo.at[:, ohalf], x1o, dsem.at[2], esem.at[2], me.pc)
    swap_h = rcopy(hv.at[:, hohalf], ho, dsem.at[3], esem.at[3], me.pc)
    swap_du2 = rcopy(zd.at[body], zod, dsem.at[4], esem.at[4], me.pc)
    swap_du1 = rcopy(dz, dzo, dsem.at[5], esem.at[5], me.pc)
    swap_s2 = rcopy(s2, e2, dsem.at[6], esem.at[6], me.pc)
    swap_s1 = rcopy(s1, e1, dsem.at[7], esem.at[7], me.pc)

    def load_h(src):
        return pltpu.make_async_copy(src, hv.at[mine], csem.at[9])

    def give_h(src):
        return rcopy(src, hv.at[mine], dsem.at[12], esem.at[12], me.pc)

    def swap_dz(p):
        part_cols = pl.ds(512 * p, 512)
        return rcopy(dz.at[:, part_cols], dzo.at[:, part_cols], dsem.at[8 + p], esem.at[8 + p], me.pc)

    for k, own in ((0, ha), (1, hb)):
        @pl.when(c == k)
        def _(own=own):
            load_h(own).start()
    load_w1.start()
    load_w2a.start()
    me.barrier()
    for k, other in ((0, hb), (1, ha)):
        @pl.when(c == k)
        def _(other=other):
            give_h(other).start()
    lacc[...] = jnp.zeros_like(lacc)

    def matmul(src, w, dst, st):
        def step(j, carry):
            res = nn(src[...], w[:, cols(j)])
            dst[:, cols(j)] = res
            st[pl.ds(j, 1)] = jnp.sum(res, axis=0, keepdims=True)
            st[pl.ds(NB + j, 1)] = jnp.sum(res * res, axis=0, keepdims=True)
            return carry
        lax.fori_loop(0, NB, step, 0)

    def norm(u, x, st, layer):
        mean = st[0:NB] * (1.0 / ALL_ROWS)
        var = st[NB:2 * NB] * (1.0 / ALL_ROWS) - mean * mean
        inv = lax.rsqrt(var + BN_EPS)
        st[0:NB] = mean
        st[NB:2 * NB] = inv
        rs[NB * layer:NB * layer + NB] = inv

        def step(j, carry):
            nrm = (u[:, cols(j)] - st[pl.ds(j, 1)]) * st[pl.ds(NB + j, 1)]
            act = gb[pl.ds(2 * NB * layer + j, 1)] * nrm + gb[pl.ds(2 * NB * layer + NB + j, 1)]
            u[:, cols(j)] = nrm
            x[:, cols(j)] = jnp.maximum(act, 0.0).astype(BF16)
            return carry
        lax.fori_loop(0, NB, step, 0)

    load_w1.wait()
    load_h(ha).wait()
    give_h(ha).wait()
    swap_h.start()
    matmul(hv, w1v, da, f1)
    SmallReduce(me, f1, fl1, fa1, fb1).run()
    norm(da, dzo, f1, 0)
    save_n1.start()
    swap_x1.start()
    keep_x1.start()
    load_w2a.wait()
    matmul(dzo, gw, nv, f2)
    load_w3a.start()
    SmallReduce(me, f2, fl2, fa2, fb2).run()
    norm(nv, dz, f2, 1)
    swap_x1.wait()
    swap_x2.start()
    keep_x2.start()
    load_w3a.wait()

    def z_block(j):
        res = nn(dz[...], gw[:, cols(j)]).astype(BF16)
        zd[0:ROWS, cols(j)] = res
        sv[pl.ds(j, 1)] = jnp.sum(res.astype(F32), axis=0, keepdims=True)

    def z_blocks(first):
        def step(j, carry):
            z_block(first + j)
            return carry
        lax.fori_loop(0, 2, step, 0)

    z_blocks(0)
    red0 = SmallReduce(me, sv, sl, sa, sb)
    red2 = SmallReduce(me, s2, l2, a2, b2)
    red1 = SmallReduce(me, s1, l1, a1, b1)
    sc = Scatter(me, part, (r1, r2, r3, r4), ssem, rsem)

    def compute(u):
        p = lax.rem(u, SLOTS)

        @pl.when(u < GRAM_UNITS)
        def _():
            for k in range(2):
                i, j = block_of(2 * u + k)
                part[p, k] = tn(zd[0:ROWS, cols(i)], zd[0:ROWS, cols(j)])

        w, rb, cb = grad_unit(u)
        for w_, la, lb, ra, rb_ in ((0, x2h, x2o, dz, dzo), (1, x1h, x1o, zd, zod), (2, hv, ho, dz, dzo)):
            @pl.when((u >= GRAM_UNITS) & (w == w_))
            def _(w_=w_, la=la, lb=lb, ra=ra, rb_=rb_):
                lc, oc = (hhalf, slice(None)) if w_ == 2 else (cols(rb), cols(rb))
                rc = pl.ds(pl.multiple_of(cb * 512, 512), 512)
                res = tn(la[:, lc], ra[0:ROWS, rc]) + tn(lb[:, oc], rb_[:, rc])
                part[p, 0] = res[:, 0:BLK]
                part[p, 1] = res[:, BLK:2 * BLK]

    def grad_unit(u):
        v = u - GRAM_UNITS
        w = v // 16
        q = lax.rem(v, 16)
        return w, jnp.where(w == 2, 0, lax.rem(q, 4)), jnp.where(w == 2, q, q // 4)

    def base(u):
        w, rb, cb = grad_unit(u)
        return w * 2048 + c * jnp.where(w == 2, 256, 1024) + rb * 256, cb * 512

    def region(u, k, off, n):
        r0, c0 = base(u)
        return g_o.at[rows_at(r0 + off, n), pl.ds(pl.multiple_of(c0 + k * BLK, BLK), BLK)]

    def keep_copy(u, k):
        return pltpu.make_async_copy(part.at[lax.rem(u, SLOTS), k, rows_at(me.keep[k][4], 16)],
                                     region(u, k, me.keep[k][4], 16), lsem.at[k, lax.rem(u, RING)])

    def spread(u, s, k):
        r = lax.rem(u, RING)
        dst = region(u, k, me.keep[k][s], BLK >> s)
        src = part.at[lax.rem(u, SLOTS), k, rows_at(me.keep[k][4], 16)] if s == 4 else dst
        return rcopy(src, dst, asem.at[s, k, r], bsem.at[s, k, r], me.peers[k][s - 1])

    def cross(u):
        r = lax.rem(u, RING)
        r0, c0 = base(u)
        reg = g_o.at[rows_at(r0, BLK), pl.ds(pl.multiple_of(c0, 512), 512)]
        return rcopy(reg, reg, asem.at[0, 0, r], bsem.at[0, 0, r], me.pc)

    def spread_gram(u, s, k):
        i, j = block_of(2 * u + k)
        r = lax.rem(u, RING)
        buf = gw.at[rows_at(i * BLK + me.keep[k][s], BLK >> s), cols(j)]
        return rcopy(buf, buf, gasem.at[s - 1, k, r], gbsem.at[s - 1, k, r], me.peers[k][s - 1])

    def final(u):
        @pl.when(u >= GRAM_UNITS)
        def _():
            for k in range(2):
                spread(u, 4, k).start()
                keep_copy(u, k).start()

        @pl.when(u < GRAM_UNITS)
        def _():
            for k in range(2):
                i, j = block_of(2 * u + k)
                own = rows_at(me.keep[k][4], 16)
                row0 = rows_at(i * BLK + me.keep[k][4], 16)
                mu_r = mut[row0]
                mu_c = sv[pl.ds(j, 1)]
                mm = ALL_ROWS * jnp.concatenate([mu_r, mu_r], axis=1) * mu_c
                cov = (part[lax.rem(u, SLOTS), k, own] - mm) * (1.0 / (ALL_ROWS - 1))
                row = lax.broadcasted_iota(jnp.int32, (16, BLK), 0) + (i * BLK + me.keep[k][4])
                col = lax.broadcasted_iota(jnp.int32, (16, BLK), 1) + j * BLK
                diag = row == col
                std = jnp.sqrt(jnp.where(diag, cov, 1.0) + STD_EPS)
                hinge = jnp.where(std < 1.0, VAR_WEIGHT / (2.0 * std), 0.0)
                weight = jnp.where(i == j, COV_WEIGHT, 2.0 * COV_WEIGHT)
                term = jnp.where(diag, VAR_WEIGHT * jnp.maximum(1.0 - std, 0.0), weight * cov * cov)
                lacc[...] = lacc[...] + term[0:8] + term[8:16]
                gw[row0, cols(j)] = jnp.where(diag, -hinge, (2.0 * COV_WEIGHT) * cov).astype(BF16)
                spread_gram(u, 4, k).start()

    def dz_block(j):
        acc = nn(zd[...], gw[:, cols(j)])
        mean = acc[ROWS:ROWS + 1] + acc[ROWS + 1:ROWS + 2] + acc[ROWS + 2:ROWS + 3]
        diff = zd[0:ROWS, cols(j)].astype(F32) - zod[:, cols(j)].astype(F32)
        sq = jnp.sum((diff * diff).reshape(ROWS // 8, 8, BLK), axis=0)
        lacc[...] = lacc[...] + (0.5 * INV_WEIGHT / ALL_ROWS) * sq
        dz[:, cols(j)] = ((2.0 * INV_WEIGHT / ALL_ROWS) * diff
                          + (2.0 / (ALL_ROWS - 1)) * (acc[0:ROWS] - mean)).astype(BF16)

    def back_block(j, grad, st, layer):
        dx = nt(grad[0:ROWS, :], gw[cols(j)])
        nrm = nv[:, cols(j)]
        act = gb[pl.ds(2 * NB * layer + j, 1)] * nrm + gb[pl.ds(2 * NB * layer + NB + j, 1)]
        d_act = jnp.where(act > 0.0, dx, 0.0)
        da[:, cols(j)] = d_act
        st[pl.ds(j, 1)] = jnp.sum(d_act, axis=0, keepdims=True)
        st[pl.ds(NB + j, 1)] = jnp.sum(d_act * nrm, axis=0, keepdims=True)

    def back_pre(dst, st, layer):
        def step(j, carry):
            scale = gb[pl.ds(2 * NB * layer + j, 1)] * rs[pl.ds(NB * layer + j, 1)]
            m0 = st[pl.ds(j, 1)] * (1.0 / ALL_ROWS)
            m1 = st[pl.ds(NB + j, 1)] * (1.0 / ALL_ROWS)
            dst[0:ROWS, cols(j)] = (scale * (da[:, cols(j)] - m0 - nv[:, cols(j)] * m1)).astype(BF16)
            return carry
        lax.fori_loop(0, NB, step, 0)

    compute(jnp.int32(0))

    def slot(t, carry):
        u, ok = unit_at(t - 9 * LAG)

        @pl.when(ok & (u >= GRAM_UNITS))
        def _(u=u):
            cross(u).wait()

        for s in (1, 2, 3, 4):
            u, ok = unit_at(t - LAG * (9 - s))

            @pl.when(ok & (u >= GRAM_UNITS))
            def _(s=s, u=u):
                for k in range(2):
                    cp = spread(u, s, k)
                    cp.wait_send()
                    cp.wait_recv()
                    if s == 4:
                        keep_copy(u, k).wait()
                    if s > 1:
                        spread(u, s - 1, k).start()
                if s == 1:
                    cross(u).start()

            @pl.when(ok & (u < GRAM_UNITS))
            def _(s=s, u=u):
                for k in range(2):
                    cp = spread_gram(u, s, k)
                    cp.wait_send()
                    cp.wait_recv()
                    if s > 1:
                        spread_gram(u, s - 1, k).start()
                if s == 1:
                    for k in range(2):
                        i, j = block_of(2 * u + k)

                        @pl.when(i != j)
                        def _():
                            gw[rows_at(j * BLK, BLK), cols(i)] = gw[rows_at(i * BLK, BLK), cols(j)].T

        sc.advance(t, final)
        u, ok = unit_at(t)

        @pl.when(ok)
        def _(u=u):
            sc.begin(u)

        for first, red in ((3, red0), (PASS_2 + 3, red2), (PASS_1 + 3, red1)):
            for ph in range(2):
                @pl.when(t == first + ph + 1)
                def _(red=red, ph=ph):
                    red.finish(ph)

                @pl.when(t == first + ph)
                def _(red=red, ph=ph):
                    red.start(ph)

        @pl.when(t == 5)
        def _():
            mean = sv[...] * (1.0 / ALL_ROWS)
            sv[...] = mean
            hi = mean.astype(BF16)
            mid = (mean - hi.astype(F32)).astype(BF16)
            low = (mean - hi.astype(F32) - mid.astype(F32)).astype(BF16)
            for j in range(NB):
                for h in range(2):
                    lanes = slice(128 * h, 128 * h + 128)
                    dst = slice(j * BLK + 128 * h, j * BLK + 128 * h + 128)
                    mut[dst] = jnp.broadcast_to(mean[j:j + 1, lanes], (128, 128)).T
                zd[ROWS:ROWS + 16, j * BLK:(j + 1) * BLK] = jnp.concatenate(
                    [hi[j:j + 1], mid[j:j + 1], low[j:j + 1], jnp.zeros((13, BLK), BF16)], axis=0)

        @pl.when(t < 3)
        def _():
            z_blocks(2 * t + 2)

        @pl.when(t == 3)
        def _():
            keep_x1.wait()
            keep_x2.wait()
            swap_x2.wait()
            swap_h.wait()
            save_n1.wait()
            swap_z.start()

        @pl.when(t == DZ_SLOTS[0] - 1)
        def _():
            swap_z.wait()

        for p, first in enumerate(DZ_SLOTS):
            @pl.when(t == first + 1)
            def _(p=p):
                swap_dz(p).wait()

            @pl.when(t == first)
            def _(p=p):
                def step(j, carry):
                    dz_block(2 * p + j)
                    return carry
                lax.fori_loop(0, 2, step, 0)
                swap_dz(p).start()

        @pl.when(t == DZ_SLOTS[3])
        def _():
            load_w3.start()

        @pl.when(t == PASS_2)
        def _():
            s2[2 * NB:3 * NB] = lacc[...]
            load_w3.wait()

        @pl.when(t == PASS_1)
        def _():
            load_w2.wait()
            load_n1.wait()

        @pl.when(t == START_2 - 1)
        def _():
            swap_du2.wait()

        @pl.when(t == START_2 + 14)
        def _():
            swap_du1.wait()

        for first, grad, st, layer, dst in ((PASS_2, dz, s2, 1, zd), (PASS_1, zd, s1, 0, dz)):
            @pl.when((t >= first) & (t < first + 3))
            def _(first=first, grad=grad, st=st, layer=layer):
                def step(j, carry):
                    back_block(j, grad, st, layer)
                    return carry
                lo = 3 * (t - first)
                lax.fori_loop(lo, jnp.minimum(lo + 3, NB), step, 0)

            @pl.when(t == first + 5)
            def _(st=st, layer=layer, dst=dst):
                back_pre(dst, st, layer)

        @pl.when(t == PASS_2 + 3)
        def _():
            load_w2.start()

        @pl.when(t == PASS_2 + 5)
        def _():
            load_n1.start()
            swap_du2.start()
            swap_s2.start()

        @pl.when(t == PASS_1 + 5)
        def _():
            swap_du1.start()
            swap_s1.start()

        u, ok = unit_at(t + 1)

        @pl.when(ok)
        def _(u=u):
            compute(u)
        return carry
    lax.fori_loop(0, END, slot, 0)
    swap_s2.wait()
    swap_s1.wait()
    st2_o[...] = s2[...] + e2[...]
    st1_o[...] = s1[...] + e1[...]


def train_step(ha, hb, w1, w2, w3, gb):
    act = pltpu.VMEM((ROWS, DIM), BF16)
    piece = pltpu.VMEM((ROWS, 1024), BF16)
    wide = pltpu.VMEM((ROWS, DIM), F32)
    dma = pltpu.SemaphoreType.DMA
    return pl.pallas_call(
        step_kernel,
        out_shape=(sds((2 * DIM + FEAT, DIM), F32), sds((ROWS, DIM), F32), sds((3 * NB, BLK), F32),
                   sds((2 * NB, BLK), F32)),
        in_specs=[ANY] * 5 + [INV],
        out_specs=(ANY, ANY, INV, INV),
        scratch_shapes=[pltpu.VMEM((ROWS + 16, DIM), BF16), act, act, act, pltpu.VMEM((DIM, DIM), BF16),
                        piece, piece, piece, piece, pltpu.VMEM((ROWS, FEAT), BF16), pltpu.VMEM((ROWS, 256), BF16),
                        wide, wide, pltpu.VMEM((DIM, 128), F32), pltpu.VMEM((NB, BLK), F32),
                        pltpu.VMEM((2 * NB, BLK), F32)]
        + scatter_scratch(SLOTS) + small_scratch(NB) + small_scratch(2 * NB) + small_scratch(2 * NB)
        + small_scratch(3 * NB) + small_scratch(2 * NB)
        + [pltpu.VMEM((3 * NB, BLK), F32), pltpu.VMEM((2 * NB, BLK), F32),
           dma((4, 2, RING)), dma((4, 2, RING)), dma((5, 2, RING)), dma((5, 2, RING)), dma((2, RING)),
           dma((10,)), dma((13,)), dma((13,))],
        compiler_params=pltpu.CompilerParams(collective_id=0, has_side_effects=True, vmem_limit_bytes=VMEM_LIMIT),
        name='train_step',
    )(ha, hb, w1, w2, w3, gb)


def solution(mesh):
    def local_step(h_a, h_b, w_one, w_two, w_three, gain_one, bias_one, gain_two, bias_two):
        gb = jnp.stack([gain_one, bias_one, gain_two, bias_two]).reshape(4 * NB, BLK)
        grads, _, st2, st1 = train_step(h_a, h_b, w_one, w_two, w_three, gb)
        loss = jnp.sum(st2[2 * NB:])
        return (loss, grads[2 * DIM:], grads[DIM:2 * DIM], grads[:DIM],
                st1[NB:2 * NB].reshape(DIM), st1[:NB].reshape(DIM),
                st2[NB:2 * NB].reshape(DIM), st2[:NB].reshape(DIM))

    row_spec = P('data', None)
    return jax.shard_map(local_step, mesh=mesh,
                         in_specs=(row_spec, row_spec, P(), P(), P(), P(), P(), P(), P()),
                         out_specs=(P(), P(), P(), P(), P(), P(), P(), P()),
                         check_vma=False)
```

```python
import functools

import jax
import jax.numpy as jnp
from jax import lax
from jax.experimental import pallas as pl
from jax.experimental.pallas import tpu as pltpu
from jax.sharding import PartitionSpec as P

BN_EPS = 1e-5
STD_EPS = 1e-4
INV_WEIGHT = 2.0
VAR_WEIGHT = 1.0
COV_WEIGHT = 2.0

F32 = jnp.float32
BF16 = jnp.bfloat16
MESH = pl.DeviceIdType.MESH
VMEM_LIMIT = 67043328

ROWS = 1024
HALF = 512
FEAT = 512
DIM = 2048
NB = 8
BLK = 256
LAG = 2
RING = 4
ALL_ROWS = 16384


def sds(shape, dtype):
    return jax.ShapeDtypeStruct(shape, dtype)


ANY = pl.BlockSpec(memory_space=pl.ANY)
INV = pl.BlockSpec(memory_space=pltpu.VMEM)


class Place:
    def __init__(self):
        i = lax.axis_index('data')
        self.c = lax.rem(i, 2)
        x = lax.rem(i // 2, 2)
        y = lax.rem(i // 4, 2)
        z = i // 8
        zl = lax.rem(z, 2)
        zh = z // 2
        self.pc = i + 1 - 2 * self.c
        px = i + 2 - 4 * x
        py = i + 4 - 8 * y
        p1 = i + 8 - 16 * zl
        p2 = i + 16 - 32 * zh
        pd = px + py - i
        p3 = p1 + p2 - i
        self.phases = ((px, py, pd), (p1, p2, p3))
        self.bits = ((x, zl, y, zh), (y, zl, x, zh))
        self.peers = ((px, p1, py, p2), (py, p1, px, p2))
        self.keep = []
        self.send = []
        for k in range(2):
            keep = [0]
            send = [None]
            for s in range(1, 5):
                n = BLK >> s
                bit = self.bits[k][s - 1]
                send.append(keep[-1] + (1 - bit) * n)
                keep.append(keep[-1] + bit * n)
            self.keep.append(keep)
            self.send.append(send)

    def barrier(self):
        sem = pltpu.get_barrier_semaphore()
        for p in (self.pc,) + self.phases[0] + self.phases[1]:
            pl.semaphore_signal(sem, inc=1, device_id=(p,), device_id_type=MESH)
        pl.semaphore_wait(sem, 7)


def rcopy(src, dst, ssem, rsem, dev):
    return pltpu.make_async_remote_copy(src_ref=src, dst_ref=dst, send_sem=ssem, recv_sem=rsem,
                                        device_id=(dev,), device_id_type=MESH)


def rows_at(off, n):
    return pl.ds(pl.multiple_of(off, n), n)


def nn(a, b):
    return jnp.dot(a, b, preferred_element_type=F32)


def nt(a, b):
    return lax.dot_general(a, b, (((1,), (1,)), ((), ())), preferred_element_type=F32)


def tn(a, b):
    return lax.dot_general(a, b, (((0,), (0,)), ((), ())), preferred_element_type=F32)


def lanes_at(off):
    return pl.ds(pl.multiple_of(off, 128), 128)


def cols_at(off):
    return pl.ds(pl.multiple_of(off, BLK), BLK)


def cols(j):
    return pl.ds(pl.multiple_of(j * BLK, BLK), BLK)


class Scatter:
    def __init__(self, place, part, lands, ssem, rsem):
        self.pl, self.part, self.lands, self.ssem, self.rsem = place, part, lands, ssem, rsem

    def copy(self, u, s, k):
        n = BLK >> s
        r = lax.rem(u, RING)
        return rcopy(self.part.at[lax.rem(u, SLOTS), k, rows_at(self.pl.send[k][s], n)],
                     self.lands[s - 1].at[r, k], self.ssem.at[s - 1, k, r], self.rsem.at[s - 1, k, r],
                     self.pl.peers[k][s - 1])

    def begin(self, u):
        for k in range(2):
            self.copy(u, 1, k).start()

    def advance(self, t, final):
        for s in (4, 3, 2, 1):
            u, ok = unit_at(t - LAG * s)

            @pl.when(ok)
            def _(s=s, u=u):
                n = BLK >> s
                p, r = lax.rem(u, SLOTS), lax.rem(u, RING)
                for k in range(2):
                    cp = self.copy(u, s, k)
                    cp.wait_send()
                    cp.wait_recv()
                    rr = rows_at(self.pl.keep[k][s], n)
                    self.part[p, k, rr] = self.part[p, k, rr] + self.lands[s - 1][r, k]
                    if s < 4:
                        self.copy(u, s + 1, k).start()
                if s == 4:
                    final(u)


def scatter_scratch(slots):
    return [pltpu.VMEM((slots, 2, BLK, BLK), F32)] + \
        [pltpu.VMEM((RING, 2, BLK >> s, BLK), F32) for s in range(1, 5)] + \
        [pltpu.SemaphoreType.DMA((4, 2, RING)), pltpu.SemaphoreType.DMA((4, 2, RING))]


class SmallReduce:
    def __init__(self, place, val, land, ssem, rsem):
        self.pl, self.val, self.land, self.ssem, self.rsem = place, val, land, ssem, rsem

    def copies(self, ph):
        return [rcopy(self.val, self.land.at[ph, k], self.ssem.at[ph, k], self.rsem.at[ph, k], p)
                for k, p in enumerate(self.pl.phases[ph])]

    def start(self, ph):
        for cp in self.copies(ph):
            cp.start()

    def finish(self, ph):
        for cp in self.copies(ph):
            cp.wait()
        self.val[...] = (self.val[...] + self.land[ph, 0]) + (self.land[ph, 1] + self.land[ph, 2])

    def run(self):
        for ph in range(2):
            self.start(ph)
            self.finish(ph)


def small_scratch(n):
    return [pltpu.VMEM((n, BLK), F32), pltpu.VMEM((2, 3, n, BLK), F32),
            pltpu.SemaphoreType.DMA((2, 3)), pltpu.SemaphoreType.DMA((2, 3))]


GRAM_UNITS = 18
UNITS = 54
SLOTS = 4 * LAG + 1
START_3 = 24
START_2 = 41
END = START_2 + 21 + 9 * LAG
DZ_SLOTS = (20, 23, 26, 28, 30, 32, 33, 34)
PASS_2 = 35
PASS_1 = 42


def block_of(q):
    i = jnp.int32(0)
    for first in (8, 15, 21, 26, 30, 33, 35):
        i = i + jnp.where(q >= first, 1, 0)
    return i, i + q - (17 * i - i * i) // 2


def unit_at(t):
    u = jnp.where(t < START_3, t, jnp.where(t < START_2, t - (START_3 - 18), t - (START_2 - 34)))
    ok = ((t >= 0) & (t < 18)) | ((t >= START_3) & (t < START_3 + 16)) | ((t >= START_2) & (t < START_2 + 20))
    return jnp.where(ok, u, 0), ok


def step_kernel(ha, hb, w1, w2, w3, g1, b1, g2, b2, g3_o, g2_o, g1_o, n1_o, st_o,
                zd, zod, dz, dzo, gw, x2h, x2o, x1h, x1o, hh, ho, g2v, g1v, lacc, rs, stage,
                part, r1, r2, r3, r4, ssem, rsem, sv, sl, sa, sb, f1, fl1, fa1, fb1, f2, fl2, fa2, fb2,
                s2, l2, sa2, sb2, s1, l1, sa1, sb1, e2, e1,
                gasem, gbsem, asem, bsem, lsem, psem, csem, dsem, esem):
    me = Place()
    c = me.c
    nv, da = g2v.at[pl.ds(0, ROWS)], g2v.at[pl.ds(ROWS, ROWS)]
    hv = x2o.at[:, pl.ds(0, FEAT)]
    gains, biases = (g1, g2), (b1, b2)
    half = pl.ds(pl.multiple_of(c * 1024, 1024), 1024)
    ohalf = pl.ds(pl.multiple_of((1 - c) * 1024, 1024), 1024)
    hhalf = pl.ds(pl.multiple_of(c * 256, 256), 256)
    hohalf = pl.ds(pl.multiple_of((1 - c) * 256, 256), 256)
    mine = pl.ds(pl.multiple_of(c * HALF, HALF), HALF)
    body = pl.ds(0, ROWS)
    w1v = zod.at[pl.ds(0, FEAT)]
    load_w1 = pltpu.make_async_copy(w1, w1v, csem.at[0])
    load_w2a = pltpu.make_async_copy(w2, gw, csem.at[1])
    load_w3a = pltpu.make_async_copy(w3, gw, csem.at[2])
    load_w3 = pltpu.make_async_copy(w3, gw, csem.at[2])
    load_w2 = pltpu.make_async_copy(w2, gw, csem.at[6])
    load_n1 = pltpu.make_async_copy(n1_o, nv, csem.at[7])
    save_n1 = pltpu.make_async_copy(da, n1_o, csem.at[8])
    keep_x1 = pltpu.make_async_copy(dzo.at[:, half], x1h, csem.at[3])
    keep_h = pltpu.make_async_copy(hv.at[:, hhalf], hh, csem.at[5])
    keep_x2 = pltpu.make_async_copy(dz.at[:, half], x2h, csem.at[4])
    swap_z = rcopy(zd.at[body], zod, dsem.at[0], esem.at[0], me.pc)
    swap_x2 = rcopy(dz.at[:, ohalf], x2o, dsem.at[1], esem.at[1], me.pc)
    swap_x1 = rcopy(dzo.at[:, ohalf], x1o, dsem.at[2], esem.at[2], me.pc)
    swap_h = rcopy(hv.at[:, hohalf], ho, dsem.at[3], esem.at[3], me.pc)
    swap_du2 = rcopy(zd.at[body], zod, dsem.at[4], esem.at[4], me.pc)
    swap_du1 = rcopy(dz, dzo, dsem.at[5], esem.at[5], me.pc)
    swap_s2 = rcopy(s2, e2, dsem.at[6], esem.at[6], me.pc)
    swap_s1 = rcopy(s1, e1, dsem.at[7], esem.at[7], me.pc)

    def load_h(src):
        return pltpu.make_async_copy(src, hv.at[mine], csem.at[9])

    def give_h(src):
        return rcopy(src, hv.at[mine], dsem.at[16], esem.at[16], me.pc)

    def swap_dz(j):
        return rcopy(dz.at[:, cols(j)], dzo.at[:, cols(j)], dsem.at[8 + j], esem.at[8 + j], me.pc)

    for k, own in ((0, ha), (1, hb)):
        @pl.when(c == k)
        def _(own=own):
            load_h(own).start()
    load_w1.start()
    load_w2a.start()
    me.barrier()
    for k, other in ((0, hb), (1, ha)):
        @pl.when(c == k)
        def _(other=other):
            give_h(other).start()
    lacc[...] = jnp.zeros_like(lacc)

    def matmul(src, w, dst, st):
        def step(j, carry):
            res = nn(src[...], w[:, cols(j)])
            dst[:, cols(j)] = res
            st[pl.ds(j, 1)] = jnp.sum(res, axis=0, keepdims=True)
            st[pl.ds(NB + j, 1)] = jnp.sum(res * res, axis=0, keepdims=True)
            return carry
        lax.fori_loop(0, NB, step, 0)

    def norm(u, x, st, layer):
        mean = st[0:NB] * (1.0 / ALL_ROWS)
        var = st[NB:2 * NB] * (1.0 / ALL_ROWS) - mean * mean
        inv = lax.rsqrt(var + BN_EPS)
        st[0:NB] = mean
        st[NB:2 * NB] = inv
        rs[NB * layer:NB * layer + NB] = inv

        def step(j, carry):
            nrm = (u[:, cols(j)] - st[pl.ds(j, 1)]) * st[pl.ds(NB + j, 1)]
            act = gains[layer][:, cols(j)] * nrm + biases[layer][:, cols(j)]
            u[:, cols(j)] = nrm
            x[:, cols(j)] = jnp.maximum(act, 0.0).astype(BF16)
            return carry
        lax.fori_loop(0, NB, step, 0)

    load_w1.wait()
    load_h(ha).wait()
    give_h(ha).wait()
    swap_h.start()
    keep_h.start()
    matmul(hv, w1v, da, f1)
    SmallReduce(me, f1, fl1, fa1, fb1).run()
    norm(da, dzo, f1, 0)
    save_n1.start()
    keep_h.wait()
    swap_h.wait()
    swap_x1.start()
    keep_x1.start()
    load_w2a.wait()
    matmul(dzo, gw, nv, f2)
    load_w3a.start()
    SmallReduce(me, f2, fl2, fa2, fb2).run()
    norm(nv, dz, f2, 1)
    swap_x1.wait()
    swap_x2.start()
    keep_x2.start()
    load_w3a.wait()

    def z_block(j):
        res = nn(dz[...], gw[:, cols(j)]).astype(BF16)
        zd[0:ROWS, cols(j)] = res
        sv[pl.ds(j, 1)] = jnp.sum(res.astype(F32), axis=0, keepdims=True)

    def z_blocks(first):
        def step(j, carry):
            z_block(first + j)
            return carry
        lax.fori_loop(0, 2, step, 0)

    z_blocks(0)
    red0 = SmallReduce(me, sv, sl, sa, sb)
    red2 = SmallReduce(me, s2, l2, sa2, sb2)
    red1 = SmallReduce(me, s1, l1, sa1, sb1)
    sc = Scatter(me, part, (r1, r2, r3, r4), ssem, rsem)

    def compute(u):
        p = lax.rem(u, SLOTS)

        @pl.when(u < GRAM_UNITS)
        def _():
            for k in range(2):
                i, j = block_of(2 * u + k)
                part[p, k] = tn(zd[0:ROWS, cols(i)], zd[0:ROWS, cols(j)])

        w, q = grad_unit(u)
        for w_, la, lb, ra, rb in ((0, x2h, x2o, dz, dzo), (1, x1h, x1o, zd, zod)):
            @pl.when((u >= GRAM_UNITS) & (w == w_))
            def _(la=la, lb=lb, ra=ra, rb=rb):
                lc = pl.ds(pl.multiple_of(lax.rem(q, 2) * 512, 512), 512)
                rc = cols(q // 2)
                res = tn(la[:, lc], ra[0:ROWS, rc]) + tn(lb[:, lc], rb[:, rc])
                part[p, 0] = res[0:BLK]
                part[p, 1] = res[BLK:2 * BLK]

        @pl.when((u >= GRAM_UNITS) & (w == 2))
        def _():
            rc = pl.ds(pl.multiple_of(q * 512, 512), 512)
            res = tn(hh[...], dz[:, rc]) + tn(ho[...], dzo[:, rc])
            part[p, 0] = res[:, 0:BLK]
            part[p, 1] = res[:, BLK:2 * BLK]

    def grad_unit(u):
        v = jnp.maximum(u - GRAM_UNITS, 0)
        return v // 16, lax.rem(v, 16)

    def of_weight(u, w):
        return (u >= GRAM_UNITS) & (grad_unit(u)[0] == w)

    def region(u, w, k, off, n):
        q = grad_unit(u)[1]
        if w == 2:
            r0, c0 = c * 256, q * 512 + k * BLK
        else:
            r0, c0 = c * 1024 + lax.rem(q, 2) * 512 + k * BLK, (q // 2) * BLK
        return rows_at(r0 + off, n), cols_at(c0)

    grads = (g3_o, g2v, g1v)

    def keep_copy(u, k):
        own = region(u, 0, k, me.keep[k][4], 16)
        return pltpu.make_async_copy(stage.at[lax.rem(u, RING), k], g3_o.at[own], lsem.at[k, lax.rem(u, RING)])

    def spread(u, w, s, k):
        r = lax.rem(u, RING)
        dst = grads[w].at[region(u, w, k, me.keep[k][s], BLK >> s)]
        src = stage.at[r, k] if s == 4 and w == 0 else dst
        return rcopy(src, dst, asem.at[s, k, r], bsem.at[s, k, r], me.peers[k][s - 1])

    def cross(u, w):
        r = lax.rem(u, RING)
        q = grad_unit(u)[1]
        buf = grads[w].at[unit_region(q, w, c)]
        return rcopy(buf, buf, asem.at[0, 0, r], bsem.at[0, 0, r], me.pc)

    def unit_region(q, w, core):
        if w == 2:
            return rows_at(core * 256, 256), pl.ds(pl.multiple_of(q * 512, 512), 512)
        return rows_at(core * 1024 + lax.rem(q, 2) * 512, 512), cols(q // 2)

    def put(u, w, own):
        reg = unit_region(grad_unit(u)[1], w, c if own else 1 - c)
        out = (None, g2_o, g1_o)[w]
        return pltpu.make_async_copy(grads[w].at[reg], out.at[reg], psem.at[0 if own else 1, lax.rem(u, RING)])

    def spread_gram(u, s, k):
        i, j = block_of(2 * u + k)
        r = lax.rem(u, RING)
        buf = gw.at[rows_at(i * BLK + me.keep[k][s], BLK >> s), cols(j)]
        return rcopy(buf, buf, gasem.at[s - 1, k, r], gbsem.at[s - 1, k, r], me.peers[k][s - 1])

    def final(u):
        for w in range(3):
            @pl.when(of_weight(u, w))
            def _(w=w):
                for k in range(2):
                    piece = part[lax.rem(u, SLOTS), k, rows_at(me.keep[k][4], 16)]
                    if w == 0:
                        stage[lax.rem(u, RING), k] = piece
                        keep_copy(u, k).start()
                    else:
                        rr, cc = region(u, w, k, me.keep[k][4], 16)
                        grads[w][rr, cc] = piece
                    spread(u, w, 4, k).start()

        @pl.when(u < GRAM_UNITS)
        def _():
            for k in range(2):
                i, j = block_of(2 * u + k)
                own = rows_at(me.keep[k][4], 16)
                row0 = rows_at(i * BLK + me.keep[k][4], 16)
                mu_r = g1v[rows_at(lax.rem(i, 2) * BLK + me.keep[k][4], 16), lanes_at((i // 2) * 128)]
                mu_c = sv[pl.ds(j, 1)]
                mm = ALL_ROWS * jnp.concatenate([mu_r, mu_r], axis=1) * mu_c
                cov = (part[lax.rem(u, SLOTS), k, own] - mm) * (1.0 / (ALL_ROWS - 1))
                row = lax.broadcasted_iota(jnp.int32, (16, BLK), 0) + (i * BLK + me.keep[k][4])
                col = lax.broadcasted_iota(jnp.int32, (16, BLK), 1) + j * BLK
                diag = row == col
                std = jnp.sqrt(jnp.where(diag, cov, 1.0) + STD_EPS)
                hinge = jnp.where(std < 1.0, VAR_WEIGHT / (2.0 * std), 0.0)
                weight = jnp.where(i == j, COV_WEIGHT, 2.0 * COV_WEIGHT)
                term = jnp.where(diag, VAR_WEIGHT * jnp.maximum(1.0 - std, 0.0), weight * cov * cov)
                lacc[...] = lacc[...] + term[0:8] + term[8:16]
                gw[row0, cols(j)] = jnp.where(diag, -hinge, (2.0 * COV_WEIGHT) * cov).astype(BF16)
                spread_gram(u, 4, k).start()

    def diff_block(j):
        diff = zd[0:ROWS, cols(j)].astype(F32) - zod[:, cols(j)].astype(F32)
        sq = jnp.sum((diff * diff).reshape(ROWS // 8, 8, BLK), axis=0)
        lacc[...] = lacc[...] + (0.5 * INV_WEIGHT / ALL_ROWS) * sq
        da[:, cols(j)] = (2.0 * INV_WEIGHT / ALL_ROWS) * diff

    def dz_block(j):
        acc = nn(zd[...], gw[:, cols(j)])
        mean = acc[ROWS:ROWS + 1] + acc[ROWS + 1:ROWS + 2] + acc[ROWS + 2:ROWS + 3]
        dz[:, cols(j)] = (da[:, cols(j)] + (2.0 / (ALL_ROWS - 1)) * (acc[0:ROWS] - mean)).astype(BF16)

    def back_block(j, grad, st, layer):
        dx = nt(grad[0:ROWS, :], gw[cols(j)])
        nrm = nv[:, cols(j)]
        act = gains[layer][:, cols(j)] * nrm + biases[layer][:, cols(j)]
        d_act = jnp.where(act > 0.0, dx, 0.0)
        da[:, cols(j)] = d_act
        st[pl.ds(j, 1)] = jnp.sum(d_act, axis=0, keepdims=True)
        st[pl.ds(NB + j, 1)] = jnp.sum(d_act * nrm, axis=0, keepdims=True)

    def back_pre(dst, st, layer):
        def step(j, carry):
            scale = gains[layer][:, cols(j)] * rs[pl.ds(NB * layer + j, 1)]
            m0 = st[pl.ds(j, 1)] * (1.0 / ALL_ROWS)
            m1 = st[pl.ds(NB + j, 1)] * (1.0 / ALL_ROWS)
            dst[0:ROWS, cols(j)] = (scale * (da[:, cols(j)] - m0 - nv[:, cols(j)] * m1)).astype(BF16)
            return carry
        lax.fori_loop(0, NB, step, 0)

    compute(jnp.int32(0))

    def slot(t, carry):
        u, ok = unit_at(t - 9 * LAG - 1)
        for w in (1, 2):
            @pl.when(ok & of_weight(u, w))
            def _(u=u, w=w):
                put(u, w, False).wait()

        u, ok = unit_at(t - 9 * LAG)
        for w in range(3):
            @pl.when(ok & of_weight(u, w))
            def _(u=u, w=w):
                cross(u, w).wait()
                if w > 0:
                    put(u, w, True).wait()
                    put(u, w, False).start()

        for s in (1, 2, 3, 4):
            u, ok = unit_at(t - LAG * (9 - s))
            for w in range(3):
                @pl.when(ok & of_weight(u, w))
                def _(s=s, u=u, w=w):
                    for k in range(2):
                        cp = spread(u, w, s, k)
                        cp.wait_send()
                        cp.wait_recv()
                        if s == 4 and w == 0:
                            keep_copy(u, k).wait()
                        if s > 1:
                            spread(u, w, s - 1, k).start()
                    if s == 1:
                        cross(u, w).start()
                        if w > 0:
                            put(u, w, True).start()

            @pl.when(ok & (u < GRAM_UNITS))
            def _(s=s, u=u):
                for k in range(2):
                    cp = spread_gram(u, s, k)
                    cp.wait_send()
                    cp.wait_recv()
                    if s > 1:
                        spread_gram(u, s - 1, k).start()
                if s == 1:
                    for k in range(2):
                        i, j = block_of(2 * u + k)

                        @pl.when(i != j)
                        def _():
                            gw[rows_at(j * BLK, BLK), cols(i)] = gw[rows_at(i * BLK, BLK), cols(j)].T

        for first, red in ((3, red0), (PASS_2 + 2, red2), (PASS_1 + 2, red1)):
            for ph in range(2):
                @pl.when(t == first + ph + 1)
                def _(red=red, ph=ph):
                    red.finish(ph)

                @pl.when(t == first + ph)
                def _(red=red, ph=ph):
                    red.start(ph)

        for first, st, layer, dst in ((PASS_2, s2, 1, zd), (PASS_1, s1, 0, dz)):
            @pl.when(t == first + 4)
            def _(st=st, layer=layer, dst=dst):
                back_pre(dst, st, layer)

        @pl.when(t == PASS_2 + 2)
        def _():
            load_w2.start()

        @pl.when(t == PASS_2 + 4)
        def _():
            load_n1.start()
            swap_du2.start()
            swap_s2.start()

        @pl.when(t == PASS_1 + 4)
        def _():
            swap_du1.start()
            swap_s1.start()

        sc.advance(t, final)
        u, ok = unit_at(t)

        @pl.when(ok)
        def _(u=u):
            sc.begin(u)

        @pl.when(t == 5)
        def _():
            mean = sv[...] * (1.0 / ALL_ROWS)
            sv[...] = mean
            hi = mean.astype(BF16)
            mid = (mean - hi.astype(F32)).astype(BF16)
            low = (mean - hi.astype(F32) - mid.astype(F32)).astype(BF16)
            for j in range(NB):
                for h in range(2):
                    lanes = slice(128 * h, 128 * h + 128)
                    r0, c0 = (j % 2) * BLK + 128 * h, (j // 2) * 128
                    g1v[r0:r0 + 128, c0:c0 + 128] = jnp.broadcast_to(mean[j:j + 1, lanes], (128, 128)).T
                zd[ROWS:ROWS + 16, j * BLK:(j + 1) * BLK] = jnp.concatenate(
                    [hi[j:j + 1], mid[j:j + 1], low[j:j + 1], jnp.zeros((13, BLK), BF16)], axis=0)

        @pl.when(t < 3)
        def _():
            z_blocks(2 * t + 2)

        @pl.when(t == 3)
        def _():
            keep_x1.wait()
            keep_x2.wait()
            swap_x2.wait()
            save_n1.wait()
            swap_z.start()

        @pl.when(t == 7)
        def _():
            swap_z.wait()

        @pl.when((t >= 8) & (t < 8 + NB))
        def _():
            diff_block(t - 8)

        for j, first in enumerate(DZ_SLOTS):
            @pl.when(t == first + 1)
            def _(j=j):
                swap_dz(j).wait()

        mine_now = jnp.int32(-1)
        for j, first in enumerate(DZ_SLOTS):
            mine_now = jnp.where(t == first, j, mine_now)

        @pl.when(mine_now >= 0)
        def _():
            dz_block(mine_now)
            swap_dz(mine_now).start()

        @pl.when(t == DZ_SLOTS[-1])
        def _():
            load_w3.start()

        @pl.when(t == PASS_2)
        def _():
            s2[2 * NB:3 * NB] = lacc[...]
            load_w3.wait()

        @pl.when(t == PASS_1)
        def _():
            load_w2.wait()
            load_n1.wait()

        @pl.when(t == START_2 - 1)
        def _():
            swap_du2.wait()

        @pl.when(t == START_2 + 14)
        def _():
            swap_du1.wait()

        for first, grad, st, layer in ((PASS_2, dz, s2, 1), (PASS_1, zd, s1, 0)):
            @pl.when((t >= first) & (t < first + 2))
            def _(first=first, grad=grad, st=st, layer=layer):
                def step(j, carry):
                    back_block(j, grad, st, layer)
                    return carry
                lo = 4 * (t - first)
                lax.fori_loop(lo, lo + 4, step, 0)

        u, ok = unit_at(t + 1)

        @pl.when(ok)
        def _(u=u):
            compute(u)
        return carry
    lax.fori_loop(0, END, slot, 0)
    swap_s2.wait()
    swap_s1.wait()
    sum2, sum1 = s2[...] + e2[...], s1[...] + e1[...]
    for j in range(NB):
        lanes = slice(j * BLK, (j + 1) * BLK)
        st_o[0:1, lanes] = sum1[NB + j:NB + j + 1]
        st_o[1:2, lanes] = sum1[j:j + 1]
        st_o[2:3, lanes] = sum2[NB + j:NB + j + 1]
        st_o[3:4, lanes] = sum2[j:j + 1]
    total = jnp.sum(jnp.sum(sum2[2 * NB:], axis=0, keepdims=True), axis=1, keepdims=True)
    st_o[4:5, 0:128] = jnp.broadcast_to(total, (1, 128))


def train_step(ha, hb, w1, w2, w3, g1, b1, g2, b2):
    act = pltpu.VMEM((ROWS, DIM), BF16)
    piece = pltpu.VMEM((ROWS, 1024), BF16)
    dma = pltpu.SemaphoreType.DMA
    return pl.pallas_call(
        step_kernel,
        out_shape=(sds((DIM, DIM), F32), sds((DIM, DIM), F32), sds((FEAT, DIM), F32), sds((ROWS, DIM), F32),
                   sds((8, DIM), F32)),
        in_specs=[ANY] * 5 + [INV] * 4,
        out_specs=(ANY, ANY, ANY, ANY, INV),
        scratch_shapes=[pltpu.VMEM((ROWS + 16, DIM), BF16), act, act, act, pltpu.VMEM((DIM, DIM), BF16),
                        piece, piece, piece, piece, pltpu.VMEM((ROWS, 256), BF16), pltpu.VMEM((ROWS, 256), BF16),
                        pltpu.VMEM((DIM, DIM), F32), pltpu.VMEM((FEAT, DIM), F32),
                        pltpu.VMEM((NB, BLK), F32), pltpu.VMEM((2 * NB, BLK), F32),
                        pltpu.VMEM((RING, 2, 16, BLK), F32)]
        + scatter_scratch(SLOTS) + small_scratch(NB) + small_scratch(2 * NB) + small_scratch(2 * NB)
        + small_scratch(3 * NB) + small_scratch(2 * NB)
        + [pltpu.VMEM((3 * NB, BLK), F32), pltpu.VMEM((2 * NB, BLK), F32),
           dma((4, 2, RING)), dma((4, 2, RING)), dma((5, 2, RING)), dma((5, 2, RING)), dma((2, RING)),
           dma((2, RING)), dma((10,)), dma((17,)), dma((17,))],
        compiler_params=pltpu.CompilerParams(collective_id=0, has_side_effects=True, vmem_limit_bytes=VMEM_LIMIT),
        name='train_step',
    )(ha, hb, w1, w2, w3, g1, b1, g2, b2)


def solution(mesh):
    def local_step(h_a, h_b, w_one, w_two, w_three, gain_one, bias_one, gain_two, bias_two):
        vecs = [v.reshape(1, DIM) for v in (gain_one, bias_one, gain_two, bias_two)]
        d_three, d_two, d_one, _, st = train_step(h_a, h_b, w_one, w_two, w_three, *vecs)
        return st[4, 0], d_one, d_two, d_three, st[0], st[1], st[2], st[3]

    row_spec = P('data', None)
    return jax.shard_map(local_step, mesh=mesh,
                         in_specs=(row_spec, row_spec, P(), P(), P(), P(), P(), P(), P()),
                         out_specs=(P(), P(), P(), P(), P(), P(), P(), P()),
                         check_vma=False)
```

```python
import functools

import jax
import jax.numpy as jnp
from jax import lax
from jax.experimental import pallas as pl
from jax.experimental.pallas import tpu as pltpu
from jax.sharding import PartitionSpec as P

BN_EPS = 1e-5
STD_EPS = 1e-4
INV_WEIGHT = 2.0
VAR_WEIGHT = 1.0
COV_WEIGHT = 2.0

F32 = jnp.float32
BF16 = jnp.bfloat16
MESH = pl.DeviceIdType.MESH
VMEM_LIMIT = 67043328

ROWS = 1024
HALF = 512
FEAT = 512
DIM = 2048
NB = 8
BLK = 256
LAG = 2
RING = 6
ALL_ROWS = 16384


def sds(shape, dtype):
    return jax.ShapeDtypeStruct(shape, dtype)


ANY = pl.BlockSpec(memory_space=pl.ANY)
INV = pl.BlockSpec(memory_space=pltpu.VMEM)


class Place:
    def __init__(self):
        i = lax.axis_index('data')
        self.c = lax.rem(i, 2)
        x = lax.rem(i // 2, 2)
        y = lax.rem(i // 4, 2)
        z = i // 8
        zl = lax.rem(z, 2)
        zh = z // 2
        self.pc = i + 1 - 2 * self.c
        px = i + 2 - 4 * x
        py = i + 4 - 8 * y
        p1 = i + 8 - 16 * zl
        p2 = i + 16 - 32 * zh
        pd = px + py - i
        p3 = p1 + p2 - i
        self.phases = ((px, py, pd), (p1, p2, p3))
        self.end = zl == zh
        self.p1, self.p3 = p1, p3
        self.first, self.last = (px, py), (py, px)
        self.keep = [b * 128 for b in (x, y)]
        self.send = [(1 - b) * 128 for b in (x, y)]
        self.near = [k + zh * 64 for k in self.keep]
        self.far = [k + (1 - zh) * 64 for k in self.keep]
        self.own = [n + b * 32 for n, b in zip(self.near, (y, x))]
        self.give = [n + (1 - b) * 32 for n, b in zip(self.near, (y, x))]

    def barrier(self):
        sem = pltpu.get_barrier_semaphore()
        for p in (self.pc,) + self.phases[0] + self.phases[1]:
            pl.semaphore_signal(sem, inc=1, device_id=(p,), device_id_type=MESH)
        pl.semaphore_wait(sem, 7)


def rcopy(src, dst, ssem, rsem, dev):
    return pltpu.make_async_remote_copy(src_ref=src, dst_ref=dst, send_sem=ssem, recv_sem=rsem,
                                        device_id=(dev,), device_id_type=MESH)


def rows_at(off, n):
    return pl.ds(pl.multiple_of(off, n), n)


def nn(a, b):
    return jnp.dot(a, b, preferred_element_type=F32)


def nt(a, b):
    return lax.dot_general(a, b, (((1,), (1,)), ((), ())), preferred_element_type=F32)


def tn(a, b):
    return lax.dot_general(a, b, (((0,), (0,)), ((), ())), preferred_element_type=F32)


def lanes_at(off):
    return pl.ds(pl.multiple_of(off, 128), 128)


def cols_at(off):
    return pl.ds(pl.multiple_of(off, BLK), BLK)


def cols(j):
    return pl.ds(pl.multiple_of(j * BLK, BLK), BLK)


class Scatter:
    def __init__(self, place, part, lands, ssem, rsem):
        self.pl, self.part, self.ssem, self.rsem = place, part, ssem, rsem
        self.lands = (lands[0], lands[1], lands[2], lands[1], lands[3])

    def copy(self, u, e, k):
        me = self.pl
        off, n, dev = ((me.send[k], 128, me.first[k]), (me.far[k], 64, me.p1), (me.far[k], 64, me.p3),
                       (me.near[k], 64, me.p1), (me.give[k], 32, me.last[k]))[e]
        land, r = self.lands[e], lax.rem(u, RING)
        return rcopy(self.part.at[lax.rem(u, SLOTS), k, rows_at(off, n)],
                     land.at[lax.rem(u, land.shape[0]), k], self.ssem.at[e, k, r], self.rsem.at[e, k, r], dev)

    def start(self, u, e):
        for k in range(2):
            self.copy(u, e, k).start()

    def sent(self, u, e):
        for k in range(2):
            self.copy(u, e, k).wait_send()

    def add(self, u, e, off):
        p, n = lax.rem(u, SLOTS), (128, 64, 64, 64, 32)[e]
        land = self.lands[e]
        for k in range(2):
            self.copy(u, e, k).wait_recv()
            rr = rows_at(off[k], n)
            self.part[p, k, rr] = self.part[p, k, rr] + land[lax.rem(u, land.shape[0]), k]

    def advance(self, t, final):
        me = self.pl
        u5, ok5 = unit_at(t - 5 * LAG)
        u4, ok4 = unit_at(t - 4 * LAG)
        u3, ok3 = unit_at(t - 3 * LAG)
        u2, ok2 = unit_at(t - 2 * LAG)
        u1, ok1 = unit_at(t - LAG)
        inner = jnp.logical_not(me.end)

        @pl.when(ok5 & me.end)
        def _():
            self.sent(u5, 4)
            self.add(u5, 4, me.own)
            final(u5)

        @pl.when(ok4 & me.end)
        def _():
            self.add(u4, 3, me.near)
            self.start(u4, 4)

        @pl.when(ok4 & inner)
        def _():
            self.sent(u4, 3)

        @pl.when(ok3 & inner)
        def _():
            self.sent(u3, 2)
            self.add(u3, 2, me.near)
            self.start(u3, 3)

        @pl.when(ok2 & inner)
        def _():
            self.add(u2, 1, me.far)
            self.start(u2, 2)

        @pl.when(ok2 & me.end)
        def _():
            self.sent(u2, 1)

        @pl.when(ok1)
        def _():
            self.sent(u1, 0)
            self.add(u1, 0, me.keep)

        @pl.when(ok1 & me.end)
        def _():
            self.start(u1, 1)


def scatter_scratch(slots):
    return [pltpu.VMEM((slots, 2, BLK, BLK), F32), pltpu.VMEM((4, 2, 128, BLK), F32),
            pltpu.VMEM((6, 2, 64, BLK), F32), pltpu.VMEM((4, 2, 64, BLK), F32), pltpu.VMEM((4, 2, 32, BLK), F32),
            pltpu.SemaphoreType.DMA((5, 2, RING)), pltpu.SemaphoreType.DMA((5, 2, RING))]


class SmallReduce:
    def __init__(self, place, val, land, ssem, rsem):
        self.pl, self.val, self.land, self.ssem, self.rsem = place, val, land, ssem, rsem

    def copies(self, ph):
        return [rcopy(self.val, self.land.at[ph, k], self.ssem.at[ph, k], self.rsem.at[ph, k], p)
                for k, p in enumerate(self.pl.phases[ph])]

    def start(self, ph):
        for cp in self.copies(ph):
            cp.start()

    def finish(self, ph):
        for cp in self.copies(ph):
            cp.wait()
        self.val[...] = (self.val[...] + self.land[ph, 0]) + (self.land[ph, 1] + self.land[ph, 2])

    def run(self):
        for ph in range(2):
            self.start(ph)
            self.finish(ph)


def small_scratch(n):
    return [pltpu.VMEM((n, BLK), F32), pltpu.VMEM((2, 3, n, BLK), F32),
            pltpu.SemaphoreType.DMA((2, 3)), pltpu.SemaphoreType.DMA((2, 3))]


GRAM_UNITS = 18
GRAM = 3
UNITS = 54
SLOTS = 5 * LAG + 1
START_3 = 28
START_2 = 44
END = START_2 + 21 + 11 * LAG
DZ_SLOTS = (23, 27, 30, 32, 34, 36, 37, 38)
PASS_2 = 39
PASS_1 = 45
SPAN_2, SPAN_1 = 3, 4


def block_of(q):
    i = jnp.int32(0)
    for first in (8, 15, 21, 26, 30, 33, 35):
        i = i + jnp.where(q >= first, 1, 0)
    return i, i + q - (17 * i - i * i) // 2


def unit_at(t):
    u = jnp.where(t < START_3, t, jnp.where(t < START_2, t - (START_3 - 18), t - (START_2 - 34)))
    ok = ((t >= 0) & (t < 18)) | ((t >= START_3) & (t < START_3 + 16)) | ((t >= START_2) & (t < START_2 + 20))
    return jnp.where(ok, u, 0), ok


def step_kernel(ha, hb, w1, w2, w3, g1, b1, g2, b2, g3_o, g2_o, g1_o, n1_o, h_o, ho_o, st_o,
                zd, zod, dz, dzo, gw, x2h, x2o, x1h, x1o, g2v, g1v, lacc, rs, stage,
                part, r1, r2, r3, r4, ssem, rsem, sv, sl, sa, sb, f1, fl1, fa1, fb1, f2, fl2, fa2, fb2,
                s2, l2, sa2, sb2, s1, l1, sa1, sb1, e2, e1,
                asem, bsem, lsem, psem, csem, dsem, esem, wsem):
    me = Place()
    c = me.c
    nv, da = g2v.at[pl.ds(0, ROWS)], g2v.at[pl.ds(ROWS, ROWS)]
    hv = x2o.at[:, pl.ds(0, FEAT)]
    gains, biases = (g1, g2), (b1, b2)
    half = pl.ds(pl.multiple_of(c * 1024, 1024), 1024)
    ohalf = pl.ds(pl.multiple_of((1 - c) * 1024, 1024), 1024)
    hhalf = pl.ds(pl.multiple_of(c * 256, 256), 256)
    hohalf = pl.ds(pl.multiple_of((1 - c) * 256, 256), 256)
    mine = pl.ds(pl.multiple_of(c * HALF, HALF), HALF)
    body = pl.ds(0, ROWS)
    w1v = zod.at[pl.ds(0, FEAT)]
    load_w1 = pltpu.make_async_copy(w1, w1v, csem.at[0])
    load_w2a = pltpu.make_async_copy(w2, gw, csem.at[1])
    load_w3a = pltpu.make_async_copy(w3, gw, csem.at[2])
    load_w2 = pltpu.make_async_copy(w2, gw, csem.at[6])
    load_n1 = pltpu.make_async_copy(n1_o, nv, csem.at[7])
    save_n1 = pltpu.make_async_copy(da, n1_o, csem.at[8])
    keep_x1 = pltpu.make_async_copy(dzo.at[:, half], x1h, csem.at[3])
    keep_h = pltpu.make_async_copy(hv.at[:, hhalf], h_o, csem.at[5])
    hh, ho = x2h.at[:, pl.ds(0, 256)], x2o.at[:, pl.ds(0, 256)]
    load_h2 = [pltpu.make_async_copy(h_o, hh, csem.at[5]), pltpu.make_async_copy(ho_o, ho, csem.at[2])]
    keep_x2 = pltpu.make_async_copy(dz.at[:, half], x2h, csem.at[4])
    swap_z = rcopy(zd.at[body], zod, dsem.at[0], esem.at[0], me.pc)
    swap_x2 = rcopy(dz.at[:, ohalf], x2o, dsem.at[1], esem.at[1], me.pc)
    swap_x1 = rcopy(dzo.at[:, ohalf], x1o, dsem.at[2], esem.at[2], me.pc)
    swap_h = rcopy(hv.at[:, hohalf], ho_o, dsem.at[3], esem.at[3], me.pc)
    swap_du1 = rcopy(dz, dzo, dsem.at[5], esem.at[5], me.pc)
    swap_s2 = rcopy(s2, e2, dsem.at[6], esem.at[6], me.pc)
    swap_s1 = rcopy(s1, e1, dsem.at[7], esem.at[7], me.pc)

    def load_h(src):
        return pltpu.make_async_copy(src, hv.at[mine], csem.at[9])

    def give_h(src):
        return rcopy(src, hv.at[mine], dsem.at[16], esem.at[16], me.pc)

    def load_w3(j):
        return pltpu.make_async_copy(w3.at[cols(j)], gw.at[cols(j)], wsem.at[j])

    def swap_du2(j):
        return rcopy(zd.at[body, cols(j)], zod.at[:, cols(j)], dsem.at[17 + j], esem.at[17 + j], me.pc)

    def swap_dz(j):
        return rcopy(dz.at[:, cols(j)], dzo.at[:, cols(j)], dsem.at[8 + j], esem.at[8 + j], me.pc)

    for k, own in ((0, ha), (1, hb)):
        @pl.when(c == k)
        def _(own=own):
            load_h(own).start()
    load_w1.start()
    load_w2a.start()
    me.barrier()
    for k, other in ((0, hb), (1, ha)):
        @pl.when(c == k)
        def _(other=other):
            give_h(other).start()
    lacc[...] = jnp.zeros_like(lacc)

    def matmul(src, w, dst, st):
        def step(j, carry):
            res = nn(src[...], w[:, cols(j)])
            dst[:, cols(j)] = res
            st[pl.ds(j, 1)] = jnp.sum(res, axis=0, keepdims=True)
            st[pl.ds(NB + j, 1)] = jnp.sum(res * res, axis=0, keepdims=True)
            return carry
        lax.fori_loop(0, NB, step, 0)

    def norm(u, x, st, layer):
        mean = st[0:NB] * (1.0 / ALL_ROWS)
        var = st[NB:2 * NB] * (1.0 / ALL_ROWS) - mean * mean
        inv = lax.rsqrt(var + BN_EPS)
        st[0:NB] = mean
        st[NB:2 * NB] = inv
        rs[NB * layer:NB * layer + NB] = inv

        def step(j, carry):
            nrm = (u[:, cols(j)] - st[pl.ds(j, 1)]) * st[pl.ds(NB + j, 1)]
            act = gains[layer][:, cols(j)] * nrm + biases[layer][:, cols(j)]
            u[:, cols(j)] = nrm
            x[:, cols(j)] = jnp.maximum(act, 0.0).astype(BF16)
            return carry
        lax.fori_loop(0, NB, step, 0)

    load_w1.wait()
    load_h(ha).wait()
    give_h(ha).wait()
    swap_h.start()
    keep_h.start()
    matmul(hv, w1v, da, f1)
    SmallReduce(me, f1, fl1, fa1, fb1).run()
    norm(da, dzo, f1, 0)
    save_n1.start()
    keep_h.wait()
    swap_h.wait()
    swap_x1.start()
    keep_x1.start()
    load_w2a.wait()
    matmul(dzo, gw, nv, f2)
    load_w3a.start()
    SmallReduce(me, f2, fl2, fa2, fb2).run()
    norm(nv, dz, f2, 1)
    swap_x1.wait()
    swap_x2.start()
    keep_x2.start()
    load_w3a.wait()

    def z_block(j):
        res = nn(dz[...], gw[:, cols(j)]).astype(BF16)
        zd[0:ROWS, cols(j)] = res
        sv[pl.ds(j, 1)] = jnp.sum(res.astype(F32), axis=0, keepdims=True)

    def z_blocks(first):
        def step(j, carry):
            z_block(first + j)
            return carry
        lax.fori_loop(0, 2, step, 0)

    z_blocks(0)
    red0 = SmallReduce(me, sv, sl, sa, sb)
    red2 = SmallReduce(me, s2, l2, sa2, sb2)
    red1 = SmallReduce(me, s1, l1, sa1, sb1)
    sc = Scatter(me, part, (r1, r2, r3, r4), ssem, rsem)

    def compute(u):
        p = lax.rem(u, SLOTS)

        @pl.when(u < GRAM_UNITS)
        def _():
            for k in range(2):
                i, j = block_of(2 * u + k)
                part[p, k] = tn(zd[0:ROWS, cols(i)], zd[0:ROWS, cols(j)])

        w, q = grad_unit(u)
        for w_, la, lb, ra, rb in ((0, x2h, x2o, dz, dzo), (1, x1h, x1o, zd, zod)):
            @pl.when((u >= GRAM_UNITS) & (w == w_))
            def _(la=la, lb=lb, ra=ra, rb=rb):
                lc = pl.ds(pl.multiple_of(lax.rem(q, 2) * 512, 512), 512)
                rc = cols(q // 2)
                res = tn(la[:, lc], ra[0:ROWS, rc]) + tn(lb[:, lc], rb[:, rc])
                part[p, 0] = res[0:BLK]
                part[p, 1] = res[BLK:2 * BLK]

        @pl.when((u >= GRAM_UNITS) & (w == 2))
        def _():
            rc = pl.ds(pl.multiple_of(q * 512, 512), 512)
            res = tn(hh[...], dz[:, rc]) + tn(ho[...], dzo[:, rc])
            part[p, 0] = res[:, 0:BLK]
            part[p, 1] = res[:, BLK:2 * BLK]

    def grad_unit(u):
        v = jnp.maximum(u - GRAM_UNITS, 0)
        return v // 16, lax.rem(v, 16)

    def of_weight(u, w):
        if w == GRAM:
            return u < GRAM_UNITS
        return (u >= GRAM_UNITS) & (grad_unit(u)[0] == w)

    def region(u, w, k, off, n):
        q = grad_unit(u)[1]
        if w == 2:
            r0, c0 = c * 256, q * 512 + k * BLK
        else:
            r0, c0 = c * 1024 + lax.rem(q, 2) * 512 + k * BLK, (q // 2) * BLK
        return rows_at(r0 + off, n), cols_at(c0)

    grads = (g3_o, g2v, g1v)

    def keep_copy(u, k):
        own = region(u, 0, k, me.own[k], 32)
        return pltpu.make_async_copy(stage.at[lax.rem(u, 4), k], g3_o.at[own], lsem.at[k, lax.rem(u, RING)])

    def hop(e, k):
        return ((me.own[k], 32, me.last[k]), (me.near[k], 64, me.p1), (me.near[k], 64, me.p3),
                (me.far[k], 64, me.p1), (me.keep[k], 128, me.first[k]))[e]

    def spread(u, w, e, k):
        r = lax.rem(u, RING)
        off, n, dev = hop(e, k)
        if w == GRAM:
            i, j = block_of(2 * u + k)
            src = dst = gw.at[rows_at(i * BLK + off, n), cols(j)]
        else:
            dst = grads[w].at[region(u, w, k, off, n)]
            src = stage.at[lax.rem(u, 4), k] if e == 0 and w == 0 else dst
        g = 0 if w == GRAM else 1
        return rcopy(src, dst, asem.at[g, e, k, r], bsem.at[g, e, k, r], dev)

    def cross(u, w):
        r = lax.rem(u, RING)
        q = grad_unit(u)[1]
        buf = grads[w].at[unit_region(q, w, c)]
        return rcopy(buf, buf, asem.at[1, 5, 0, r], bsem.at[1, 5, 0, r], me.pc)

    def unit_region(q, w, core):
        if w == 2:
            return rows_at(core * 256, 256), pl.ds(pl.multiple_of(q * 512, 512), 512)
        return rows_at(core * 1024 + lax.rem(q, 2) * 512, 512), cols(q // 2)

    def put(u, w, own):
        reg = unit_region(grad_unit(u)[1], w, c if own else 1 - c)
        out = (None, g2_o, g1_o)[w]
        return pltpu.make_async_copy(grads[w].at[reg], out.at[reg], psem.at[0 if own else 1, lax.rem(u, RING)])

    def final(u):
        for w in range(3):
            @pl.when(of_weight(u, w))
            def _(w=w):
                for k in range(2):
                    piece = part[lax.rem(u, SLOTS), k, rows_at(me.own[k], 32)]
                    if w == 0:
                        stage[lax.rem(u, 4), k] = piece
                        keep_copy(u, k).start()
                    else:
                        rr, cc = region(u, w, k, me.own[k], 32)
                        grads[w][rr, cc] = piece
                    spread(u, w, 0, k).start()

        @pl.when(u < GRAM_UNITS)
        def _():
            for k in range(2):
                i, j = block_of(2 * u + k)
                own = rows_at(me.own[k], 32)
                row0 = rows_at(i * BLK + me.own[k], 32)
                mu_r = g1v[rows_at(lax.rem(i, 2) * BLK + me.own[k], 32), lanes_at((i // 2) * 128)]
                mu_c = sv[pl.ds(j, 1)]
                mm = ALL_ROWS * jnp.concatenate([mu_r, mu_r], axis=1) * mu_c
                cov = (part[lax.rem(u, SLOTS), k, own] - mm) * (1.0 / (ALL_ROWS - 1))
                row = lax.broadcasted_iota(jnp.int32, (32, BLK), 0) + (i * BLK + me.own[k])
                col = lax.broadcasted_iota(jnp.int32, (32, BLK), 1) + j * BLK
                diag = row == col
                std = jnp.sqrt(jnp.where(diag, cov, 1.0) + STD_EPS)
                hinge = jnp.where(std < 1.0, VAR_WEIGHT / (2.0 * std), 0.0)
                weight = jnp.where(i == j, COV_WEIGHT, 2.0 * COV_WEIGHT)
                term = jnp.where(diag, VAR_WEIGHT * jnp.maximum(1.0 - std, 0.0), weight * cov * cov)
                lacc[...] = lacc[...] + ((term[0:8] + term[8:16]) + (term[16:24] + term[24:32]))
                gw[row0, cols(j)] = jnp.where(diag, -hinge, (2.0 * COV_WEIGHT) * cov).astype(BF16)
                spread(u, GRAM, 0, k).start()

    def diff_block(j):
        diff = zd[0:ROWS, cols(j)].astype(F32) - zod[:, cols(j)].astype(F32)
        sq = jnp.sum((diff * diff).reshape(ROWS // 8, 8, BLK), axis=0)
        lacc[...] = lacc[...] + (0.5 * INV_WEIGHT / ALL_ROWS) * sq
        da[:, cols(j)] = (2.0 * INV_WEIGHT / ALL_ROWS) * diff

    def dz_block(j):
        acc = nn(zd[...], gw[:, cols(j)])
        mean = acc[ROWS:ROWS + 1] + acc[ROWS + 1:ROWS + 2] + acc[ROWS + 2:ROWS + 3]
        dz[:, cols(j)] = (da[:, cols(j)] + (2.0 / (ALL_ROWS - 1)) * (acc[0:ROWS] - mean)).astype(BF16)

    def back_block(j, grad, st, layer):
        dx = nt(grad[0:ROWS, :], gw[cols(j)])
        nrm = nv[:, cols(j)]
        act = gains[layer][:, cols(j)] * nrm + biases[layer][:, cols(j)]
        d_act = jnp.where(act > 0.0, dx, 0.0)
        da[:, cols(j)] = d_act
        st[pl.ds(j, 1)] = jnp.sum(d_act, axis=0, keepdims=True)
        st[pl.ds(NB + j, 1)] = jnp.sum(d_act * nrm, axis=0, keepdims=True)

    def back_pre(dst, st, layer, after):
        def step(j, carry):
            scale = gains[layer][:, cols(j)] * rs[pl.ds(NB * layer + j, 1)]
            m0 = st[pl.ds(j, 1)] * (1.0 / ALL_ROWS)
            m1 = st[pl.ds(NB + j, 1)] * (1.0 / ALL_ROWS)
            dst[0:ROWS, cols(j)] = (scale * (da[:, cols(j)] - m0 - nv[:, cols(j)] * m1)).astype(BF16)
            after(j)
            return carry
        lax.fori_loop(0, NB, step, 0)

    def gather_step(e, u, w):
        def each(f):
            for k in range(2):
                f(k)

        def wait_send(k):
            spread(u, w, e - 1, k).wait_send()

        def wait_recv(k):
            spread(u, w, e - 1, k).wait_recv()

        def begin(k):
            spread(u, w, e, k).start()

        def at_end():
            if e == 1 and w == 0:
                each(lambda k: keep_copy(u, k).wait())
            if e in (1, 2, 5):
                each(wait_send)
            if e in (1, 4, 5):
                each(wait_recv)
            if e in (1, 4):
                each(begin)

        def at_inner():
            if e in (3, 4, 5):
                each(wait_send)
            if e in (2, 3, 5):
                each(wait_recv)
            if e in (2, 3, 4):
                each(begin)

        if e == 5:
            at_end()
        else:
            pl.when(me.end)(at_end)
            if e > 1:
                pl.when(jnp.logical_not(me.end))(at_inner)
        if e == 5 and w < 3:
            cross(u, w).start()
            if w > 0:
                put(u, w, True).start()
        if e == 5 and w == GRAM:
            for k in range(2):
                i, j = block_of(2 * u + k)

                @pl.when(i != j)
                def _():
                    gw[rows_at(j * BLK, BLK), cols(i)] = gw[rows_at(i * BLK, BLK), cols(j)].T

    compute(jnp.int32(0))

    def slot(t, carry):
        u, ok = unit_at(t - 11 * LAG - 1)
        for w in (1, 2):
            @pl.when(ok & of_weight(u, w))
            def _(u=u, w=w):
                put(u, w, False).wait()

        u, ok = unit_at(t - 11 * LAG)
        for w in range(3):
            @pl.when(ok & of_weight(u, w))
            def _(u=u, w=w):
                cross(u, w).wait()
                if w > 0:
                    put(u, w, True).wait()
                    put(u, w, False).start()

        for e in (5, 4, 3, 2, 1):
            u, ok = unit_at(t - (5 + e) * LAG)
            for w in range(4):
                @pl.when(ok & of_weight(u, w))
                def _(e=e, u=u, w=w):
                    gather_step(e, u, w)

        for first, red in ((2, red0), (PASS_2 + SPAN_2 - 1, red2), (PASS_1 + SPAN_1 - 1, red1)):
            @pl.when(t == first + 1)
            def _(red=red):
                red.finish(0)
                red.start(1)

            @pl.when(t == first + 2)
            def _(red=red):
                red.finish(1)

        for first, st, layer, dst in ((PASS_2 + SPAN_2 + 1, s2, 1, zd), (PASS_1 + SPAN_1 + 1, s1, 0, dz)):
            @pl.when(t == first)
            def _(st=st, layer=layer, dst=dst):
                back_pre(dst, st, layer, (lambda j: swap_du2(j).start()) if layer == 1 else (lambda j: None))

        @pl.when(t == PASS_2 + SPAN_2)
        def _():
            load_w2.start()

        @pl.when(t == PASS_2 + SPAN_2 + 1)
        def _():
            load_n1.start()
            swap_s2.start()

        @pl.when(t == PASS_1 + SPAN_1 + 1)
        def _():
            swap_du1.start()
            swap_s1.start()

        sc.advance(t, final)
        u, ok = unit_at(t)

        @pl.when(ok)
        def _(u=u):
            sc.start(u, 0)

        @pl.when(t == 4)
        def _():
            mean = sv[...] * (1.0 / ALL_ROWS)
            sv[...] = mean
            hi = mean.astype(BF16)
            mid = (mean - hi.astype(F32)).astype(BF16)
            low = (mean - hi.astype(F32) - mid.astype(F32)).astype(BF16)
            for j in range(NB):
                for h in range(2):
                    lanes = slice(128 * h, 128 * h + 128)
                    r0, c0 = (j % 2) * BLK + 128 * h, (j // 2) * 128
                    g1v[r0:r0 + 128, c0:c0 + 128] = jnp.broadcast_to(mean[j:j + 1, lanes], (128, 128)).T
                zd[ROWS:ROWS + 16, j * BLK:(j + 1) * BLK] = jnp.concatenate(
                    [hi[j:j + 1], mid[j:j + 1], low[j:j + 1], jnp.zeros((13, BLK), BF16)], axis=0)

        @pl.when(t < 3)
        def _():
            z_blocks(2 * t + 2)

        @pl.when(t == 3)
        def _():
            keep_x1.wait()
            keep_x2.wait()
            swap_x2.wait()
            save_n1.wait()
            swap_z.start()

        @pl.when(t == 7)
        def _():
            swap_z.wait()

        @pl.when((t >= 8) & (t < 8 + NB))
        def _():
            diff_block(t - 8)

        for j, first in enumerate(DZ_SLOTS):
            @pl.when(t == first + 1)
            def _(j=j):
                swap_dz(j).wait()

        mine_now = jnp.int32(-1)
        for j, first in enumerate(DZ_SLOTS):
            mine_now = jnp.where(t == first, j, mine_now)

        @pl.when(mine_now >= 0)
        def _():
            dz_block(mine_now)
            swap_dz(mine_now).start()

        @pl.when(t == DZ_SLOTS[-1])
        def _():
            for j in range(NB):
                load_w3(j).start()

        @pl.when(t == PASS_2)
        def _():
            s2[2 * NB:3 * NB] = lacc[...]

        @pl.when(t == PASS_1)
        def _():
            load_w2.wait()
            load_n1.wait()

        block = (t - (START_2 - 1)) // 2

        @pl.when((t >= START_2 - 1) & (t < START_2 + 15) & (t == START_2 - 1 + 2 * block))
        def _():
            swap_du2(block).wait()

        @pl.when(t == START_2 + 8)
        def _():
            for cp in load_h2:
                cp.start()

        @pl.when(t == START_2 + 14)
        def _():
            swap_du1.wait()
            for cp in load_h2:
                cp.wait()

        for first, span, grad, st, layer in ((PASS_2, SPAN_2, dz, s2, 1), (PASS_1, SPAN_1, zd, s1, 0)):
            @pl.when((t >= first) & (t < first + span))
            def _(first=first, n=-(-NB // span), grad=grad, st=st, layer=layer):
                def step(j, carry):
                    if layer == 1:
                        load_w3(j).wait()
                    back_block(j, grad, st, layer)
                    return carry
                lo = n * (t - first)
                lax.fori_loop(lo, jnp.minimum(lo + n, NB), step, 0)

        for last, red in ((2, red0), (PASS_2 + SPAN_2 - 1, red2), (PASS_1 + SPAN_1 - 1, red1)):
            @pl.when(t == last)
            def _(red=red):
                red.start(0)

        u, ok = unit_at(t + 1)

        @pl.when(ok)
        def _(u=u):
            compute(u)
        return carry
    lax.fori_loop(0, END, slot, 0)
    swap_s2.wait()
    swap_s1.wait()
    sum2, sum1 = s2[...] + e2[...], s1[...] + e1[...]
    for j in range(NB):
        lanes = slice(j * BLK, (j + 1) * BLK)
        st_o[0:1, lanes] = sum1[NB + j:NB + j + 1]
        st_o[1:2, lanes] = sum1[j:j + 1]
        st_o[2:3, lanes] = sum2[NB + j:NB + j + 1]
        st_o[3:4, lanes] = sum2[j:j + 1]
    total = jnp.sum(jnp.sum(sum2[2 * NB:], axis=0, keepdims=True), axis=1, keepdims=True)
    st_o[4:5, 0:128] = jnp.broadcast_to(total, (1, 128))


def train_step(ha, hb, w1, w2, w3, g1, b1, g2, b2):
    act = pltpu.VMEM((ROWS, DIM), BF16)
    piece = pltpu.VMEM((ROWS, 1024), BF16)
    dma = pltpu.SemaphoreType.DMA
    return pl.pallas_call(
        step_kernel,
        out_shape=(sds((DIM, DIM), F32), sds((DIM, DIM), F32), sds((FEAT, DIM), F32), sds((ROWS, DIM), F32),
                   sds((ROWS, 256), BF16), sds((ROWS, 256), BF16), sds((8, DIM), F32)),
        in_specs=[ANY] * 5 + [INV] * 4,
        out_specs=(ANY,) * 6 + (INV,),
        scratch_shapes=[pltpu.VMEM((ROWS + 16, DIM), BF16), act, act, act, pltpu.VMEM((DIM, DIM), BF16),
                        piece, piece, piece, piece,
                        pltpu.VMEM((DIM, DIM), F32), pltpu.VMEM((FEAT, DIM), F32),
                        pltpu.VMEM((NB, BLK), F32), pltpu.VMEM((2 * NB, BLK), F32),
                        pltpu.VMEM((4, 2, 32, BLK), F32)]
        + scatter_scratch(SLOTS) + small_scratch(NB) + small_scratch(2 * NB) + small_scratch(2 * NB)
        + small_scratch(3 * NB) + small_scratch(2 * NB)
        + [pltpu.VMEM((3 * NB, BLK), F32), pltpu.VMEM((2 * NB, BLK), F32),
           dma((2, 6, 2, RING)), dma((2, 6, 2, RING)), dma((2, RING)),
           dma((2, RING)), dma((10,)), dma((25,)), dma((25,)), dma((NB,))],
        compiler_params=pltpu.CompilerParams(collective_id=0, has_side_effects=True, vmem_limit_bytes=VMEM_LIMIT),
        name='train_step',
    )(ha, hb, w1, w2, w3, g1, b1, g2, b2)


def solution(mesh):
    def local_step(h_a, h_b, w_one, w_two, w_three, gain_one, bias_one, gain_two, bias_two):
        vecs = [v.reshape(1, DIM) for v in (gain_one, bias_one, gain_two, bias_two)]
        d_three, d_two, d_one, _, _, _, st = train_step(h_a, h_b, w_one, w_two, w_three, *vecs)
        return st[4, 0], d_one, d_two, d_three, st[0], st[1], st[2], st[3]

    row_spec = P('data', None)
    return jax.shard_map(local_step, mesh=mesh,
                         in_specs=(row_spec, row_spec, P(), P(), P(), P(), P(), P(), P()),
                         out_specs=(P(), P(), P(), P(), P(), P(), P(), P()),
                         check_vma=False)
```

```python
import functools

import jax
import jax.numpy as jnp
from jax import lax
from jax.experimental import pallas as pl
from jax.experimental.pallas import tpu as pltpu
from jax.sharding import PartitionSpec as P

BN_EPS = 1e-5
STD_EPS = 1e-4
INV_WEIGHT = 2.0
VAR_WEIGHT = 1.0
COV_WEIGHT = 2.0

F32 = jnp.float32
BF16 = jnp.bfloat16
MESH = pl.DeviceIdType.MESH
VMEM_LIMIT = 67043328

ROWS = 1024
HALF = 512
FEAT = 512
DIM = 2048
NB = 8
BLK = 256
LAG = 2
RING = 8
ALL_ROWS = 16384


def sds(shape, dtype):
    return jax.ShapeDtypeStruct(shape, dtype)


ANY = pl.BlockSpec(memory_space=pl.ANY)
INV = pl.BlockSpec(memory_space=pltpu.VMEM)


class Place:
    def __init__(self):
        i = lax.axis_index('data')
        self.c = lax.rem(i, 2)
        x = lax.rem(i // 2, 2)
        y = lax.rem(i // 4, 2)
        z = i // 8
        zl = lax.rem(z, 2)
        zh = z // 2
        self.pc = i + 1 - 2 * self.c
        px = i + 2 - 4 * x
        py = i + 4 - 8 * y
        p1 = i + 8 - 16 * zl
        p2 = i + 16 - 32 * zh
        pd = px + py - i
        p3 = p1 + p2 - i
        self.phases = ((px, py, pd), (p1, p2, p3))
        self.end = zl == zh
        self.p1, self.p3 = p1, p3
        self.first, self.last = (px, py), (py, px)
        self.keep = [b * 128 for b in (x, y)]
        self.send = [(1 - b) * 128 for b in (x, y)]
        self.near = [k + zh * 64 for k in self.keep]
        self.far = [k + (1 - zh) * 64 for k in self.keep]
        self.own = [n + b * 32 for n, b in zip(self.near, (y, x))]
        self.give = [n + (1 - b) * 32 for n, b in zip(self.near, (y, x))]

    def barrier(self):
        sem = pltpu.get_barrier_semaphore()
        for p in (self.pc,) + self.phases[0] + self.phases[1]:
            pl.semaphore_signal(sem, inc=1, device_id=(p,), device_id_type=MESH)
        pl.semaphore_wait(sem, 7)


def rcopy(src, dst, ssem, rsem, dev):
    return pltpu.make_async_remote_copy(src_ref=src, dst_ref=dst, send_sem=ssem, recv_sem=rsem,
                                        device_id=(dev,), device_id_type=MESH)


def rows_at(off, n):
    return pl.ds(pl.multiple_of(off, n), n)


def nn(a, b):
    return jnp.dot(a, b, preferred_element_type=F32)


def nt(a, b):
    return lax.dot_general(a, b, (((1,), (1,)), ((), ())), preferred_element_type=F32)


def tn(a, b):
    return lax.dot_general(a, b, (((0,), (0,)), ((), ())), preferred_element_type=F32)


def lanes_at(off):
    return pl.ds(pl.multiple_of(off, 128), 128)


def cols_at(off):
    return pl.ds(pl.multiple_of(off, BLK), BLK)


def cols(j):
    return pl.ds(pl.multiple_of(j * BLK, BLK), BLK)


def is_inward(u):
    return (u >= GRAM_UNITS) & (lax.rem(jnp.maximum(u - GRAM_UNITS, 0), 4) == 0)


class Scatter:
    def __init__(self, place, part, lands, ssem, rsem):
        self.pl, self.part, self.lands, self.ssem, self.rsem = place, part, lands, ssem, rsem

    def landing(self, u, e, k, n):
        v = jnp.maximum(u - GRAM_UNITS, 0)
        q, r = v // 4, lax.rem(v, 4)
        gram = u < GRAM_UNITS
        if e in (0, 2):
            return self.lands[e].at[lax.rem(u, 4), k]
        if e == 4:
            turn = jnp.where(gram, u, jnp.where(r == 0, q, v - 1 - q))
            return self.lands[3].at[lax.rem(turn, 4), k]
        off = jnp.where(gram, lax.rem(u, 8) * 64, lax.rem(q, 2) * 320 + jnp.where(r == 0, 0, 64 + r * 64))
        return self.lands[1].at[k, pl.ds(pl.multiple_of(off, 64), n)]

    def copy(self, u, e, k, inward=False):
        me = self.pl
        off, n, dev = ((me.send[k], 128, me.first[k]), (me.far[k], 64, me.p1), (me.far[k], 64, me.p3),
                       (me.near[k], 64, me.p1), (me.give[k], 32, me.last[k]))[e]
        if e == 1 and inward:
            off, n = me.keep[k], 128
        r = lax.rem(u, RING)
        return rcopy(self.part.at[lax.rem(u, SLOTS), k, pl.ds(pl.multiple_of(off, 32), n)], self.landing(u, e, k, n),
                     self.ssem.at[e, k, r], self.rsem.at[e, k, r], dev)

    def start(self, u, e, inward=False):
        for k in range(2):
            self.copy(u, e, k, inward).start()

    def sent(self, u, e, inward=False):
        for k in range(2):
            self.copy(u, e, k, inward).wait_send()

    def add(self, u, e, off, inward=False):
        p, n = lax.rem(u, SLOTS), 128 if inward else (128, 64, 64, 64, 32)[e]
        for k in range(2):
            self.copy(u, e, k, inward).wait_recv()
            rr = pl.ds(pl.multiple_of(off[k], 32), n)
            self.part[p, k, rr] = self.part[p, k, rr] + self.landing(u, e, k, n)[...]

    def advance(self, t, final):
        me = self.pl
        u5, ok5 = unit_at(t - 5 * LAG)
        u4, ok4 = unit_at(t - 4 * LAG)
        u3, ok3 = unit_at(t - 3 * LAG)
        u2, ok2 = unit_at(t - 2 * LAG)
        u1, ok1 = unit_at(t - LAG)
        end, inner = me.end, jnp.logical_not(me.end)
        in5, in4, in3, in2, in1 = (is_inward(u) for u in (u5, u4, u3, u2, u1))

        def out(flag):
            return jnp.logical_not(flag)

        @pl.when(ok5 & ((end & out(in5)) | (inner & in5)))
        def _():
            self.sent(u5, 4)
            self.add(u5, 4, me.own)
            final(u5)

        @pl.when(ok4 & end & out(in4))
        def _():
            self.add(u4, 3, me.near)

        @pl.when(ok4 & ((end & out(in4)) | (inner & in4)))
        def _():
            self.start(u4, 4)

        @pl.when(ok4 & inner & out(in4))
        def _():
            self.sent(u4, 3)

        @pl.when(ok3 & inner)
        def _():
            self.sent(u3, 2)
            self.add(u3, 2, me.near)

        @pl.when(ok3 & inner & out(in3))
        def _():
            self.start(u3, 3)

        for inward, flag2, flag1 in ((False, out(in2), out(in1)), (True, in2, in1)):
            @pl.when(ok2 & inner & flag2)
            def _(inward=inward):
                self.add(u2, 1, me.keep if inward else me.far, inward)

            @pl.when(ok2 & end & flag2)
            def _(inward=inward):
                self.sent(u2, 1, inward)

        @pl.when(ok2 & inner)
        def _():
            self.start(u2, 2)

        @pl.when(ok1)
        def _():
            self.sent(u1, 0)
            self.add(u1, 0, me.keep)

        for inward, flag1 in ((False, out(in1)), (True, in1)):
            @pl.when(ok1 & end & flag1)
            def _(inward=inward):
                self.start(u1, 1, inward)


def scatter_scratch(slots):
    return [pltpu.VMEM((slots, 2, BLK, BLK), F32), pltpu.VMEM((4, 2, 128, BLK), F32),
            pltpu.VMEM((2, 640, BLK), F32), pltpu.VMEM((4, 2, 64, BLK), F32), pltpu.VMEM((4, 2, 32, BLK), F32),
            pltpu.SemaphoreType.DMA((5, 2, RING)), pltpu.SemaphoreType.DMA((5, 2, RING))]


class SmallReduce:
    def __init__(self, place, val, land, ssem, rsem):
        self.pl, self.val, self.ssem, self.rsem = place, val, ssem, rsem
        self.land = land.at[:, :, pl.ds(0, val.shape[0])]

    def copies(self, ph):
        return [rcopy(self.val, self.land.at[ph, k], self.ssem.at[ph, k], self.rsem.at[ph, k], p)
                for k, p in enumerate(self.pl.phases[ph])]

    def start(self, ph):
        for cp in self.copies(ph):
            cp.start()

    def finish(self, ph):
        for cp in self.copies(ph):
            cp.wait()
        land = self.land
        self.val[...] = (self.val[...] + land[ph, 0]) + (land[ph, 1] + land[ph, 2])

    def run(self):
        for ph in range(2):
            self.start(ph)
            self.finish(ph)


def small_scratch(n):
    return [pltpu.VMEM((n, BLK), F32), pltpu.SemaphoreType.DMA((2, 3)), pltpu.SemaphoreType.DMA((2, 3))]


GRAM_UNITS = 18
GRAM = 3
UNITS = 54
SLOTS = 5 * LAG + 1
START_3 = 28
START_2 = 44
END = START_2 + 21 + 11 * LAG
DZ_SLOTS = (23, 27, 30, 32, 34, 36, 37, 38)
PASS_2 = 39
PASS_1 = 45
SPAN_2, SPAN_1 = 3, 4


def block_of(q):
    i = jnp.int32(0)
    for first in (8, 15, 21, 26, 30, 33, 35):
        i = i + jnp.where(q >= first, 1, 0)
    return i, i + q - (17 * i - i * i) // 2


def unit_at(t):
    u = jnp.where(t < START_3, t, jnp.where(t < START_2, t - (START_3 - 18), t - (START_2 - 34)))
    ok = ((t >= 0) & (t < 18)) | ((t >= START_3) & (t < START_3 + 16)) | ((t >= START_2) & (t < START_2 + 20))
    return jnp.where(ok, u, 0), ok


def step_kernel(ha, hb, w1, w2, w3, g1, b1, g2, b2, g3_o, g2_o, g1_o, n1_o, h_o, ho_o, st_o, loss_o,
                zd, zod, dz, dzo, gw, x2h, x2o, x1h, x1o, g2v, g1v, lacc, rs, stage,
                part, r1, r2, r3, r4, ssem, rsem, sv, sa, sb, fa1, fb1, fa2, fb2,
                s2, sa2, sb2, s1, sa1, sb1, odd_land, even_land, e2, e1,
                asem, bsem, lsem, psem, csem, dsem, esem, wsem):
    me = Place()
    c = me.c
    nv, da = g2v.at[pl.ds(0, ROWS)], g2v.at[pl.ds(ROWS, ROWS)]
    hv = x2o.at[:, pl.ds(0, FEAT)]
    f1, f2 = s1, s2.at[pl.ds(0, 2 * NB)]
    gains, biases = (g1, g2), (b1, b2)
    half = pl.ds(pl.multiple_of(c * 1024, 1024), 1024)
    ohalf = pl.ds(pl.multiple_of((1 - c) * 1024, 1024), 1024)
    hhalf = pl.ds(pl.multiple_of(c * 256, 256), 256)
    hohalf = pl.ds(pl.multiple_of((1 - c) * 256, 256), 256)
    mine = pl.ds(pl.multiple_of(c * HALF, HALF), HALF)
    body = pl.ds(0, ROWS)
    w1v = zod.at[pl.ds(0, FEAT)]
    load_w1 = pltpu.make_async_copy(w1, w1v, csem.at[0])
    load_w2a = pltpu.make_async_copy(w2, gw, csem.at[1])
    load_w3a = pltpu.make_async_copy(w3, gw, csem.at[2])
    load_w2 = pltpu.make_async_copy(w2, gw, csem.at[6])
    load_n1 = pltpu.make_async_copy(n1_o, nv, csem.at[7])
    save_n1 = pltpu.make_async_copy(da, n1_o, csem.at[8])
    keep_x1 = pltpu.make_async_copy(dzo.at[:, half], x1h, csem.at[3])
    keep_h = pltpu.make_async_copy(hv.at[:, hhalf], h_o, csem.at[5])
    hh, ho = x2h.at[:, pl.ds(0, 256)], x2o.at[:, pl.ds(0, 256)]
    load_h2 = [pltpu.make_async_copy(h_o, hh, csem.at[5]), pltpu.make_async_copy(ho_o, ho, csem.at[2])]
    keep_x2 = pltpu.make_async_copy(dz.at[:, half], x2h, csem.at[4])
    swap_z = rcopy(zd.at[body], zod, dsem.at[0], esem.at[0], me.pc)
    swap_x2 = rcopy(dz.at[:, ohalf], x2o, dsem.at[1], esem.at[1], me.pc)
    swap_x1 = rcopy(dzo.at[:, ohalf], x1o, dsem.at[2], esem.at[2], me.pc)
    swap_h = rcopy(hv.at[:, hohalf], ho_o, dsem.at[3], esem.at[3], me.pc)
    swap_du1 = rcopy(dz, dzo, dsem.at[5], esem.at[5], me.pc)
    swap_s2 = rcopy(s2, e2, dsem.at[6], esem.at[6], me.pc)
    swap_s1 = rcopy(s1, e1, dsem.at[7], esem.at[7], me.pc)

    def load_h(src):
        return pltpu.make_async_copy(src, hv.at[mine], csem.at[9])

    def give_h(src):
        return rcopy(src, hv.at[mine], dsem.at[16], esem.at[16], me.pc)

    def load_w3(j):
        return pltpu.make_async_copy(w3.at[cols(j)], gw.at[cols(j)], wsem.at[j])

    def swap_du2(j):
        return rcopy(zd.at[body, cols(j)], zod.at[:, cols(j)], dsem.at[17 + j], esem.at[17 + j], me.pc)

    def swap_dz(j):
        return rcopy(dz.at[:, cols(j)], dzo.at[:, cols(j)], dsem.at[8 + j], esem.at[8 + j], me.pc)

    for k, own in ((0, ha), (1, hb)):
        @pl.when(c == k)
        def _(own=own):
            load_h(own).start()
    load_w1.start()
    load_w2a.start()
    me.barrier()
    for k, other in ((0, hb), (1, ha)):
        @pl.when(c == k)
        def _(other=other):
            give_h(other).start()
    lacc[...] = jnp.zeros_like(lacc)

    def matmul(src, w, dst, st):
        def step(j, carry):
            res = nn(src[...], w[:, cols(j)])
            dst[:, cols(j)] = res
            st[pl.ds(j, 1)] = jnp.sum(res, axis=0, keepdims=True)
            st[pl.ds(NB + j, 1)] = jnp.sum(res * res, axis=0, keepdims=True)
            return carry
        lax.fori_loop(0, NB, step, 0)

    def norm(u, x, st, layer):
        mean = st[0:NB] * (1.0 / ALL_ROWS)
        var = st[NB:2 * NB] * (1.0 / ALL_ROWS) - mean * mean
        inv = lax.rsqrt(var + BN_EPS)
        st[0:NB] = mean
        st[NB:2 * NB] = inv
        rs[NB * layer:NB * layer + NB] = inv

        def step(j, carry):
            nrm = (u[:, cols(j)] - st[pl.ds(j, 1)]) * st[pl.ds(NB + j, 1)]
            act = gains[layer][:, cols(j)] * nrm + biases[layer][:, cols(j)]
            u[:, cols(j)] = nrm
            x[:, cols(j)] = jnp.maximum(act, 0.0).astype(BF16)
            return carry
        lax.fori_loop(0, NB, step, 0)

    load_w1.wait()
    load_h(ha).wait()
    give_h(ha).wait()
    swap_h.start()
    keep_h.start()
    matmul(hv, w1v, da, f1)
    SmallReduce(me, f1, odd_land, fa1, fb1).run()
    norm(da, dzo, f1, 0)
    save_n1.start()
    keep_h.wait()
    swap_h.wait()
    swap_x1.start()
    keep_x1.start()
    load_w2a.wait()
    matmul(dzo, gw, nv, f2)
    load_w3a.start()
    SmallReduce(me, f2, even_land, fa2, fb2).run()
    norm(nv, dz, f2, 1)
    swap_x1.wait()
    swap_x2.start()
    keep_x2.start()
    load_w3a.wait()

    def z_block(j):
        res = nn(dz[...], gw[:, cols(j)]).astype(BF16)
        zd[0:ROWS, cols(j)] = res
        sv[pl.ds(j, 1)] = jnp.sum(res.astype(F32), axis=0, keepdims=True)

    def z_blocks(first):
        def step(j, carry):
            z_block(first + j)
            return carry
        lax.fori_loop(0, 2, step, 0)

    z_blocks(0)
    red0 = SmallReduce(me, sv, odd_land, sa, sb)
    red2 = SmallReduce(me, s2, even_land, sa2, sb2)
    red1 = SmallReduce(me, s1, odd_land, sa1, sb1)
    sc = Scatter(me, part, (r1, r2, r3, r4), ssem, rsem)

    def compute(u):
        p = lax.rem(u, SLOTS)

        @pl.when(u < GRAM_UNITS)
        def _():
            for k in range(2):
                i, j = block_of(2 * u + k)
                part[p, k] = tn(zd[0:ROWS, cols(i)], zd[0:ROWS, cols(j)])

        w, q = grad_unit(u)
        for w_, la, lb, ra, rb in ((0, x2h, x2o, dz, dzo), (1, x1h, x1o, zd, zod)):
            @pl.when((u >= GRAM_UNITS) & (w == w_))
            def _(la=la, lb=lb, ra=ra, rb=rb):
                lc = pl.ds(pl.multiple_of(lax.rem(q, 2) * 512, 512), 512)
                rc = cols(q // 2)
                res = tn(la[:, lc], ra[0:ROWS, rc]) + tn(lb[:, lc], rb[:, rc])
                part[p, 0] = res[0:BLK]
                part[p, 1] = res[BLK:2 * BLK]

        @pl.when((u >= GRAM_UNITS) & (w == 2))
        def _():
            rc = pl.ds(pl.multiple_of(q * 512, 512), 512)
            res = tn(hh[...], dz[:, rc]) + tn(ho[...], dzo[:, rc])
            part[p, 0] = res[:, 0:BLK]
            part[p, 1] = res[:, BLK:2 * BLK]

    def grad_unit(u):
        v = jnp.maximum(u - GRAM_UNITS, 0)
        return v // 16, lax.rem(v, 16)

    def of_weight(u, w):
        if w == GRAM:
            return u < GRAM_UNITS
        return (u >= GRAM_UNITS) & (grad_unit(u)[0] == w)

    def region(u, w, k, off, n):
        q = grad_unit(u)[1]
        if w == 2:
            r0, c0 = c * 256, q * 512 + k * BLK
        else:
            r0, c0 = c * 1024 + lax.rem(q, 2) * 512 + k * BLK, (q // 2) * BLK
        return rows_at(r0 + off, n), cols_at(c0)

    grads = (g3_o, g2v, g1v)

    def keep_copy(u, k):
        own = region(u, 0, k, me.own[k], 32)
        return pltpu.make_async_copy(stage.at[lax.rem(u, 3), k], g3_o.at[own], lsem.at[k, lax.rem(u, RING)])

    def hop(e, k, inward):
        if e == 3 and inward:
            return me.keep[k], 128, me.p1
        return ((me.own[k], 32, me.last[k]), (me.near[k], 64, me.p1), (me.near[k], 64, me.p3),
                (me.far[k], 64, me.p1), (me.keep[k], 128, me.first[k]))[e]

    def spread(u, w, e, k, inward=False):
        r = lax.rem(u, RING)
        off, n, dev = hop(e, k, inward)
        if w == GRAM:
            i, j = block_of(2 * u + k)
            src = dst = gw.at[rows_at(i * BLK + off, n), cols(j)]
        else:
            dst = grads[w].at[region(u, w, k, off, n)]
            src = stage.at[lax.rem(u, 3), k] if e == 0 and w == 0 else dst
        g = 0 if w == GRAM else 1
        return rcopy(src, dst, asem.at[g, e, k, r], bsem.at[g, e, k, r], dev)

    def cross(u, w):
        r = lax.rem(u, RING)
        q = grad_unit(u)[1]
        buf = grads[w].at[unit_region(q, w, c)]
        return rcopy(buf, buf, asem.at[1, 5, 0, r], bsem.at[1, 5, 0, r], me.pc)

    def unit_region(q, w, core):
        if w == 2:
            return rows_at(core * 256, 256), pl.ds(pl.multiple_of(q * 512, 512), 512)
        return rows_at(core * 1024 + lax.rem(q, 2) * 512, 512), cols(q // 2)

    def put(u, w, own):
        reg = unit_region(grad_unit(u)[1], w, c if own else 1 - c)
        out = (None, g2_o, g1_o)[w]
        return pltpu.make_async_copy(grads[w].at[reg], out.at[reg], psem.at[0 if own else 1, lax.rem(u, RING)])

    def final(u):
        for w in range(3):
            @pl.when(of_weight(u, w))
            def _(w=w):
                for k in range(2):
                    piece = part[lax.rem(u, SLOTS), k, rows_at(me.own[k], 32)]
                    if w == 0:
                        stage[lax.rem(u, 3), k] = piece
                        keep_copy(u, k).start()
                    else:
                        rr, cc = region(u, w, k, me.own[k], 32)
                        grads[w][rr, cc] = piece
                    spread(u, w, 0, k).start()

        @pl.when(u < GRAM_UNITS)
        def _():
            for k in range(2):
                i, j = block_of(2 * u + k)
                own = rows_at(me.own[k], 32)
                row0 = rows_at(i * BLK + me.own[k], 32)
                mu_r = g1v[rows_at(lax.rem(i, 2) * BLK + me.own[k], 32), lanes_at((i // 2) * 128)]
                mu_c = sv[pl.ds(j, 1)]
                mm = ALL_ROWS * jnp.concatenate([mu_r, mu_r], axis=1) * mu_c
                cov = (part[lax.rem(u, SLOTS), k, own] - mm) * (1.0 / (ALL_ROWS - 1))
                row = lax.broadcasted_iota(jnp.int32, (32, BLK), 0) + (i * BLK + me.own[k])
                col = lax.broadcasted_iota(jnp.int32, (32, BLK), 1) + j * BLK
                diag = row == col
                std = jnp.sqrt(jnp.where(diag, cov, 1.0) + STD_EPS)
                hinge = jnp.where(std < 1.0, VAR_WEIGHT / (2.0 * std), 0.0)
                weight = jnp.where(i == j, COV_WEIGHT, 2.0 * COV_WEIGHT)
                term = jnp.where(diag, VAR_WEIGHT * jnp.maximum(1.0 - std, 0.0), weight * cov * cov)
                lacc[...] = lacc[...] + ((term[0:8] + term[8:16]) + (term[16:24] + term[24:32]))
                gw[row0, cols(j)] = jnp.where(diag, -hinge, (2.0 * COV_WEIGHT) * cov).astype(BF16)
                spread(u, GRAM, 0, k).start()

    def diff_block(j):
        diff = zd[0:ROWS, cols(j)].astype(F32) - zod[:, cols(j)].astype(F32)
        sq = jnp.sum((diff * diff).reshape(ROWS // 8, 8, BLK), axis=0)
        lacc[...] = lacc[...] + (0.5 * INV_WEIGHT / ALL_ROWS) * sq
        da[:, cols(j)] = (2.0 * INV_WEIGHT / ALL_ROWS) * diff

    def dz_block(j):
        acc = nn(zd[...], gw[:, cols(j)])
        mean = acc[ROWS:ROWS + 1] + acc[ROWS + 1:ROWS + 2] + acc[ROWS + 2:ROWS + 3]
        dz[:, cols(j)] = (da[:, cols(j)] + (2.0 / (ALL_ROWS - 1)) * (acc[0:ROWS] - mean)).astype(BF16)

    def back_block(j, grad, st, layer):
        dx = nt(grad[0:ROWS, :], gw[cols(j)])
        nrm = nv[:, cols(j)]
        act = gains[layer][:, cols(j)] * nrm + biases[layer][:, cols(j)]
        d_act = jnp.where(act > 0.0, dx, 0.0)
        da[:, cols(j)] = d_act
        st[pl.ds(j, 1)] = jnp.sum(d_act, axis=0, keepdims=True)
        st[pl.ds(NB + j, 1)] = jnp.sum(d_act * nrm, axis=0, keepdims=True)

    def back_pre(dst, st, layer, after):
        def step(j, carry):
            scale = gains[layer][:, cols(j)] * rs[pl.ds(NB * layer + j, 1)]
            m0 = st[pl.ds(j, 1)] * (1.0 / ALL_ROWS)
            m1 = st[pl.ds(NB + j, 1)] * (1.0 / ALL_ROWS)
            dst[0:ROWS, cols(j)] = (scale * (da[:, cols(j)] - m0 - nv[:, cols(j)] * m1)).astype(BF16)
            after(j)
            return carry
        lax.fori_loop(0, NB, step, 0)

    def gather_step(e, u, w, inward):
        def each(f):
            for k in range(2):
                f(k)

        def wait_send(k):
            spread(u, w, e - 1, k, inward).wait_send()

        def wait_recv(k):
            spread(u, w, e - 1, k, inward).wait_recv()

        def begin(k):
            spread(u, w, e, k, inward).start()

        def run(sends, recvs, begins):
            if e == 1 and w == 0:
                each(lambda k: keep_copy(u, k).wait())
            if e in sends:
                each(wait_send)
            if e in recvs:
                each(wait_recv)
            if e in begins:
                each(begin)

        def at_end():
            if inward:
                run((), (4,), (4,))
            else:
                run((1, 2, 5), (1, 4, 5), (1, 4))

        def at_inner():
            if inward:
                run((1, 3, 4), (1, 3), (2, 3, 4))
            else:
                run((3, 4), (2, 3), (2, 3, 4))

        if e == 5:
            at_end()
        else:
            if e == 4 or not inward:
                pl.when(me.end)(at_end)
            if e > 1 or inward:
                pl.when(jnp.logical_not(me.end))(at_inner)
        if e == 5 and w < 3:
            cross(u, w).start()
            if w > 0:
                put(u, w, True).start()
        if e == 5 and w == GRAM:
            for k in range(2):
                i, j = block_of(2 * u + k)

                @pl.when(i != j)
                def _():
                    gw[rows_at(j * BLK, BLK), cols(i)] = gw[rows_at(i * BLK, BLK), cols(j)].T

    compute(jnp.int32(0))

    def slot(t, carry):
        u, ok = unit_at(t - 11 * LAG - 1)
        for w in (1, 2):
            @pl.when(ok & of_weight(u, w))
            def _(u=u, w=w):
                put(u, w, False).wait()

        u, ok = unit_at(t - 11 * LAG)
        for w in range(3):
            @pl.when(ok & of_weight(u, w))
            def _(u=u, w=w):
                cross(u, w).wait()
                if w > 0:
                    put(u, w, True).wait()
                    put(u, w, False).start()

        for e in (5, 4, 3, 2, 1):
            u, ok = unit_at(t - (5 + e) * LAG)
            flag = is_inward(u)
            for w in range(4):
                for inward in ((False,) if w == GRAM or e == 5 else (False, True)):
                    hit = ok & of_weight(u, w)
                    if w != GRAM and e < 5:
                        hit = hit & (flag if inward else jnp.logical_not(flag))

                    @pl.when(hit)
                    def _(e=e, u=u, w=w, inward=inward):
                        gather_step(e, u, w, inward)

        for first, red in ((2, red0), (PASS_2 + SPAN_2 - 1, red2), (PASS_1 + SPAN_1 - 1, red1)):
            @pl.when(t == first + 1)
            def _(red=red):
                red.finish(0)
                red.start(1)

            @pl.when(t == first + 2)
            def _(red=red):
                red.finish(1)

        for first, st, layer, dst in ((PASS_2 + SPAN_2 + 1, s2, 1, zd), (PASS_1 + SPAN_1 + 1, s1, 0, dz)):
            @pl.when(t == first)
            def _(st=st, layer=layer, dst=dst):
                back_pre(dst, st, layer, (lambda j: swap_du2(j).start()) if layer == 1 else (lambda j: None))

        @pl.when(t == PASS_2 + SPAN_2)
        def _():
            load_w2.start()

        @pl.when(t == PASS_2 + SPAN_2 + 1)
        def _():
            load_n1.start()
            swap_s2.start()

        @pl.when(t == PASS_1 + SPAN_1 + 1)
        def _():
            swap_du1.start()
            swap_s1.start()

        sc.advance(t, final)
        u, ok = unit_at(t)

        @pl.when(ok)
        def _(u=u):
            sc.start(u, 0)

        @pl.when(t == 4)
        def _():
            mean = sv[...] * (1.0 / ALL_ROWS)
            sv[...] = mean
            hi = mean.astype(BF16)
            mid = (mean - hi.astype(F32)).astype(BF16)
            low = (mean - hi.astype(F32) - mid.astype(F32)).astype(BF16)
            for j in range(NB):
                for h in range(2):
                    lanes = slice(128 * h, 128 * h + 128)
                    r0, c0 = (j % 2) * BLK + 128 * h, (j // 2) * 128
                    g1v[r0:r0 + 128, c0:c0 + 128] = jnp.broadcast_to(mean[j:j + 1, lanes], (128, 128)).T
                zd[ROWS:ROWS + 8, j * BLK:(j + 1) * BLK] = jnp.concatenate(
                    [hi[j:j + 1], mid[j:j + 1], low[j:j + 1], jnp.zeros((5, BLK), BF16)], axis=0)

        @pl.when(t < 3)
        def _():
            z_blocks(2 * t + 2)

        @pl.when(t == 3)
        def _():
            keep_x1.wait()
            keep_x2.wait()
            swap_x2.wait()
            save_n1.wait()
            swap_z.start()

        @pl.when(t == 7)
        def _():
            swap_z.wait()

        @pl.when((t >= 8) & (t < 8 + NB))
        def _():
            diff_block(t - 8)

        for j, first in enumerate(DZ_SLOTS):
            @pl.when(t == first + 1)
            def _(j=j):
                swap_dz(j).wait()

        mine_now = jnp.int32(-1)
        for j, first in enumerate(DZ_SLOTS):
            mine_now = jnp.where(t == first, j, mine_now)

        @pl.when(mine_now >= 0)
        def _():
            dz_block(mine_now)
            swap_dz(mine_now).start()

        @pl.when(t == DZ_SLOTS[-1])
        def _():
            for j in range(NB):
                load_w3(j).start()

        @pl.when(t == PASS_2)
        def _():
            s2[2 * NB:3 * NB] = lacc[...]

        @pl.when(t == PASS_1)
        def _():
            load_w2.wait()
            load_n1.wait()

        block = (t - (START_2 - 1)) // 2

        @pl.when((t >= START_2 - 1) & (t < START_2 + 15) & (t == START_2 - 1 + 2 * block))
        def _():
            swap_du2(block).wait()

        @pl.when(t == START_2 + 8)
        def _():
            for cp in load_h2:
                cp.start()

        @pl.when(t == START_2 + 14)
        def _():
            swap_du1.wait()
            for cp in load_h2:
                cp.wait()

        for first, span, grad, st, layer in ((PASS_2, SPAN_2, dz, s2, 1), (PASS_1, SPAN_1, zd, s1, 0)):
            @pl.when((t >= first) & (t < first + span))
            def _(first=first, n=-(-NB // span), grad=grad, st=st, layer=layer):
                def step(j, carry):
                    if layer == 1:
                        load_w3(j).wait()
                    back_block(j, grad, st, layer)
                    return carry
                lo = n * (t - first)
                lax.fori_loop(lo, jnp.minimum(lo + n, NB), step, 0)

        for last, red in ((2, red0), (PASS_2 + SPAN_2 - 1, red2), (PASS_1 + SPAN_1 - 1, red1)):
            @pl.when(t == last)
            def _(red=red):
                red.start(0)

        u, ok = unit_at(t + 1)

        @pl.when(ok)
        def _(u=u):
            compute(u)
        return carry
    lax.fori_loop(0, END, slot, 0)
    swap_s2.wait()
    swap_s1.wait()
    sum2, sum1 = s2[...] + e2[...], s1[...] + e1[...]
    for j in range(NB):
        lanes = slice(j * BLK, (j + 1) * BLK)
        st_o[0:1, lanes] = sum1[NB + j:NB + j + 1]
        st_o[1:2, lanes] = sum1[j:j + 1]
        st_o[2:3, lanes] = sum2[NB + j:NB + j + 1]
        st_o[3:4, lanes] = sum2[j:j + 1]
    loss_o[0, 0] = jnp.sum(sum2[2 * NB:])


def train_step(ha, hb, w1, w2, w3, g1, b1, g2, b2):
    act = pltpu.VMEM((ROWS, DIM), BF16)
    piece = pltpu.VMEM((ROWS, 1024), BF16)
    dma = pltpu.SemaphoreType.DMA
    return pl.pallas_call(
        step_kernel,
        out_shape=(sds((DIM, DIM), F32), sds((DIM, DIM), F32), sds((FEAT, DIM), F32), sds((ROWS, DIM), F32),
                   sds((ROWS, 256), BF16), sds((ROWS, 256), BF16), sds((4, DIM), F32), sds((1, 1), F32)),
        in_specs=[ANY] * 5 + [INV] * 4,
        out_specs=(ANY,) * 6 + (INV, pl.BlockSpec(memory_space=pltpu.SMEM)),
        scratch_shapes=[pltpu.VMEM((ROWS + 8, DIM), BF16), act, act, act, pltpu.VMEM((DIM, DIM), BF16),
                        piece, piece, piece, piece,
                        pltpu.VMEM((DIM, DIM), F32), pltpu.VMEM((FEAT, DIM), F32),
                        pltpu.VMEM((NB, BLK), F32), pltpu.VMEM((2 * NB, BLK), F32),
                        pltpu.VMEM((3, 2, 32, BLK), F32)]
        + scatter_scratch(SLOTS) + small_scratch(NB) + [dma((2, 3))] * 4
        + small_scratch(3 * NB) + small_scratch(2 * NB)
        + [pltpu.VMEM((2, 3, 2 * NB, BLK), F32), pltpu.VMEM((2, 3, 3 * NB, BLK), F32),
           pltpu.VMEM((3 * NB, BLK), F32), pltpu.VMEM((2 * NB, BLK), F32),
           dma((2, 6, 2, RING)), dma((2, 6, 2, RING)), dma((2, RING)),
           dma((2, RING)), dma((10,)), dma((25,)), dma((25,)), dma((NB,))],
        compiler_params=pltpu.CompilerParams(collective_id=0, has_side_effects=True, vmem_limit_bytes=VMEM_LIMIT),
        name='train_step',
    )(ha, hb, w1, w2, w3, g1, b1, g2, b2)


def solution(mesh):
    def local_step(h_a, h_b, w_one, w_two, w_three, gain_one, bias_one, gain_two, bias_two):
        vecs = [v.reshape(1, DIM) for v in (gain_one, bias_one, gain_two, bias_two)]
        d_three, d_two, d_one, _, _, _, st, loss = train_step(h_a, h_b, w_one, w_two, w_three, *vecs)
        return loss.reshape(()), d_one, d_two, d_three, st[0], st[1], st[2], st[3]

    row_spec = P('data', None)
    return jax.shard_map(local_step, mesh=mesh,
                         in_specs=(row_spec, row_spec, P(), P(), P(), P(), P(), P(), P()),
                         out_specs=(P(), P(), P(), P(), P(), P(), P(), P()),
                         check_vma=False)
```

```python
import functools

import jax
import jax.numpy as jnp
from jax import lax
from jax.experimental import pallas as pl
from jax.experimental.pallas import tpu as pltpu
from jax.sharding import PartitionSpec as P

BN_EPS = 1e-5
STD_EPS = 1e-4
INV_WEIGHT = 2.0
VAR_WEIGHT = 1.0
COV_WEIGHT = 2.0

F32 = jnp.float32
BF16 = jnp.bfloat16
MESH = pl.DeviceIdType.MESH
VMEM_LIMIT = 67043328

ROWS = 1024
HALF = 512
FEAT = 512
DIM = 2048
NB = 8
BLK = 256
LAG = 2
RING = 8
ALL_ROWS = 16384


def sds(shape, dtype):
    return jax.ShapeDtypeStruct(shape, dtype)


ANY = pl.BlockSpec(memory_space=pl.ANY)
INV = pl.BlockSpec(memory_space=pltpu.VMEM)


class Place:
    def __init__(self):
        i = lax.axis_index('data')
        self.c = lax.rem(i, 2)
        x = lax.rem(i // 2, 2)
        y = lax.rem(i // 4, 2)
        z = i // 8
        zl = lax.rem(z, 2)
        zh = z // 2
        self.pc = i + 1 - 2 * self.c
        px = i + 2 - 4 * x
        py = i + 4 - 8 * y
        p1 = i + 8 - 16 * zl
        p2 = i + 16 - 32 * zh
        pd = px + py - i
        p3 = p1 + p2 - i
        self.phases = ((px, py, pd), (p1, p2, p3))
        self.end = zl == zh
        self.p1, self.p3 = p1, p3
        self.first, self.last = (px, py), (py, px)
        self.keep = [b * 128 for b in (x, y)]
        self.send = [(1 - b) * 128 for b in (x, y)]
        self.near = [k + zh * 64 for k in self.keep]
        self.far = [k + (1 - zh) * 64 for k in self.keep]
        self.own = [n + b * 32 for n, b in zip(self.near, (y, x))]
        self.give = [n + (1 - b) * 32 for n, b in zip(self.near, (y, x))]

    def announce(self):
        sem = pltpu.get_barrier_semaphore()
        for p in (self.pc,) + self.phases[0] + self.phases[1]:
            pl.semaphore_signal(sem, inc=1, device_id=(p,), device_id_type=MESH)

    def await_all(self):
        pl.semaphore_wait(pltpu.get_barrier_semaphore(), 7)


def rcopy(src, dst, ssem, rsem, dev):
    return pltpu.make_async_remote_copy(src_ref=src, dst_ref=dst, send_sem=ssem, recv_sem=rsem,
                                        device_id=(dev,), device_id_type=MESH)


def rows_at(off, n):
    return pl.ds(pl.multiple_of(off, n), n)


def nn(a, b):
    return jnp.dot(a, b, preferred_element_type=F32)


def nt(a, b):
    return lax.dot_general(a, b, (((1,), (1,)), ((), ())), preferred_element_type=F32)


def tn(a, b):
    return lax.dot_general(a, b, (((0,), (0,)), ((), ())), preferred_element_type=F32)


def lanes_at(off):
    return pl.ds(pl.multiple_of(off, 128), 128)


def cols_at(off):
    return pl.ds(pl.multiple_of(off, BLK), BLK)


def cols(j):
    return pl.ds(pl.multiple_of(j * BLK, BLK), BLK)


def is_inward(u):
    return (u >= GRAM_UNITS) & (lax.rem(jnp.maximum(u - GRAM_UNITS, 0), 4) == 0)


class Scatter:
    def __init__(self, place, part, lands, ssem, rsem):
        self.pl, self.part, self.lands, self.ssem, self.rsem = place, part, lands, ssem, rsem

    def landing(self, u, e, k, n):
        v = jnp.maximum(u - GRAM_UNITS, 0)
        q, r = v // 4, lax.rem(v, 4)
        gram = u < GRAM_UNITS
        if e in (0, 2):
            return self.lands[e].at[lax.rem(u, 4), k]
        if e == 4:
            turn = jnp.where(gram, u, jnp.where(r == 0, q, v - 1 - q))
            return self.lands[3].at[lax.rem(turn, 4), k]
        off = jnp.where(gram, lax.rem(u, 8) * 64, lax.rem(q, 2) * 320 + jnp.where(r == 0, 0, 64 + r * 64))
        return self.lands[1].at[k, pl.ds(pl.multiple_of(off, 64), n)]

    def copy(self, u, e, k, inward=False):
        me = self.pl
        off, n, dev = ((me.send[k], 128, me.first[k]), (me.far[k], 64, me.p1), (me.far[k], 64, me.p3),
                       (me.near[k], 64, me.p1), (me.give[k], 32, me.last[k]))[e]
        if e == 1 and inward:
            off, n = me.keep[k], 128
        r = lax.rem(u, RING)
        return rcopy(self.part.at[lax.rem(u, SLOTS), k, pl.ds(pl.multiple_of(off, 32), n)], self.landing(u, e, k, n),
                     self.ssem.at[e, k, r], self.rsem.at[e, k, r], dev)

    def start(self, u, e, inward=False):
        for k in range(2):
            self.copy(u, e, k, inward).start()

    def sent(self, u, e, inward=False):
        for k in range(2):
            self.copy(u, e, k, inward).wait_send()

    def add(self, u, e, off, inward=False):
        p, n = lax.rem(u, SLOTS), 128 if inward else (128, 64, 64, 64, 32)[e]
        for k in range(2):
            self.copy(u, e, k, inward).wait_recv()
            rr = pl.ds(pl.multiple_of(off[k], 32), n)
            self.part[p, k, rr] = self.part[p, k, rr] + self.landing(u, e, k, n)[...]

    def step(self, e, u, gram, final):
        me = self.pl
        if gram:
            owner, passes = me.end, jnp.logical_not(me.end)
        else:
            inward = is_inward(u)
            owner, passes = me.end != inward, jnp.logical_not(me.end) & jnp.logical_not(inward)
        variants = (False,) if gram else (False, True)

        def of(variant):
            return me.end if gram else me.end & (inward if variant else jnp.logical_not(inward))

        if e == 1:
            self.sent(u, 0)
            self.add(u, 0, me.keep)
            for v in variants:
                pl.when(of(v))(functools.partial(self.start, u, 1, v))
        if e == 2:
            for v in variants:
                pl.when(of(v))(functools.partial(self.sent, u, 1, v))

            @pl.when(jnp.logical_not(me.end))
            def _():
                for v in variants:
                    def gather(v=v):
                        self.add(u, 1, me.keep if v else me.far, v)
                    if gram:
                        gather()
                    else:
                        pl.when(inward if v else jnp.logical_not(inward))(gather)
                self.start(u, 2)
        if e == 3:
            @pl.when(jnp.logical_not(me.end))
            def _():
                self.sent(u, 2)
                self.add(u, 2, me.near)

            pl.when(passes)(functools.partial(self.start, u, 3))
        if e == 4:
            pl.when(of(False))(functools.partial(self.add, u, 3, me.near))
            pl.when(owner)(functools.partial(self.start, u, 4))
            pl.when(passes)(functools.partial(self.sent, u, 3))
        if e == 5:
            @pl.when(owner)
            def _():
                self.sent(u, 4)
                self.add(u, 4, me.own)
                final(u)


class Span:
    def __init__(self, lo, hi, t):
        self.lo, self.hi, self.t = lo, hi, t

    def at(self, slot, f):
        if self.lo <= slot < self.hi:
            pl.when(self.t == slot)(f)

    def within(self, first, stop, f):
        if max(first, self.lo) >= min(stop, self.hi):
            return
        conds = ([] if first <= self.lo else [self.t >= first]) + ([] if stop >= self.hi else [self.t < stop])
        if not conds:
            f()
        else:
            pl.when(conds[0] if len(conds) == 1 else conds[0] & conds[1])(f)

    def units(self, lag, f):
        for w, first, stop, base in ((GRAM, 0, GRAM_UNITS, 0), (0, START_3, START_3 + 16, 18),
                                     (1, START_2, START_2 + 16, 34), (2, START_2 + 16, START_2 + 20, 50)):
            u = self.t - (lag + first - base)
            self.within(first + lag, stop + lag, functools.partial(f, u, w))


def scatter_scratch(slots):
    return [pltpu.VMEM((slots, 2, BLK, BLK), F32), pltpu.VMEM((4, 2, 128, BLK), F32),
            pltpu.VMEM((2, 640, BLK), F32), pltpu.VMEM((4, 2, 64, BLK), F32), pltpu.VMEM((4, 2, 32, BLK), F32),
            pltpu.SemaphoreType.DMA((5, 2, RING)), pltpu.SemaphoreType.DMA((5, 2, RING))]


class SmallReduce:
    def __init__(self, place, val, land, ssem, rsem):
        self.pl, self.val, self.ssem, self.rsem = place, val, ssem, rsem
        self.land = land.at[:, :, pl.ds(0, val.shape[0])]

    def copies(self, ph):
        return [rcopy(self.val, self.land.at[ph, k], self.ssem.at[ph, k], self.rsem.at[ph, k], p)
                for k, p in enumerate(self.pl.phases[ph])]

    def start(self, ph):
        for cp in self.copies(ph):
            cp.start()

    def finish(self, ph):
        for cp in self.copies(ph):
            cp.wait()
        land = self.land
        self.val[...] = (self.val[...] + land[ph, 0]) + (land[ph, 1] + land[ph, 2])

    def run(self):
        for ph in range(2):
            self.start(ph)
            self.finish(ph)


def small_scratch(n):
    return [pltpu.VMEM((n, BLK), F32), pltpu.SemaphoreType.DMA((2, 3)), pltpu.SemaphoreType.DMA((2, 3))]


GRAM_UNITS = 18
GRAM = 3
UNITS = 54
SLOTS = 5 * LAG + 1
START_3 = 28
START_2 = 44
END = START_2 + 21 + 11 * LAG
LOOPS = (0, 18, 39, 54, 66, END)
DZ_SLOTS = (23, 27, 30, 32, 34, 36, 37, 38)
PASS_2 = 39
PASS_1 = 45
SPAN_2, SPAN_1 = 3, 4


def block_of(q):
    i = jnp.int32(0)
    for first in (8, 15, 21, 26, 30, 33, 35):
        i = i + jnp.where(q >= first, 1, 0)
    return i, i + q - (17 * i - i * i) // 2


def step_kernel(ha, hb, w1, w2, w3, g1, b1, g2, b2, g3_o, g2_o, g1_o, n1_o, h_o, ho_o, st_o, loss_o,
                zd, zod, dz, dzo, gw, x2h, x2o, x1h, x1o, g2v, g1v, lacc, rs, stage,
                part, r1, r2, r3, r4, ssem, rsem, sv, sa, sb, fa1, fb1, fa2, fb2,
                s2, sa2, sb2, s1, sa1, sb1, odd_land, even_land, e2, e1,
                asem, bsem, lsem, psem, csem, dsem, esem, wsem):
    me = Place()
    me.announce()
    c = me.c
    nv, da = g2v.at[pl.ds(0, ROWS)], g2v.at[pl.ds(ROWS, ROWS)]
    hv = x2o.at[:, pl.ds(0, FEAT)]
    f1, f2 = s1, s2.at[pl.ds(0, 2 * NB)]
    gains, biases = (g1, g2), (b1, b2)
    half = pl.ds(pl.multiple_of(c * 1024, 1024), 1024)
    ohalf = pl.ds(pl.multiple_of((1 - c) * 1024, 1024), 1024)
    hhalf = pl.ds(pl.multiple_of(c * 256, 256), 256)
    hohalf = pl.ds(pl.multiple_of((1 - c) * 256, 256), 256)
    mine = pl.ds(pl.multiple_of(c * HALF, HALF), HALF)
    theirs = pl.ds(pl.multiple_of((1 - c) * HALF, HALF), HALF)
    body = pl.ds(0, ROWS)
    w1v = zod.at[pl.ds(0, FEAT)]
    load_w1 = pltpu.make_async_copy(w1, w1v, csem.at[0])
    load_w2a = pltpu.make_async_copy(w2, gw, csem.at[1])
    load_w3a = pltpu.make_async_copy(w3, gw, csem.at[2])
    load_w2 = pltpu.make_async_copy(w2, gw, csem.at[6])
    load_n1 = pltpu.make_async_copy(n1_o, nv, csem.at[7])
    save_n1 = pltpu.make_async_copy(da, n1_o, csem.at[8])
    keep_x1 = pltpu.make_async_copy(dzo.at[:, half], x1h, csem.at[3])
    keep_h = pltpu.make_async_copy(hv.at[:, hhalf], h_o, csem.at[5])
    hh, ho = x2h.at[:, pl.ds(0, 256)], x2o.at[:, pl.ds(0, 256)]
    load_h2 = [pltpu.make_async_copy(h_o, hh, csem.at[5]), pltpu.make_async_copy(ho_o, ho, csem.at[2])]
    keep_x2 = pltpu.make_async_copy(dz.at[:, half], x2h, csem.at[4])
    swap_z = rcopy(zd.at[body], zod, dsem.at[0], esem.at[0], me.pc)
    swap_x2 = rcopy(dz.at[:, ohalf], x2o, dsem.at[1], esem.at[1], me.pc)
    swap_x1 = rcopy(dzo.at[:, ohalf], x1o, dsem.at[2], esem.at[2], me.pc)
    swap_h = rcopy(hv.at[:, hohalf], ho_o, dsem.at[3], esem.at[3], me.pc)
    swap_du1 = rcopy(dz, dzo, dsem.at[5], esem.at[5], me.pc)
    swap_s2 = rcopy(s2, e2, dsem.at[6], esem.at[6], me.pc)
    swap_s1 = rcopy(s1, e1, dsem.at[7], esem.at[7], me.pc)

    def load_h(src):
        return pltpu.make_async_copy(src, hv.at[mine], csem.at[9])

    def give_h(src):
        return rcopy(src, hv.at[mine], dsem.at[16], esem.at[16], me.pc)

    def load_w3(j):
        return pltpu.make_async_copy(w3.at[cols(j)], gw.at[cols(j)], wsem.at[j])

    def swap_du2(j):
        return rcopy(zd.at[body, cols(j)], zod.at[:, cols(j)], dsem.at[17 + j], esem.at[17 + j], me.pc)

    def swap_dz(j):
        return rcopy(dz.at[:, cols(j)], dzo.at[:, cols(j)], dsem.at[8 + j], esem.at[8 + j], me.pc)

    for k, own in ((0, ha), (1, hb)):
        @pl.when(c == k)
        def _(own=own):
            load_h(own).start()
    load_w1.start()
    me.await_all()
    for k, other in ((0, hb), (1, ha)):
        @pl.when(c == k)
        def _(other=other):
            give_h(other).start()
    load_w2a.start()
    lacc[...] = jnp.zeros_like(lacc)

    def matmul(src, w, dst, st, rows, add):
        def step(j, carry):
            res = nn(src[rows, :], w[:, cols(j)])
            dst[rows, cols(j)] = res
            one = jnp.sum(res, axis=0, keepdims=True)
            two = jnp.sum(res * res, axis=0, keepdims=True)
            if add:
                one = one + st[pl.ds(j, 1)]
                two = two + st[pl.ds(NB + j, 1)]
            st[pl.ds(j, 1)] = one
            st[pl.ds(NB + j, 1)] = two
            return carry
        lax.fori_loop(0, NB, step, 0)

    def norm(u, x, st, layer):
        mean = st[0:NB] * (1.0 / ALL_ROWS)
        var = st[NB:2 * NB] * (1.0 / ALL_ROWS) - mean * mean
        inv = lax.rsqrt(var + BN_EPS)
        st[0:NB] = mean
        st[NB:2 * NB] = inv
        rs[NB * layer:NB * layer + NB] = inv

        def step(j, carry):
            nrm = (u[:, cols(j)] - st[pl.ds(j, 1)]) * st[pl.ds(NB + j, 1)]
            act = gains[layer][:, cols(j)] * nrm + biases[layer][:, cols(j)]
            u[:, cols(j)] = nrm
            x[:, cols(j)] = jnp.maximum(act, 0.0).astype(BF16)
            return carry
        lax.fori_loop(0, NB, step, 0)

    load_w1.wait()
    load_h(ha).wait()
    matmul(hv, w1v, da, f1, mine, False)
    give_h(ha).wait()
    swap_h.start()
    keep_h.start()
    matmul(hv, w1v, da, f1, theirs, True)
    SmallReduce(me, f1, odd_land, fa1, fb1).run()
    norm(da, dzo, f1, 0)
    save_n1.start()
    keep_h.wait()
    swap_h.wait()
    swap_x1.start()
    keep_x1.start()
    load_w2a.wait()
    matmul(dzo, gw, nv, f2, body, False)
    load_w3a.start()
    SmallReduce(me, f2, even_land, fa2, fb2).run()
    norm(nv, dz, f2, 1)
    swap_x1.wait()
    swap_x2.start()
    keep_x2.start()
    load_w3a.wait()

    def z_block(j):
        res = nn(dz[...], gw[:, cols(j)]).astype(BF16)
        zd[0:ROWS, cols(j)] = res
        sv[pl.ds(j, 1)] = jnp.sum(res.astype(F32), axis=0, keepdims=True)

    def z_blocks(first):
        def step(j, carry):
            z_block(first + j)
            return carry
        lax.fori_loop(0, 2, step, 0)

    z_blocks(0)
    red0 = SmallReduce(me, sv, odd_land, sa, sb)
    red2 = SmallReduce(me, s2, even_land, sa2, sb2)
    red1 = SmallReduce(me, s1, odd_land, sa1, sb1)
    sc = Scatter(me, part, (r1, r2, r3, r4), ssem, rsem)

    def compute(u, w):
        p = lax.rem(u, SLOTS)
        if w == GRAM:
            for k in range(2):
                i, j = block_of(2 * u + k)
                part[p, k] = tn(zd[0:ROWS, cols(i)], zd[0:ROWS, cols(j)])
            return
        q = grad_unit(u)[1]
        if w == 2:
            rc = pl.ds(pl.multiple_of(q * 512, 512), 512)
            res = tn(hh[...], dz[:, rc]) + tn(ho[...], dzo[:, rc])
            part[p, 0] = res[:, 0:BLK]
            part[p, 1] = res[:, BLK:2 * BLK]
            return
        la, lb, ra, rb = ((x2h, x2o, dz, dzo), (x1h, x1o, zd, zod))[w]
        lc = pl.ds(pl.multiple_of(lax.rem(q, 2) * 512, 512), 512)
        rc = cols(q // 2)
        res = tn(la[:, lc], ra[0:ROWS, rc]) + tn(lb[:, lc], rb[:, rc])
        part[p, 0] = res[0:BLK]
        part[p, 1] = res[BLK:2 * BLK]

    def grad_unit(u):
        v = jnp.maximum(u - GRAM_UNITS, 0)
        return v // 16, lax.rem(v, 16)

    def region(u, w, k, off, n):
        q = grad_unit(u)[1]
        if w == 2:
            r0, c0 = c * 256, q * 512 + k * BLK
        else:
            r0, c0 = c * 1024 + lax.rem(q, 2) * 512 + k * BLK, (q // 2) * BLK
        return rows_at(r0 + off, n), cols_at(c0)

    grads = (g3_o, g2v, g1v)

    def keep_copy(u, k):
        own = region(u, 0, k, me.own[k], 32)
        return pltpu.make_async_copy(stage.at[lax.rem(u, 3), k], g3_o.at[own], lsem.at[k, lax.rem(u, RING)])

    def hop(e, k, inward):
        if e == 3 and inward:
            return me.keep[k], 128, me.p1
        return ((me.own[k], 32, me.last[k]), (me.near[k], 64, me.p1), (me.near[k], 64, me.p3),
                (me.far[k], 64, me.p1), (me.keep[k], 128, me.first[k]))[e]

    def spread(u, w, e, k, inward=False):
        r = lax.rem(u, RING)
        off, n, dev = hop(e, k, inward)
        if w == GRAM:
            i, j = block_of(2 * u + k)
            src = dst = gw.at[rows_at(i * BLK + off, n), cols(j)]
        else:
            dst = grads[w].at[region(u, w, k, off, n)]
            src = stage.at[lax.rem(u, 3), k] if e == 0 and w == 0 else dst
        g = 0 if w == GRAM else 1
        return rcopy(src, dst, asem.at[g, e, k, r], bsem.at[g, e, k, r], dev)

    def cross(u, w):
        r = lax.rem(u, RING)
        q = grad_unit(u)[1]
        buf = grads[w].at[unit_region(q, w, c)]
        return rcopy(buf, buf, asem.at[1, 5, 0, r], bsem.at[1, 5, 0, r], me.pc)

    def unit_region(q, w, core):
        if w == 2:
            return rows_at(core * 256, 256), pl.ds(pl.multiple_of(q * 512, 512), 512)
        return rows_at(core * 1024 + lax.rem(q, 2) * 512, 512), cols(q // 2)

    def put(u, w, own):
        reg = unit_region(grad_unit(u)[1], w, c if own else 1 - c)
        out = (None, g2_o, g1_o)[w]
        return pltpu.make_async_copy(grads[w].at[reg], out.at[reg], psem.at[0 if own else 1, lax.rem(u, RING)])

    def final(u, w):
        if w < 3:
            for k in range(2):
                piece = part[lax.rem(u, SLOTS), k, rows_at(me.own[k], 32)]
                if w == 0:
                    stage[lax.rem(u, 3), k] = piece
                    keep_copy(u, k).start()
                else:
                    rr, cc = region(u, w, k, me.own[k], 32)
                    grads[w][rr, cc] = piece
                spread(u, w, 0, k).start()
            return
        for k in range(2):
            i, j = block_of(2 * u + k)
            own = rows_at(me.own[k], 32)
            row0 = rows_at(i * BLK + me.own[k], 32)
            mu_r = g1v[rows_at(lax.rem(i, 2) * BLK + me.own[k], 32), lanes_at((i // 2) * 128)]
            mu_c = sv[pl.ds(j, 1)]
            mm = ALL_ROWS * jnp.concatenate([mu_r, mu_r], axis=1) * mu_c
            cov = (part[lax.rem(u, SLOTS), k, own] - mm) * (1.0 / (ALL_ROWS - 1))
            row = lax.broadcasted_iota(jnp.int32, (32, BLK), 0) + (i * BLK + me.own[k])
            col = lax.broadcasted_iota(jnp.int32, (32, BLK), 1) + j * BLK
            diag = row == col
            std = jnp.sqrt(jnp.where(diag, cov, 1.0) + STD_EPS)
            hinge = jnp.where(std < 1.0, VAR_WEIGHT / (2.0 * std), 0.0)
            weight = jnp.where(i == j, COV_WEIGHT, 2.0 * COV_WEIGHT)
            term = jnp.where(diag, VAR_WEIGHT * jnp.maximum(1.0 - std, 0.0), weight * cov * cov)
            lacc[...] = lacc[...] + ((term[0:8] + term[8:16]) + (term[16:24] + term[24:32]))
            gw[row0, cols(j)] = jnp.where(diag, -hinge, (2.0 * COV_WEIGHT) * cov).astype(BF16)
            spread(u, GRAM, 0, k).start()

    def diff_block(j):
        diff = zd[0:ROWS, cols(j)].astype(F32) - zod[:, cols(j)].astype(F32)
        sq = jnp.sum((diff * diff).reshape(ROWS // 8, 8, BLK), axis=0)
        lacc[...] = lacc[...] + (0.5 * INV_WEIGHT / ALL_ROWS) * sq
        da[:, cols(j)] = (2.0 * INV_WEIGHT / ALL_ROWS) * diff

    def dz_block(j):
        acc = nn(zd[...], gw[:, cols(j)])
        mean = acc[ROWS:ROWS + 1] + acc[ROWS + 1:ROWS + 2] + acc[ROWS + 2:ROWS + 3]
        dz[:, cols(j)] = (da[:, cols(j)] + (2.0 / (ALL_ROWS - 1)) * (acc[0:ROWS] - mean)).astype(BF16)

    def back_block(j, grad, st, layer):
        dx = nt(grad[0:ROWS, :], gw[cols(j)])
        nrm = nv[:, cols(j)]
        act = gains[layer][:, cols(j)] * nrm + biases[layer][:, cols(j)]
        d_act = jnp.where(act > 0.0, dx, 0.0)
        da[:, cols(j)] = d_act
        st[pl.ds(j, 1)] = jnp.sum(d_act, axis=0, keepdims=True)
        st[pl.ds(NB + j, 1)] = jnp.sum(d_act * nrm, axis=0, keepdims=True)

    def back_pre(dst, st, layer, after):
        def step(j, carry):
            scale = gains[layer][:, cols(j)] * rs[pl.ds(NB * layer + j, 1)]
            m0 = st[pl.ds(j, 1)] * (1.0 / ALL_ROWS)
            m1 = st[pl.ds(NB + j, 1)] * (1.0 / ALL_ROWS)
            dst[0:ROWS, cols(j)] = (scale * (da[:, cols(j)] - m0 - nv[:, cols(j)] * m1)).astype(BF16)
            after(j)
            return carry
        lax.fori_loop(0, NB, step, 0)

    def gather_step(e, u, w, inward):
        def each(f):
            for k in range(2):
                f(k)

        def wait_send(k):
            spread(u, w, e - 1, k, inward).wait_send()

        def wait_recv(k):
            spread(u, w, e - 1, k, inward).wait_recv()

        def begin(k):
            spread(u, w, e, k, inward).start()

        def run(sends, recvs, begins):
            if e == 1 and w == 0:
                each(lambda k: keep_copy(u, k).wait())
            if e in sends:
                each(wait_send)
            if e in recvs:
                each(wait_recv)
            if e in begins:
                each(begin)

        def at_end():
            if inward:
                run((), (4,), (4,))
            else:
                run((1, 2, 5), (1, 4, 5), (1, 4))

        def at_inner():
            if inward:
                run((1, 3, 4), (1, 3), (2, 3, 4))
            else:
                run((3, 4), (2, 3), (2, 3, 4))

        if e == 5:
            at_end()
        else:
            if e == 4 or not inward:
                pl.when(me.end)(at_end)
            if e > 1 or inward:
                pl.when(jnp.logical_not(me.end))(at_inner)
        if e == 5 and w < 3:
            cross(u, w).start()
            if w > 0:
                put(u, w, True).start()
        if e == 5 and w == GRAM:
            for k in range(2):
                i, j = block_of(2 * u + k)

                @pl.when(i != j)
                def _():
                    gw[rows_at(j * BLK, BLK), cols(i)] = gw[rows_at(i * BLK, BLK), cols(j)].T

    compute(jnp.int32(0), GRAM)

    def gather(e, u, w):
        if w == GRAM or e == 5:
            gather_step(e, u, w, False)
            return
        inward = is_inward(u)
        pl.when(jnp.logical_not(inward))(lambda: gather_step(e, u, w, False))
        pl.when(inward)(lambda: gather_step(e, u, w, True))

    def put_end(u, w):
        if w in (1, 2):
            put(u, w, False).wait()

    def cross_end(u, w):
        if w < 3:
            cross(u, w).wait()
        if w in (1, 2):
            put(u, w, True).wait()
            put(u, w, False).start()

    def means():
        mean = sv[...] * (1.0 / ALL_ROWS)
        sv[...] = mean
        hi = mean.astype(BF16)
        mid = (mean - hi.astype(F32)).astype(BF16)
        low = (mean - hi.astype(F32) - mid.astype(F32)).astype(BF16)
        for j in range(NB):
            for h in range(2):
                lanes = slice(128 * h, 128 * h + 128)
                r0, c0 = (j % 2) * BLK + 128 * h, (j // 2) * 128
                g1v[r0:r0 + 128, c0:c0 + 128] = jnp.broadcast_to(mean[j:j + 1, lanes], (128, 128)).T
            zd[ROWS:ROWS + 8, j * BLK:(j + 1) * BLK] = jnp.concatenate(
                [hi[j:j + 1], mid[j:j + 1], low[j:j + 1], jnp.zeros((5, BLK), BF16)], axis=0)

    def slots(lo, hi):
        def slot(t, carry):
            run_slot(Span(lo, hi, t), t)
            return carry
        lax.fori_loop(lo, hi, slot, 0)

    def run_slot(span, t):
        span.units(11 * LAG + 1, put_end)
        span.units(11 * LAG, cross_end)
        for e in (5, 4, 3, 2, 1):
            span.units((5 + e) * LAG, functools.partial(gather, e))
        reds = ((2, red0), (PASS_2 + SPAN_2 - 1, red2), (PASS_1 + SPAN_1 - 1, red1))
        for first, red in reds:
            @functools.partial(span.at, first + 1)
            def _(red=red):
                red.finish(0)
                red.start(1)

            @functools.partial(span.at, first + 2)
            def _(red=red):
                red.finish(1)

        @functools.partial(span.at, PASS_2 + SPAN_2)
        def _():
            load_w2.start()

        @functools.partial(span.at, PASS_2 + SPAN_2 + 1)
        def _():
            back_pre(zd, s2, 1, lambda j: swap_du2(j).start())
            load_n1.start()
            swap_s2.start()

        @functools.partial(span.at, PASS_1 + SPAN_1 + 1)
        def _():
            back_pre(dz, s1, 0, lambda j: None)
            swap_du1.start()
            swap_s1.start()

        for e in (5, 4, 3, 2, 1):
            span.units(e * LAG, lambda u, w, e=e: sc.step(e, u, w == GRAM, lambda v: final(v, w)))
        span.units(0, lambda u, w: sc.start(u, 0))
        span.at(4, means)
        span.within(0, 3, lambda: z_blocks(2 * t + 2))

        @functools.partial(span.at, 3)
        def _():
            keep_x1.wait()
            keep_x2.wait()
            swap_x2.wait()
            save_n1.wait()
            swap_z.start()

        span.at(7, swap_z.wait)
        span.within(8, 8 + NB, lambda: diff_block(t - 8))
        for j, first in enumerate(DZ_SLOTS):
            span.at(first + 1, lambda j=j: swap_dz(j).wait())
        mine_now = jnp.int32(-1)
        for j, first in enumerate(DZ_SLOTS):
            if span.lo <= first < span.hi:
                mine_now = jnp.where(t == first, j, mine_now)
        if any(span.lo <= first < span.hi for first in DZ_SLOTS):
            @pl.when(mine_now >= 0)
            def _():
                dz_block(mine_now)
                swap_dz(mine_now).start()

        @functools.partial(span.at, DZ_SLOTS[-1])
        def _():
            for j in range(NB):
                load_w3(j).start()

        @functools.partial(span.at, PASS_2)
        def _():
            s2[2 * NB:3 * NB] = lacc[...]

        @functools.partial(span.at, PASS_1)
        def _():
            load_w2.wait()
            load_n1.wait()

        @functools.partial(span.within, START_2 - 1, START_2 + 15)
        def _():
            block = (t - (START_2 - 1)) // 2

            @pl.when(t == START_2 - 1 + 2 * block)
            def _():
                swap_du2(block).wait()

        @functools.partial(span.at, START_2 + 8)
        def _():
            for cp in load_h2:
                cp.start()

        @functools.partial(span.at, START_2 + 14)
        def _():
            swap_du1.wait()
            for cp in load_h2:
                cp.wait()

        for first, width, grad, st, layer in ((PASS_2, SPAN_2, dz, s2, 1), (PASS_1, SPAN_1, zd, s1, 0)):
            @functools.partial(span.within, first, first + width)
            def _(first=first, n=-(-NB // width), grad=grad, st=st, layer=layer):
                def step(j, carry):
                    if layer == 1:
                        load_w3(j).wait()
                    back_block(j, grad, st, layer)
                    return carry
                lo = n * (t - first)
                lax.fori_loop(lo, jnp.minimum(lo + n, NB), step, 0)

        for last, red in reds:
            span.at(last, lambda red=red: red.start(0))
        span.units(-1, compute)

    for lo, hi in zip(LOOPS, LOOPS[1:]):
        slots(lo, hi)
    swap_s2.wait()
    swap_s1.wait()
    sum2, sum1 = s2[...] + e2[...], s1[...] + e1[...]
    for j in range(NB):
        lanes = slice(j * BLK, (j + 1) * BLK)
        st_o[0:1, lanes] = sum1[NB + j:NB + j + 1]
        st_o[1:2, lanes] = sum1[j:j + 1]
        st_o[2:3, lanes] = sum2[NB + j:NB + j + 1]
        st_o[3:4, lanes] = sum2[j:j + 1]
    loss_o[0, 0] = jnp.sum(sum2[2 * NB:])


def train_step(ha, hb, w1, w2, w3, g1, b1, g2, b2):
    act = pltpu.VMEM((ROWS, DIM), BF16)
    piece = pltpu.VMEM((ROWS, 1024), BF16)
    dma = pltpu.SemaphoreType.DMA
    return pl.pallas_call(
        step_kernel,
        out_shape=(sds((DIM, DIM), F32), sds((DIM, DIM), F32), sds((FEAT, DIM), F32), sds((ROWS, DIM), F32),
                   sds((ROWS, 256), BF16), sds((ROWS, 256), BF16), sds((4, DIM), F32), sds((1, 1), F32)),
        in_specs=[ANY] * 5 + [INV] * 4,
        out_specs=(ANY,) * 6 + (INV, pl.BlockSpec(memory_space=pltpu.SMEM)),
        scratch_shapes=[pltpu.VMEM((ROWS + 8, DIM), BF16), act, act, act, pltpu.VMEM((DIM, DIM), BF16),
                        piece, piece, piece, piece,
                        pltpu.VMEM((DIM, DIM), F32), pltpu.VMEM((FEAT, DIM), F32),
                        pltpu.VMEM((NB, BLK), F32), pltpu.VMEM((2 * NB, BLK), F32),
                        pltpu.VMEM((3, 2, 32, BLK), F32)]
        + scatter_scratch(SLOTS) + small_scratch(NB) + [dma((2, 3))] * 4
        + small_scratch(3 * NB) + small_scratch(2 * NB)
        + [pltpu.VMEM((2, 3, 2 * NB, BLK), F32), pltpu.VMEM((2, 3, 3 * NB, BLK), F32),
           pltpu.VMEM((3 * NB, BLK), F32), pltpu.VMEM((2 * NB, BLK), F32),
           dma((2, 6, 2, RING)), dma((2, 6, 2, RING)), dma((2, RING)),
           dma((2, RING)), dma((10,)), dma((25,)), dma((25,)), dma((NB,))],
        compiler_params=pltpu.CompilerParams(collective_id=0, has_side_effects=True, vmem_limit_bytes=VMEM_LIMIT),
        name='train_step',
    )(ha, hb, w1, w2, w3, g1, b1, g2, b2)


def solution(mesh):
    def local_step(h_a, h_b, w_one, w_two, w_three, gain_one, bias_one, gain_two, bias_two):
        vecs = [v.reshape(1, DIM) for v in (gain_one, bias_one, gain_two, bias_two)]
        d_three, d_two, d_one, _, _, _, st, loss = train_step(h_a, h_b, w_one, w_two, w_three, *vecs)
        return loss.reshape(()), d_one, d_two, d_three, st[0], st[1], st[2], st[3]

    row_spec = P('data', None)
    return jax.shard_map(local_step, mesh=mesh,
                         in_specs=(row_spec, row_spec, P(), P(), P(), P(), P(), P(), P()),
                         out_specs=(P(), P(), P(), P(), P(), P(), P(), P()),
                         check_vma=False)
```

```python
import functools

import jax
import jax.numpy as jnp
from jax import lax
from jax.experimental import pallas as pl
from jax.experimental.pallas import tpu as pltpu
from jax.sharding import PartitionSpec as P

BN_EPS = 1e-5
STD_EPS = 1e-4
INV_WEIGHT = 2.0
VAR_WEIGHT = 1.0
COV_WEIGHT = 2.0

F32 = jnp.float32
BF16 = jnp.bfloat16
MESH = pl.DeviceIdType.MESH
VMEM_LIMIT = 67043328

ROWS = 1024
HALF = 512
FEAT = 512
DIM = 2048
NB = 8
BLK = 256
LAG = 2
RING = 8
ALL_ROWS = 16384


def sds(shape, dtype):
    return jax.ShapeDtypeStruct(shape, dtype)


ANY = pl.BlockSpec(memory_space=pl.ANY)
INV = pl.BlockSpec(memory_space=pltpu.VMEM)


class Place:
    def __init__(self):
        i = lax.axis_index('data')
        self.c = lax.rem(i, 2)
        x = lax.rem(i // 2, 2)
        y = lax.rem(i // 4, 2)
        z = i // 8
        zl = lax.rem(z, 2)
        zh = z // 2
        self.pc = i + 1 - 2 * self.c
        px = i + 2 - 4 * x
        py = i + 4 - 8 * y
        p1 = i + 8 - 16 * zl
        p2 = i + 16 - 32 * zh
        pd = px + py - i
        p3 = p1 + p2 - i
        self.phases = ((px, py, pd), (p1, p2, p3))
        self.end = zl == zh
        self.p1, self.p3 = p1, p3
        self.first, self.last = (px, py), (py, px)
        self.keep = [b * 128 for b in (x, y)]
        self.send = [(1 - b) * 128 for b in (x, y)]
        self.near = [k + zh * 64 for k in self.keep]
        self.far = [k + (1 - zh) * 64 for k in self.keep]
        self.own = [n + b * 32 for n, b in zip(self.near, (y, x))]
        self.give = [n + (1 - b) * 32 for n, b in zip(self.near, (y, x))]

    def announce(self):
        sem = pltpu.get_barrier_semaphore()
        for p in (self.pc,) + self.phases[0] + self.phases[1]:
            pl.semaphore_signal(sem, inc=1, device_id=(p,), device_id_type=MESH)

    def await_all(self):
        pl.semaphore_wait(pltpu.get_barrier_semaphore(), 7)


def rcopy(src, dst, ssem, rsem, dev):
    return pltpu.make_async_remote_copy(src_ref=src, dst_ref=dst, send_sem=ssem, recv_sem=rsem,
                                        device_id=(dev,), device_id_type=MESH)


def rows_at(off, n):
    return pl.ds(pl.multiple_of(off, n), n)


def nn(a, b):
    return jnp.dot(a, b, preferred_element_type=F32)


def nt(a, b):
    return lax.dot_general(a, b, (((1,), (1,)), ((), ())), preferred_element_type=F32)


def tn(a, b):
    return lax.dot_general(a, b, (((0,), (0,)), ((), ())), preferred_element_type=F32)


def lanes_at(off):
    return pl.ds(pl.multiple_of(off, 128), 128)


def cols_at(off):
    return pl.ds(pl.multiple_of(off, BLK), BLK)


def cols(j):
    return pl.ds(pl.multiple_of(j * BLK, BLK), BLK)


def is_inward(u):
    return (u >= GRAM_UNITS) & (lax.rem(jnp.maximum(u - GRAM_UNITS, 0), 4) == 0)


class Scatter:
    def __init__(self, place, part, lands, ssem, rsem):
        self.pl, self.part, self.lands, self.ssem, self.rsem = place, part, lands, ssem, rsem

    def landing(self, u, e, k, n):
        v = jnp.maximum(u - GRAM_UNITS, 0)
        q, r = v // 4, lax.rem(v, 4)
        gram = u < GRAM_UNITS
        if e in (0, 2):
            return self.lands[e].at[lax.rem(u, 4), k]
        if e == 4:
            turn = jnp.where(gram, u, jnp.where(r == 0, q, v - 1 - q))
            return self.lands[3].at[lax.rem(turn, 4), k]
        off = jnp.where(gram, lax.rem(u, 8) * 64, lax.rem(q, 2) * 320 + jnp.where(r == 0, 0, 64 + r * 64))
        return self.lands[1].at[k, pl.ds(pl.multiple_of(off, 64), n)]

    def copy(self, u, e, k, inward=False):
        me = self.pl
        off, n, dev = ((me.send[k], 128, me.first[k]), (me.far[k], 64, me.p1), (me.far[k], 64, me.p3),
                       (me.near[k], 64, me.p1), (me.give[k], 32, me.last[k]))[e]
        if e == 1 and inward:
            off, n = me.keep[k], 128
        r = lax.rem(u, RING)
        return rcopy(self.part.at[lax.rem(u, SLOTS), k, pl.ds(pl.multiple_of(off, 32), n)], self.landing(u, e, k, n),
                     self.ssem.at[e, k, r], self.rsem.at[e, k, r], dev)

    def start(self, u, e, inward=False):
        for k in range(2):
            self.copy(u, e, k, inward).start()

    def sent(self, u, e, inward=False):
        for k in range(2):
            self.copy(u, e, k, inward).wait_send()

    def add(self, u, e, off, inward=False):
        p, n = lax.rem(u, SLOTS), 128 if inward else (128, 64, 64, 64, 32)[e]
        for k in range(2):
            self.copy(u, e, k, inward).wait_recv()
            rr = pl.ds(pl.multiple_of(off[k], 32), n)
            self.part[p, k, rr] = self.part[p, k, rr] + self.landing(u, e, k, n)[...]

    def step(self, e, u, gram, final):
        me = self.pl
        if gram:
            owner, passes = me.end, jnp.logical_not(me.end)
        else:
            inward = is_inward(u)
            owner, passes = me.end != inward, jnp.logical_not(me.end) & jnp.logical_not(inward)
        variants = (False,) if gram else (False, True)

        def of(variant):
            return me.end if gram else me.end & (inward if variant else jnp.logical_not(inward))

        if e == 1:
            self.sent(u, 0)
            self.add(u, 0, me.keep)
            for v in variants:
                pl.when(of(v))(functools.partial(self.start, u, 1, v))
        if e == 2:
            for v in variants:
                pl.when(of(v))(functools.partial(self.sent, u, 1, v))

            @pl.when(jnp.logical_not(me.end))
            def _():
                for v in variants:
                    def gather(v=v):
                        self.add(u, 1, me.keep if v else me.far, v)
                    if gram:
                        gather()
                    else:
                        pl.when(inward if v else jnp.logical_not(inward))(gather)
                self.start(u, 2)
        if e == 3:
            @pl.when(jnp.logical_not(me.end))
            def _():
                self.sent(u, 2)
                self.add(u, 2, me.near)

            pl.when(passes)(functools.partial(self.start, u, 3))
        if e == 4:
            pl.when(of(False))(functools.partial(self.add, u, 3, me.near))
            pl.when(owner)(functools.partial(self.start, u, 4))
            pl.when(passes)(functools.partial(self.sent, u, 3))
        if e == 5:
            @pl.when(owner)
            def _():
                self.sent(u, 4)
                self.add(u, 4, me.own)
                final(u)


class Span:
    def __init__(self, lo, hi, t):
        self.lo, self.hi, self.t = lo, hi, t

    def at(self, slot, f):
        if self.lo <= slot < self.hi:
            pl.when(self.t == slot)(f)

    def within(self, first, stop, f):
        if max(first, self.lo) >= min(stop, self.hi):
            return
        conds = ([] if first <= self.lo else [self.t >= first]) + ([] if stop >= self.hi else [self.t < stop])
        if not conds:
            f()
        else:
            pl.when(conds[0] if len(conds) == 1 else conds[0] & conds[1])(f)

    def units(self, lag, f):
        for w, first, stop, base in ((GRAM, 0, GRAM_UNITS, 0), (0, START_3, START_3 + 16, 18),
                                     (1, START_2, START_2 + 16, 34), (2, START_2 + 16, START_2 + 20, 50)):
            u = self.t - (lag + first - base)
            self.within(first + lag, stop + lag, functools.partial(f, u, w))


def scatter_scratch(slots):
    return [pltpu.VMEM((slots, 2, BLK, BLK), F32), pltpu.VMEM((4, 2, 128, BLK), F32),
            pltpu.VMEM((2, 640, BLK), F32), pltpu.VMEM((4, 2, 64, BLK), F32), pltpu.VMEM((4, 2, 32, BLK), F32),
            pltpu.SemaphoreType.DMA((5, 2, RING)), pltpu.SemaphoreType.DMA((5, 2, RING))]


class SmallReduce:
    def __init__(self, place, val, land, ssem, rsem):
        self.pl, self.val, self.ssem, self.rsem = place, val, ssem, rsem
        self.land = land.at[:, :, pl.ds(0, val.shape[0])]

    def copies(self, ph):
        return [rcopy(self.val, self.land.at[ph, k], self.ssem.at[ph, k], self.rsem.at[ph, k], p)
                for k, p in enumerate(self.pl.phases[ph])]

    def start(self, ph):
        for cp in self.copies(ph):
            cp.start()

    def finish(self, ph):
        for cp in self.copies(ph):
            cp.wait()
        land = self.land
        self.val[...] = (self.val[...] + land[ph, 0]) + (land[ph, 1] + land[ph, 2])

    def run(self):
        for ph in range(2):
            self.start(ph)
            self.finish(ph)


def small_scratch(n):
    return [pltpu.VMEM((n, BLK), F32), pltpu.SemaphoreType.DMA((2, 3)), pltpu.SemaphoreType.DMA((2, 3))]


GRAM_UNITS = 18
GRAM = 3
UNITS = 54
SLOTS = 5 * LAG + 1
START_3 = 28
START_2 = 44
END = START_2 + 21 + 11 * LAG
LOOPS = (0, 18, 39, 54, 66, END)
DZ_SLOTS = (23, 27, 30, 32, 34, 36, 37, 38)
PASS_2 = 39
PASS_1 = 45
SPAN_2, SPAN_1 = 3, 4


def block_of(q):
    i = jnp.int32(0)
    for first in (8, 15, 21, 26, 30, 33, 35):
        i = i + jnp.where(q >= first, 1, 0)
    return i, i + q - (17 * i - i * i) // 2


def step_kernel(ha, hb, w1, w2, w3, g1, b1, g2, b2, g3_o, g2_o, g1_o, n1_o, h_o, ho_o, st_o, loss_o,
                zd, zod, dz, dzo, gw, x2h, x2o, x1h, x1o, g2v, g1v, lacc, rs, stage,
                part, r1, r2, r3, r4, ssem, rsem, sv, sa, sb, fa1, fb1, fa2, fb2,
                s2, sa2, sb2, s1, sa1, sb1, odd_land, even_land, e2, e1,
                asem, bsem, lsem, psem, csem, dsem, esem, wsem):
    me = Place()
    me.announce()
    c = me.c
    nv, da = g2v.at[pl.ds(0, ROWS)], g2v.at[pl.ds(ROWS, ROWS)]
    hv = x2o.at[:, pl.ds(0, FEAT)]
    f1, f2 = s1, s2.at[pl.ds(0, 2 * NB)]
    gains, biases = (g1, g2), (b1, b2)
    half = pl.ds(pl.multiple_of(c * 1024, 1024), 1024)
    ohalf = pl.ds(pl.multiple_of((1 - c) * 1024, 1024), 1024)
    hhalf = pl.ds(pl.multiple_of(c * 256, 256), 256)
    hohalf = pl.ds(pl.multiple_of((1 - c) * 256, 256), 256)
    mine = pl.ds(pl.multiple_of(c * HALF, HALF), HALF)
    theirs = pl.ds(pl.multiple_of((1 - c) * HALF, HALF), HALF)
    body = pl.ds(0, ROWS)
    w1v = zod.at[pl.ds(0, FEAT)]
    load_w1 = pltpu.make_async_copy(w1, w1v, csem.at[0])
    load_w2a = pltpu.make_async_copy(w2, gw, csem.at[1])
    load_w3a = pltpu.make_async_copy(w3, gw, csem.at[2])
    load_w2 = pltpu.make_async_copy(w2, gw, csem.at[6])
    load_n1 = pltpu.make_async_copy(n1_o, nv, csem.at[7])
    save_n1 = pltpu.make_async_copy(da, n1_o, csem.at[8])
    keep_x1 = pltpu.make_async_copy(dzo.at[:, half], x1h, csem.at[3])
    keep_h = pltpu.make_async_copy(hv.at[:, hhalf], h_o, csem.at[5])
    hh, ho = x2h.at[:, pl.ds(0, 256)], x2o.at[:, pl.ds(0, 256)]
    load_h2 = [pltpu.make_async_copy(h_o, hh, csem.at[5]), pltpu.make_async_copy(ho_o, ho, csem.at[2])]
    keep_x2 = pltpu.make_async_copy(dz.at[:, half], x2h, csem.at[4])
    swap_z = rcopy(zd.at[body], zod, dsem.at[0], esem.at[0], me.pc)
    swap_x2 = rcopy(dz.at[:, ohalf], x2o, dsem.at[1], esem.at[1], me.pc)
    swap_x1 = rcopy(dzo.at[:, ohalf], x1o, dsem.at[2], esem.at[2], me.pc)
    swap_h = rcopy(hv.at[:, hohalf], ho_o, dsem.at[3], esem.at[3], me.pc)
    swap_du1 = rcopy(dz, dzo, dsem.at[5], esem.at[5], me.pc)
    swap_s2 = rcopy(s2, e2, dsem.at[6], esem.at[6], me.pc)
    swap_s1 = rcopy(s1, e1, dsem.at[7], esem.at[7], me.pc)

    def load_h(src):
        return pltpu.make_async_copy(src, hv.at[mine], csem.at[9])

    def give_h(src):
        return rcopy(src, hv.at[mine], dsem.at[16], esem.at[16], me.pc)

    def load_w3(j):
        return pltpu.make_async_copy(w3.at[cols(j)], gw.at[cols(j)], wsem.at[j])

    def swap_du2(j):
        return rcopy(zd.at[body, cols(j)], zod.at[:, cols(j)], dsem.at[17 + j], esem.at[17 + j], me.pc)

    def swap_dz(j):
        return rcopy(dz.at[:, cols(j)], dzo.at[:, cols(j)], dsem.at[8 + j], esem.at[8 + j], me.pc)

    for k, own in ((0, ha), (1, hb)):
        @pl.when(c == k)
        def _(own=own):
            load_h(own).start()
    load_w1.start()
    me.await_all()
    for k, other in ((0, hb), (1, ha)):
        @pl.when(c == k)
        def _(other=other):
            give_h(other).start()
    load_w2a.start()
    lacc[...] = jnp.zeros_like(lacc)

    def matmul(src, w, dst, st, rows, add):
        def step(j, carry):
            res = nn(src[rows, :], w[:, cols(j)])
            dst[rows, cols(j)] = res
            one = jnp.sum(res, axis=0, keepdims=True)
            two = jnp.sum(res * res, axis=0, keepdims=True)
            if add:
                one = one + st[pl.ds(j, 1)]
                two = two + st[pl.ds(NB + j, 1)]
            st[pl.ds(j, 1)] = one
            st[pl.ds(NB + j, 1)] = two
            return carry
        lax.fori_loop(0, NB, step, 0)

    def norm(u, x, st, layer):
        mean = st[0:NB] * (1.0 / ALL_ROWS)
        var = st[NB:2 * NB] * (1.0 / ALL_ROWS) - mean * mean
        inv = lax.rsqrt(var + BN_EPS)
        st[0:NB] = mean
        st[NB:2 * NB] = inv
        rs[NB * layer:NB * layer + NB] = inv

        def step(j, carry):
            nrm = (u[:, cols(j)] - st[pl.ds(j, 1)]) * st[pl.ds(NB + j, 1)]
            act = gains[layer][:, cols(j)] * nrm + biases[layer][:, cols(j)]
            u[:, cols(j)] = nrm
            x[:, cols(j)] = jnp.maximum(act, 0.0).astype(BF16)
            return carry
        lax.fori_loop(0, NB, step, 0)

    load_w1.wait()
    load_h(ha).wait()
    matmul(hv, w1v, da, f1, mine, False)
    give_h(ha).wait()
    swap_h.start()
    keep_h.start()
    matmul(hv, w1v, da, f1, theirs, True)
    SmallReduce(me, f1, odd_land, fa1, fb1).run()
    norm(da, dzo, f1, 0)
    save_n1.start()
    keep_h.wait()
    swap_h.wait()
    swap_x1.start()
    keep_x1.start()
    load_w2a.wait()
    matmul(dzo, gw, nv, f2, body, False)
    load_w3a.start()
    SmallReduce(me, f2, even_land, fa2, fb2).run()
    norm(nv, dz, f2, 1)
    swap_x1.wait()
    swap_x2.start()
    keep_x2.start()
    load_w3a.wait()

    def z_block(j):
        res = nn(dz[...], gw[:, cols(j)]).astype(BF16)
        zd[0:ROWS, cols(j)] = res
        sv[pl.ds(j, 1)] = jnp.sum(res.astype(F32), axis=0, keepdims=True)

    def z_blocks(first):
        def step(j, carry):
            z_block(first + j)
            return carry
        lax.fori_loop(0, 2, step, 0)

    z_blocks(0)
    red0 = SmallReduce(me, sv, odd_land, sa, sb)
    red2 = SmallReduce(me, s2, even_land, sa2, sb2)
    red1 = SmallReduce(me, s1, odd_land, sa1, sb1)
    sc = Scatter(me, part, (r1, r2, r3, r4), ssem, rsem)

    def compute(u, w):
        p = lax.rem(u, SLOTS)
        if w == GRAM:
            for k in range(2):
                i, j = block_of(2 * u + k)
                part[p, k] = tn(zd[0:ROWS, cols(i)], zd[0:ROWS, cols(j)])
            return
        q = grad_unit(u)[1]
        if w == 2:
            rc = pl.ds(pl.multiple_of(q * 512, 512), 512)
            res = tn(hh[...], dz[:, rc]) + tn(ho[...], dzo[:, rc])
            part[p, 0] = res[:, 0:BLK]
            part[p, 1] = res[:, BLK:2 * BLK]
            return
        la, lb, ra, rb = ((x2h, x2o, dz, dzo), (x1h, x1o, zd, zod))[w]
        lc = pl.ds(pl.multiple_of(lax.rem(q, 2) * 512, 512), 512)
        rc = cols(q // 2)
        res = tn(la[:, lc], ra[0:ROWS, rc]) + tn(lb[:, lc], rb[:, rc])
        part[p, 0] = res[0:BLK]
        part[p, 1] = res[BLK:2 * BLK]

    def grad_unit(u):
        v = jnp.maximum(u - GRAM_UNITS, 0)
        return v // 16, lax.rem(v, 16)

    def region(u, w, k, off, n):
        q = grad_unit(u)[1]
        if w == 2:
            r0, c0 = c * 256, q * 512 + k * BLK
        else:
            r0, c0 = c * 1024 + lax.rem(q, 2) * 512 + k * BLK, (q // 2) * BLK
        return rows_at(r0 + off, n), cols_at(c0)

    grads = (g3_o, g2v, g1v)

    def keep_copy(u, k):
        own = region(u, 0, k, me.own[k], 32)
        return pltpu.make_async_copy(stage.at[lax.rem(u, 3), k], g3_o.at[own], lsem.at[k, lax.rem(u, RING)])

    def hop(e, k, inward):
        if e == 3 and inward:
            return me.keep[k], 128, me.p1
        return ((me.own[k], 32, me.last[k]), (me.near[k], 64, me.p1), (me.near[k], 64, me.p3),
                (me.far[k], 64, me.p1), (me.keep[k], 128, me.first[k]))[e]

    def spread(u, w, e, k, inward=False):
        r = lax.rem(u, RING)
        off, n, dev = hop(e, k, inward)
        if w == GRAM:
            i, j = block_of(2 * u + k)
            src = dst = gw.at[rows_at(i * BLK + off, n), cols(j)]
        else:
            dst = grads[w].at[region(u, w, k, off, n)]
            src = stage.at[lax.rem(u, 3), k] if e == 0 and w == 0 else dst
        g = 0 if w == GRAM else 1
        return rcopy(src, dst, asem.at[g, e, k, r], bsem.at[g, e, k, r], dev)

    def cross(u, w):
        r = lax.rem(u, RING)
        q = grad_unit(u)[1]
        buf = grads[w].at[unit_region(q, w, c)]
        return rcopy(buf, buf, asem.at[1, 5, 0, r], bsem.at[1, 5, 0, r], me.pc)

    def unit_region(q, w, core):
        if w == 2:
            return rows_at(core * 256, 256), pl.ds(pl.multiple_of(q * 512, 512), 512)
        return rows_at(core * 1024 + lax.rem(q, 2) * 512, 512), cols(q // 2)

    def put(u, w, own):
        reg = unit_region(grad_unit(u)[1], w, c if own else 1 - c)
        out = (None, g2_o, g1_o)[w]
        return pltpu.make_async_copy(grads[w].at[reg], out.at[reg], psem.at[0 if own else 1, lax.rem(u, RING)])

    def final(u, w):
        if w < 3:
            for k in range(2):
                piece = part[lax.rem(u, SLOTS), k, rows_at(me.own[k], 32)]
                if w == 0:
                    stage[lax.rem(u, 3), k] = piece
                    keep_copy(u, k).start()
                else:
                    rr, cc = region(u, w, k, me.own[k], 32)
                    grads[w][rr, cc] = piece
                spread(u, w, 0, k).start()
            return
        for k in range(2):
            i, j = block_of(2 * u + k)
            own = rows_at(me.own[k], 32)
            row0 = rows_at(i * BLK + me.own[k], 32)
            mu_r = g1v[rows_at(lax.rem(i, 2) * BLK + me.own[k], 32), lanes_at((i // 2) * 128)]
            mu_c = sv[pl.ds(j, 1)]
            mm = ALL_ROWS * jnp.concatenate([mu_r, mu_r], axis=1) * mu_c
            cov = (part[lax.rem(u, SLOTS), k, own] - mm) * (1.0 / (ALL_ROWS - 1))
            row = lax.broadcasted_iota(jnp.int32, (32, BLK), 0) + (i * BLK + me.own[k])
            col = lax.broadcasted_iota(jnp.int32, (32, BLK), 1) + j * BLK
            diag = row == col
            std = jnp.sqrt(jnp.where(diag, cov, 1.0) + STD_EPS)
            hinge = jnp.where(std < 1.0, VAR_WEIGHT / (2.0 * std), 0.0)
            weight = jnp.where(i == j, COV_WEIGHT, 2.0 * COV_WEIGHT)
            term = jnp.where(diag, VAR_WEIGHT * jnp.maximum(1.0 - std, 0.0), weight * cov * cov)
            lacc[...] = lacc[...] + ((term[0:8] + term[8:16]) + (term[16:24] + term[24:32]))
            gw[row0, cols(j)] = jnp.where(diag, -hinge, (2.0 * COV_WEIGHT) * cov).astype(BF16)
            spread(u, GRAM, 0, k).start()

    def diff_block(j):
        diff = zd[0:ROWS, cols(j)].astype(F32) - zod[:, cols(j)].astype(F32)
        sq = jnp.sum((diff * diff).reshape(ROWS // 8, 8, BLK), axis=0)
        lacc[...] = lacc[...] + (0.5 * INV_WEIGHT / ALL_ROWS) * sq
        da[:, cols(j)] = (2.0 * INV_WEIGHT / ALL_ROWS) * diff

    def dz_block(j):
        acc = nn(zd[...], gw[:, cols(j)])
        mean = acc[ROWS:ROWS + 1] + acc[ROWS + 1:ROWS + 2] + acc[ROWS + 2:ROWS + 3]
        dz[:, cols(j)] = (da[:, cols(j)] + (2.0 / (ALL_ROWS - 1)) * (acc[0:ROWS] - mean)).astype(BF16)

    def back_block(j, grad, st, layer):
        dx = nt(grad[0:ROWS, :], gw[cols(j)])
        nrm = nv[:, cols(j)]
        act = gains[layer][:, cols(j)] * nrm + biases[layer][:, cols(j)]
        d_act = jnp.where(act > 0.0, dx, 0.0)
        da[:, cols(j)] = d_act
        st[pl.ds(j, 1)] = jnp.sum(d_act, axis=0, keepdims=True)
        st[pl.ds(NB + j, 1)] = jnp.sum(d_act * nrm, axis=0, keepdims=True)

    def back_pre(dst, st, layer, after):
        def step(j, carry):
            scale = gains[layer][:, cols(j)] * rs[pl.ds(NB * layer + j, 1)]
            m0 = st[pl.ds(j, 1)] * (1.0 / ALL_ROWS)
            m1 = st[pl.ds(NB + j, 1)] * (1.0 / ALL_ROWS)
            dst[0:ROWS, cols(j)] = (scale * (da[:, cols(j)] - m0 - nv[:, cols(j)] * m1)).astype(BF16)
            after(j)
            return carry
        lax.fori_loop(0, NB, step, 0)

    def gather_step(e, u, w, inward):
        def each(f):
            for k in range(2):
                f(k)

        def wait_send(k):
            spread(u, w, e - 1, k, inward).wait_send()

        def wait_recv(k):
            spread(u, w, e - 1, k, inward).wait_recv()

        def begin(k):
            spread(u, w, e, k, inward).start()

        def run(sends, recvs, begins):
            if e == 1 and w == 0:
                each(lambda k: keep_copy(u, k).wait())
            if e in sends:
                each(wait_send)
            if e in recvs:
                each(wait_recv)
            if e in begins:
                each(begin)

        def at_end():
            if inward:
                run((), (4,), (4,))
            else:
                run((1, 2, 5), (1, 4, 5), (1, 4))

        def at_inner():
            if inward:
                run((1, 3, 4), (1, 3), (2, 3, 4))
            else:
                run((3, 4), (2, 3), (2, 3, 4))

        if e == 5:
            at_end()
        else:
            if e == 4 or not inward:
                pl.when(me.end)(at_end)
            if e > 1 or inward:
                pl.when(jnp.logical_not(me.end))(at_inner)
        if e == 5 and w < 3:
            cross(u, w).start()
            if w > 0:
                put(u, w, True).start()
        if e == 5 and w == GRAM:
            for k in range(2):
                i, j = block_of(2 * u + k)

                @pl.when(i != j)
                def _():
                    gw[rows_at(j * BLK, BLK), cols(i)] = gw[rows_at(i * BLK, BLK), cols(j)].T

    compute(jnp.int32(0), GRAM)

    def gather(e, u, w):
        if w == GRAM or e == 5:
            gather_step(e, u, w, False)
            return
        inward = is_inward(u)
        pl.when(jnp.logical_not(inward))(lambda: gather_step(e, u, w, False))
        pl.when(inward)(lambda: gather_step(e, u, w, True))

    def put_end(u, w):
        if w in (1, 2):
            put(u, w, False).wait()

    def cross_end(u, w):
        if w < 3:
            cross(u, w).wait()
        if w in (1, 2):
            put(u, w, True).wait()
            put(u, w, False).start()

    def means():
        mean = sv[...] * (1.0 / ALL_ROWS)
        sv[...] = mean
        hi = mean.astype(BF16)
        mid = (mean - hi.astype(F32)).astype(BF16)
        low = (mean - hi.astype(F32) - mid.astype(F32)).astype(BF16)
        for j in range(NB):
            for h in range(2):
                lanes = slice(128 * h, 128 * h + 128)
                r0, c0 = (j % 2) * BLK + 128 * h, (j // 2) * 128
                g1v[r0:r0 + 128, c0:c0 + 128] = jnp.broadcast_to(mean[j:j + 1, lanes], (128, 128)).T
            zd[ROWS:ROWS + 8, j * BLK:(j + 1) * BLK] = jnp.concatenate(
                [hi[j:j + 1], mid[j:j + 1], low[j:j + 1], jnp.zeros((5, BLK), BF16)], axis=0)

    def slots(lo, hi):
        def slot(t, carry):
            run_slot(Span(lo, hi, t), t)
            return carry
        lax.fori_loop(lo, hi, slot, 0)

    def run_slot(span, t):
        span.units(11 * LAG + 1, put_end)
        span.units(11 * LAG, cross_end)
        for e in (5, 4, 3, 2, 1):
            span.units((5 + e) * LAG, functools.partial(gather, e))
        reds = ((2, red0), (PASS_2 + SPAN_2 - 1, red2), (PASS_1 + SPAN_1 - 1, red1))
        for first, red in reds:
            @functools.partial(span.at, first + 1)
            def _(red=red):
                red.finish(0)
                red.start(1)

            @functools.partial(span.at, first + 2)
            def _(red=red):
                red.finish(1)

        @functools.partial(span.at, PASS_2 + SPAN_2)
        def _():
            load_w2.start()

        @functools.partial(span.at, PASS_2 + SPAN_2 + 1)
        def _():
            back_pre(zd, s2, 1, lambda j: swap_du2(j).start())
            load_n1.start()
            swap_s2.start()

        @functools.partial(span.at, PASS_1 + SPAN_1 + 1)
        def _():
            back_pre(dz, s1, 0, lambda j: None)
            swap_du1.start()
            swap_s1.start()

        for j, first in enumerate(DZ_SLOTS):
            span.at(first + 1, lambda j=j: swap_dz(j).wait())
        mine_now = jnp.int32(-1)
        for j, first in enumerate(DZ_SLOTS):
            if span.lo <= first < span.hi:
                mine_now = jnp.where(t == first, j, mine_now)
        if any(span.lo <= first < span.hi for first in DZ_SLOTS):
            @pl.when(mine_now >= 0)
            def _():
                dz_block(mine_now)
                swap_dz(mine_now).start()

        @functools.partial(span.at, DZ_SLOTS[-1])
        def _():
            for j in range(NB):
                load_w3(j).start()

        for e in (5, 4, 3, 2, 1):
            span.units(e * LAG, lambda u, w, e=e: sc.step(e, u, w == GRAM, lambda v: final(v, w)))
        span.units(0, lambda u, w: sc.start(u, 0))
        span.at(4, means)
        span.within(0, 3, lambda: z_blocks(2 * t + 2))

        @functools.partial(span.at, 3)
        def _():
            keep_x1.wait()
            keep_x2.wait()
            swap_x2.wait()
            save_n1.wait()
            swap_z.start()

        span.at(7, swap_z.wait)
        span.within(8, 8 + NB, lambda: diff_block(t - 8))
        @functools.partial(span.at, PASS_2)
        def _():
            s2[2 * NB:3 * NB] = lacc[...]

        @functools.partial(span.at, PASS_1)
        def _():
            load_w2.wait()
            load_n1.wait()

        @functools.partial(span.within, START_2 - 1, START_2 + 15)
        def _():
            block = (t - (START_2 - 1)) // 2

            @pl.when(t == START_2 - 1 + 2 * block)
            def _():
                swap_du2(block).wait()

        @functools.partial(span.at, START_2 + 8)
        def _():
            for cp in load_h2:
                cp.start()

        @functools.partial(span.at, START_2 + 14)
        def _():
            swap_du1.wait()
            for cp in load_h2:
                cp.wait()

        for first, width, grad, st, layer in ((PASS_2, SPAN_2, dz, s2, 1), (PASS_1, SPAN_1, zd, s1, 0)):
            @functools.partial(span.within, first, first + width)
            def _(first=first, n=-(-NB // width), grad=grad, st=st, layer=layer):
                def step(j, carry):
                    if layer == 1:
                        load_w3(j).wait()
                    back_block(j, grad, st, layer)
                    return carry
                lo = n * (t - first)
                lax.fori_loop(lo, jnp.minimum(lo + n, NB), step, 0)

        for last, red in reds:
            span.at(last, lambda red=red: red.start(0))
        span.units(-1, compute)

    for lo, hi in zip(LOOPS, LOOPS[1:]):
        slots(lo, hi)
    swap_s2.wait()
    swap_s1.wait()
    sum2, sum1 = s2[...] + e2[...], s1[...] + e1[...]
    for j in range(NB):
        lanes = slice(j * BLK, (j + 1) * BLK)
        st_o[0:1, lanes] = sum1[NB + j:NB + j + 1]
        st_o[1:2, lanes] = sum1[j:j + 1]
        st_o[2:3, lanes] = sum2[NB + j:NB + j + 1]
        st_o[3:4, lanes] = sum2[j:j + 1]
    loss_o[0, 0] = jnp.sum(sum2[2 * NB:])


def train_step(ha, hb, w1, w2, w3, g1, b1, g2, b2):
    act = pltpu.VMEM((ROWS, DIM), BF16)
    piece = pltpu.VMEM((ROWS, 1024), BF16)
    dma = pltpu.SemaphoreType.DMA
    return pl.pallas_call(
        step_kernel,
        out_shape=(sds((DIM, DIM), F32), sds((DIM, DIM), F32), sds((FEAT, DIM), F32), sds((ROWS, DIM), F32),
                   sds((ROWS, 256), BF16), sds((ROWS, 256), BF16), sds((4, DIM), F32), sds((1, 1), F32)),
        in_specs=[ANY] * 5 + [INV] * 4,
        out_specs=(ANY,) * 6 + (INV, pl.BlockSpec(memory_space=pltpu.SMEM)),
        scratch_shapes=[pltpu.VMEM((ROWS + 8, DIM), BF16), act, act, act, pltpu.VMEM((DIM, DIM), BF16),
                        piece, piece, piece, piece,
                        pltpu.VMEM((DIM, DIM), F32), pltpu.VMEM((FEAT, DIM), F32),
                        pltpu.VMEM((NB, BLK), F32), pltpu.VMEM((2 * NB, BLK), F32),
                        pltpu.VMEM((3, 2, 32, BLK), F32)]
        + scatter_scratch(SLOTS) + small_scratch(NB) + [dma((2, 3))] * 4
        + small_scratch(3 * NB) + small_scratch(2 * NB)
        + [pltpu.VMEM((2, 3, 2 * NB, BLK), F32), pltpu.VMEM((2, 3, 3 * NB, BLK), F32),
           pltpu.VMEM((3 * NB, BLK), F32), pltpu.VMEM((2 * NB, BLK), F32),
           dma((2, 6, 2, RING)), dma((2, 6, 2, RING)), dma((2, RING)),
           dma((2, RING)), dma((10,)), dma((25,)), dma((25,)), dma((NB,))],
        compiler_params=pltpu.CompilerParams(collective_id=0, has_side_effects=True, vmem_limit_bytes=VMEM_LIMIT),
        name='train_step',
    )(ha, hb, w1, w2, w3, g1, b1, g2, b2)


CHUNK = 128
BUFS = 8


def finish_kernel(g3, g2, g1, st, loss, o3, o2, o1, gain1, bias1, gain2, bias2, loss_o, buf, isem, osem, rsem):
    jobs = [(src, dst, r) for src, dst, n in ((g3, o3, DIM), (g2, o2, DIM), (g1, o1, FEAT)) for r in range(0, n, CHUNK)]

    def take(i):
        src, _, r = jobs[i]
        return pltpu.make_async_copy(src.at[pl.ds(r, CHUNK)], buf.at[i % BUFS], isem.at[i % BUFS])

    def give(i):
        _, dst, r = jobs[i]
        return pltpu.make_async_copy(buf.at[i % BUFS], dst.at[pl.ds(r, CHUNK)], osem.at[i % BUFS])

    for i in range(BUFS - 1):
        take(i).start()
    rows = [pltpu.make_async_copy(st.at[pl.ds(row, 1)], out, rsem.at[row])
            for row, out in enumerate((gain1, bias1, gain2, bias2))]
    for cp in rows:
        cp.start()
    loss_o[0, 0] = loss[0, 0]
    for i in range(len(jobs)):
        take(i).wait()
        give(i).start()
        if i + BUFS - 1 < len(jobs):
            if i > 0:
                give(i - 1).wait()
            take(i + BUFS - 1).start()
    for i in range(len(jobs) - BUFS, len(jobs)):
        give(i).wait()
    for cp in rows:
        cp.wait()


def finish(g3, g2, g1, st, loss):
    smem = pl.BlockSpec(memory_space=pltpu.SMEM)
    dma = pltpu.SemaphoreType.DMA
    return pl.pallas_call(
        finish_kernel,
        out_shape=(sds((DIM, DIM), F32), sds((DIM, DIM), F32), sds((FEAT, DIM), F32)) + (sds((1, DIM), F32),) * 4
        + (sds((1, 1), F32),),
        in_specs=[ANY] * 4 + [smem],
        out_specs=(ANY,) * 7 + (smem,),
        scratch_shapes=[pltpu.VMEM((BUFS, CHUNK, DIM), F32), dma((BUFS,)), dma((BUFS,)), dma((4,))],
        name='finish',
    )(g3, g2, g1, st, loss)


def solution(mesh):
    def local_step(h_a, h_b, w_one, w_two, w_three, gain_one, bias_one, gain_two, bias_two):
        vecs = [v.reshape(1, DIM) for v in (gain_one, bias_one, gain_two, bias_two)]
        g_three, g_two, g_one, _, _, _, st, part_loss = train_step(h_a, h_b, w_one, w_two, w_three, *vecs)
        d_three, d_two, d_one, *small, loss = finish(g_three, g_two, g_one, st, part_loss)
        return (loss.reshape(()), d_one, d_two, d_three, *[v.reshape(DIM) for v in small])

    row_spec = P('data', None)
    return jax.shard_map(local_step, mesh=mesh,
                         in_specs=(row_spec, row_spec, P(), P(), P(), P(), P(), P(), P()),
                         out_specs=(P(), P(), P(), P(), P(), P(), P(), P()),
                         check_vma=False)
```

```python
import functools

import jax
import jax.numpy as jnp
from jax import lax
from jax.experimental import pallas as pl
from jax.experimental.pallas import tpu as pltpu
from jax.sharding import PartitionSpec as P

BN_EPS = 1e-5
STD_EPS = 1e-4
INV_WEIGHT = 2.0
VAR_WEIGHT = 1.0
COV_WEIGHT = 2.0

F32 = jnp.float32
BF16 = jnp.bfloat16
MESH = pl.DeviceIdType.MESH
VMEM_LIMIT = 67043328

ROWS = 1024
HALF = 512
FEAT = 512
DIM = 2048
NB = 8
BLK = 256
LAG = 2
RING = 8
ALL_ROWS = 16384


def sds(shape, dtype):
    return jax.ShapeDtypeStruct(shape, dtype)


ANY = pl.BlockSpec(memory_space=pl.ANY)
INV = pl.BlockSpec(memory_space=pltpu.VMEM)


class Place:
    def __init__(self):
        i = lax.axis_index('data')
        self.c = lax.rem(i, 2)
        x = lax.rem(i // 2, 2)
        y = lax.rem(i // 4, 2)
        z = i // 8
        zl = lax.rem(z, 2)
        zh = z // 2
        self.pc = i + 1 - 2 * self.c
        px = i + 2 - 4 * x
        py = i + 4 - 8 * y
        p1 = i + 8 - 16 * zl
        p2 = i + 16 - 32 * zh
        pd = px + py - i
        p3 = p1 + p2 - i
        self.phases = ((px, py, pd), (p1, p2, p3))
        self.end = zl == zh
        self.p1, self.p3 = p1, p3
        self.first, self.last = (px, py), (py, px)
        self.keep = [b * 128 for b in (x, y)]
        self.send = [(1 - b) * 128 for b in (x, y)]
        self.near = [k + zh * 64 for k in self.keep]
        self.far = [k + (1 - zh) * 64 for k in self.keep]
        self.own = [n + b * 32 for n, b in zip(self.near, (y, x))]
        self.give = [n + (1 - b) * 32 for n, b in zip(self.near, (y, x))]

    def announce(self):
        sem = pltpu.get_barrier_semaphore()
        for p in (self.pc,) + self.phases[0] + self.phases[1]:
            pl.semaphore_signal(sem, inc=1, device_id=(p,), device_id_type=MESH)

    def await_all(self):
        pl.semaphore_wait(pltpu.get_barrier_semaphore(), 7)


def rcopy(src, dst, ssem, rsem, dev):
    return pltpu.make_async_remote_copy(src_ref=src, dst_ref=dst, send_sem=ssem, recv_sem=rsem,
                                        device_id=(dev,), device_id_type=MESH)


def rows_at(off, n):
    return pl.ds(pl.multiple_of(off, n), n)


def nn(a, b):
    return jnp.dot(a, b, preferred_element_type=F32)


def nt(a, b):
    return lax.dot_general(a, b, (((1,), (1,)), ((), ())), preferred_element_type=F32)


def tn(a, b):
    return lax.dot_general(a, b, (((0,), (0,)), ((), ())), preferred_element_type=F32)


def lanes_at(off):
    return pl.ds(pl.multiple_of(off, 128), 128)


def cols_at(off):
    return pl.ds(pl.multiple_of(off, BLK), BLK)


def cols(j):
    return pl.ds(pl.multiple_of(j * BLK, BLK), BLK)


def is_inward(u):
    return (u >= GRAM_UNITS) & (lax.rem(jnp.maximum(u - GRAM_UNITS, 0), 4) == 0)


class Scatter:
    def __init__(self, place, part, lands, ssem, rsem):
        self.pl, self.part, self.lands, self.ssem, self.rsem = place, part, lands, ssem, rsem

    def landing(self, u, e, k, n):
        v = jnp.maximum(u - GRAM_UNITS, 0)
        q, r = v // 4, lax.rem(v, 4)
        gram = u < GRAM_UNITS
        if e in (0, 2):
            return self.lands[e].at[lax.rem(u, 4), k]
        if e == 4:
            turn = jnp.where(gram, u, jnp.where(r == 0, q, v - 1 - q))
            return self.lands[3].at[lax.rem(turn, 4), k]
        off = jnp.where(gram, lax.rem(u, 8) * 64, lax.rem(q, 2) * 320 + jnp.where(r == 0, 0, 64 + r * 64))
        return self.lands[1].at[k, pl.ds(pl.multiple_of(off, 64), n)]

    def copy(self, u, e, k, inward=False):
        me = self.pl
        off, n, dev = ((me.send[k], 128, me.first[k]), (me.far[k], 64, me.p1), (me.far[k], 64, me.p3),
                       (me.near[k], 64, me.p1), (me.give[k], 32, me.last[k]))[e]
        if e == 1 and inward:
            off, n = me.keep[k], 128
        r = lax.rem(u, RING)
        return rcopy(self.part.at[lax.rem(u, SLOTS), k, pl.ds(pl.multiple_of(off, 32), n)], self.landing(u, e, k, n),
                     self.ssem.at[e, k, r], self.rsem.at[e, k, r], dev)

    def start(self, u, e, inward=False):
        for k in range(2):
            self.copy(u, e, k, inward).start()

    def sent(self, u, e, inward=False):
        for k in range(2):
            self.copy(u, e, k, inward).wait_send()

    def add(self, u, e, off, inward=False):
        p, n = lax.rem(u, SLOTS), 128 if inward else (128, 64, 64, 64, 32)[e]
        for k in range(2):
            self.copy(u, e, k, inward).wait_recv()
            rr = pl.ds(pl.multiple_of(off[k], 32), n)
            self.part[p, k, rr] = self.part[p, k, rr] + self.landing(u, e, k, n)[...]

    def step(self, e, u, gram, final):
        me = self.pl
        if gram:
            owner, passes = me.end, jnp.logical_not(me.end)
        else:
            inward = is_inward(u)
            owner, passes = me.end != inward, jnp.logical_not(me.end) & jnp.logical_not(inward)
        variants = (False,) if gram else (False, True)

        def of(variant):
            return me.end if gram else me.end & (inward if variant else jnp.logical_not(inward))

        if e == 1:
            self.sent(u, 0)
            self.add(u, 0, me.keep)
            for v in variants:
                pl.when(of(v))(functools.partial(self.start, u, 1, v))
        if e == 2:
            for v in variants:
                pl.when(of(v))(functools.partial(self.sent, u, 1, v))

            @pl.when(jnp.logical_not(me.end))
            def _():
                for v in variants:
                    def gather(v=v):
                        self.add(u, 1, me.keep if v else me.far, v)
                    if gram:
                        gather()
                    else:
                        pl.when(inward if v else jnp.logical_not(inward))(gather)
                self.start(u, 2)
        if e == 3:
            @pl.when(jnp.logical_not(me.end))
            def _():
                self.sent(u, 2)
                self.add(u, 2, me.near)

            pl.when(passes)(functools.partial(self.start, u, 3))
        if e == 4:
            pl.when(of(False))(functools.partial(self.add, u, 3, me.near))
            pl.when(owner)(functools.partial(self.start, u, 4))
            pl.when(passes)(functools.partial(self.sent, u, 3))
        if e == 5:
            @pl.when(owner)
            def _():
                self.sent(u, 4)
                self.add(u, 4, me.own)
                final(u)


class Span:
    def __init__(self, lo, hi, t):
        self.lo, self.hi, self.t = lo, hi, t

    def at(self, slot, f):
        if self.lo <= slot < self.hi:
            pl.when(self.t == slot)(f)

    def within(self, first, stop, f):
        if max(first, self.lo) >= min(stop, self.hi):
            return
        conds = ([] if first <= self.lo else [self.t >= first]) + ([] if stop >= self.hi else [self.t < stop])
        if not conds:
            f()
        else:
            pl.when(conds[0] if len(conds) == 1 else conds[0] & conds[1])(f)

    def units(self, lag, f):
        for w, first, stop, base in ((GRAM, 0, GRAM_UNITS, 0), (0, START_3, START_3 + 16, 18),
                                     (1, START_2, START_2 + 16, 34), (2, START_2 + 16, START_2 + 20, 50)):
            u = self.t - (lag + first - base)
            self.within(first + lag, stop + lag, functools.partial(f, u, w))


def scatter_scratch(slots):
    return [pltpu.VMEM((slots, 2, BLK, BLK), F32), pltpu.VMEM((4, 2, 128, BLK), F32),
            pltpu.VMEM((2, 640, BLK), F32), pltpu.VMEM((4, 2, 64, BLK), F32), pltpu.VMEM((4, 2, 32, BLK), F32),
            pltpu.SemaphoreType.DMA((5, 2, RING)), pltpu.SemaphoreType.DMA((5, 2, RING))]


class SmallReduce:
    def __init__(self, place, val, land, ssem, rsem, row=0):
        self.pl, self.val, self.ssem, self.rsem = place, val, ssem, rsem
        self.land = land.at[:, :, pl.ds(row, val.shape[0])]

    def copies(self, ph):
        return [rcopy(self.val, self.land.at[ph, k], self.ssem.at[ph, k], self.rsem.at[ph, k], p)
                for k, p in enumerate(self.pl.phases[ph])]

    def start(self, ph):
        for cp in self.copies(ph):
            cp.start()

    def finish(self, ph):
        for cp in self.copies(ph):
            cp.wait()
        land = self.land
        self.val[...] = (self.val[...] + land[ph, 0]) + (land[ph, 1] + land[ph, 2])


def small_scratch(n):
    return [pltpu.VMEM((n, BLK), F32), pltpu.SemaphoreType.DMA((2, 3)), pltpu.SemaphoreType.DMA((2, 3))]


GRAM_UNITS = 18
GRAM = 3
UNITS = 54
SLOTS = 5 * LAG + 1
START_3 = 28
START_2 = 44
END = START_2 + 21 + 11 * LAG
LOOPS = (0, 18, 39, 54, 66, END)
DZ_SLOTS = (23, 27, 30, 32, 34, 36, 37, 38)
PASS_2 = 39
PASS_1 = 45
SPAN_2, SPAN_1 = 3, 4


def block_of(q):
    i = jnp.int32(0)
    for first in (8, 15, 21, 26, 30, 33, 35):
        i = i + jnp.where(q >= first, 1, 0)
    return i, i + q - (17 * i - i * i) // 2


def step_kernel(ha, hb, w1, w2, w3, g1, b1, g2, b2, g3_o, g2_o, g1_o, n1_o, h_o, ho_o, st_o, loss_o,
                zd, zod, dz, dzo, gw, x2h, x2o, x1h, x1o, g2v, g1v, lacc, rs, stage,
                part, r1, r2, r3, r4, ssem, rsem, sv, sa, sb, fa1, fb1, fa2, fb2,
                s2, sa2, sb2, s1, sa1, sb1, odd_land, even_land, e2, e1,
                asem, bsem, lsem, psem, csem, dsem, esem, wsem):
    me = Place()
    me.announce()
    c = me.c
    nv, da = g2v.at[pl.ds(0, ROWS)], g2v.at[pl.ds(ROWS, ROWS)]
    hv = x2o.at[:, pl.ds(0, FEAT)]
    f1, f2 = [[st.at[pl.ds(h * NB, NB)] for h in range(2)] for st in (s1, s2)]
    gains, biases = (g1, g2), (b1, b2)
    half = pl.ds(pl.multiple_of(c * 1024, 1024), 1024)
    ohalf = pl.ds(pl.multiple_of((1 - c) * 1024, 1024), 1024)
    hhalf = pl.ds(pl.multiple_of(c * 256, 256), 256)
    hohalf = pl.ds(pl.multiple_of((1 - c) * 256, 256), 256)
    mine = pl.ds(pl.multiple_of(c * HALF, HALF), HALF)
    theirs = pl.ds(pl.multiple_of((1 - c) * HALF, HALF), HALF)
    body = pl.ds(0, ROWS)
    w1v = zod.at[pl.ds(0, FEAT)]
    load_w1 = pltpu.make_async_copy(w1, w1v, csem.at[0])
    load_w2a = pltpu.make_async_copy(w2, gw, csem.at[1])
    load_w3a = [pltpu.make_async_copy(w3.at[pl.ds(r, 1024)], gw.at[pl.ds(r, 1024)], csem.at[k])
                for r, k in ((0, 2), (1024, 4))]
    load_w2 = pltpu.make_async_copy(w2, gw, csem.at[6])
    load_n1 = pltpu.make_async_copy(n1_o, nv, csem.at[7])
    save_n1 = pltpu.make_async_copy(da, n1_o, csem.at[8])
    keep_x1 = pltpu.make_async_copy(dzo.at[:, half], x1h, csem.at[3])
    keep_h = pltpu.make_async_copy(hv.at[:, hhalf], h_o, csem.at[5])
    hh, ho = x2h.at[:, pl.ds(0, 256)], x2o.at[:, pl.ds(0, 256)]
    load_h2 = [pltpu.make_async_copy(h_o, hh, csem.at[5]), pltpu.make_async_copy(ho_o, ho, csem.at[2])]
    keep_x2 = pltpu.make_async_copy(dz.at[:, half], x2h, csem.at[10])
    swap_z = rcopy(zd.at[body], zod, dsem.at[0], esem.at[0], me.pc)
    swap_x2 = rcopy(dz.at[:, ohalf], x2o, dsem.at[1], esem.at[1], me.pc)
    swap_x1 = rcopy(dzo.at[:, ohalf], x1o, dsem.at[2], esem.at[2], me.pc)
    swap_h = rcopy(hv.at[:, hohalf], ho_o, dsem.at[3], esem.at[3], me.pc)
    swap_du1 = rcopy(dz, dzo, dsem.at[5], esem.at[5], me.pc)
    swap_s2 = rcopy(s2, e2, dsem.at[6], esem.at[6], me.pc)
    swap_s1 = rcopy(s1, e1, dsem.at[7], esem.at[7], me.pc)

    def load_h(src):
        return pltpu.make_async_copy(src, hv.at[mine], csem.at[9])

    def give_h(src):
        return rcopy(src, hv.at[mine], dsem.at[16], esem.at[16], me.pc)

    def load_w3(j):
        return pltpu.make_async_copy(w3.at[cols(j)], gw.at[cols(j)], wsem.at[j])

    def swap_du2(j):
        return rcopy(zd.at[body, cols(j)], zod.at[:, cols(j)], dsem.at[17 + j], esem.at[17 + j], me.pc)

    def swap_dz(j):
        return rcopy(dz.at[:, cols(j)], dzo.at[:, cols(j)], dsem.at[8 + j], esem.at[8 + j], me.pc)

    for k, own in ((0, ha), (1, hb)):
        @pl.when(c == k)
        def _(own=own):
            load_h(own).start()
    load_w1.start()
    me.await_all()
    for k, other in ((0, hb), (1, ha)):
        @pl.when(c == k)
        def _(other=other):
            give_h(other).start()
    load_w2a.start()
    lacc[...] = jnp.zeros_like(lacc)

    def matmul(src, w, dst, rows, depth, first, stop, st=None, add=False):
        def step(j, carry):
            res = nn(src[rows, depth], w[depth, cols(j)])
            if add == 'depth':
                res = res + dst[rows, cols(j)]
            dst[rows, cols(j)] = res
            if st is not None:
                one = jnp.sum(res, axis=0, keepdims=True)
                two = jnp.sum(res * res, axis=0, keepdims=True)
                k = lax.rem(j, 4)
                if add == 'rows':
                    one = one + st[pl.ds(k, 1)]
                    two = two + st[pl.ds(4 + k, 1)]
                st[pl.ds(k, 1)] = one
                st[pl.ds(4 + k, 1)] = two
            return carry
        lax.fori_loop(first, stop, step, 0)

    def norm(u, x, st, layer, h):
        mean = st[0:4] * (1.0 / ALL_ROWS)
        var = st[4:8] * (1.0 / ALL_ROWS) - mean * mean
        inv = lax.rsqrt(var + BN_EPS)
        st[0:4] = mean
        st[4:8] = inv
        rs[NB * layer + 4 * h:NB * layer + 4 * h + 4] = inv

        def step(j, carry):
            k = j - 4 * h
            nrm = (u[:, cols(j)] - st[pl.ds(k, 1)]) * st[pl.ds(4 + k, 1)]
            act = gains[layer][:, cols(j)] * nrm + biases[layer][:, cols(j)]
            u[:, cols(j)] = nrm
            x[:, cols(j)] = jnp.maximum(act, 0.0).astype(BF16)
            return carry
        lax.fori_loop(4 * h, 4 * h + 4, step, 0)

    low, high, full = pl.ds(0, 1024), pl.ds(1024, 1024), pl.ds(0, DIM)
    all_f = pl.ds(0, FEAT)
    red_f1 = [SmallReduce(me, f1[h], odd_land, fa1.at[h], fb1.at[h], h * NB) for h in range(2)]
    red_f2 = [SmallReduce(me, f2[h], even_land, fa2.at[h], fb2.at[h], h * NB) for h in range(2)]
    load_w1.wait()
    load_h(ha).wait()
    give_h(ha).wait()
    swap_h.start()
    keep_h.start()
    for h in range(2):
        matmul(hv, w1v, da, body, all_f, 4 * h, 4 * h + 4, f1[h])
        red_f1[h].start(0)
    for h in range(2):
        red_f1[h].finish(0)
        red_f1[h].start(1)
    red_f1[0].finish(1)
    norm(da, dzo, f1[0], 0, 0)
    load_w2a.wait()
    matmul(dzo, gw, nv, body, low, 0, NB)
    red_f1[1].finish(1)
    norm(da, dzo, f1[1], 0, 1)
    matmul(dzo, gw, nv, body, high, 0, 4, f2[0], 'depth')
    red_f2[0].start(0)
    save_n1.start()
    keep_h.wait()
    swap_h.wait()
    swap_x1.start()
    keep_x1.start()
    matmul(dzo, gw, nv, body, high, 4, 6, f2[1], 'depth')
    red_f2[0].finish(0)
    red_f2[0].start(1)
    matmul(dzo, gw, nv, body, high, 6, NB, f2[1], 'depth')
    red_f2[1].start(0)
    for cp in load_w3a:
        cp.start()
    red_f2[0].finish(1)
    norm(nv, dz, f2[0], 1, 0)
    red_f2[1].finish(0)
    red_f2[1].start(1)
    save_n1.wait()
    load_w3a[0].wait()
    matmul(dz, gw, da, body, low, 0, 4)
    red_f2[1].finish(1)
    norm(nv, dz, f2[1], 1, 1)
    swap_x1.wait()
    swap_x2.start()
    keep_x2.start()
    load_w3a[1].wait()

    def z_block(j, part_done):
        if part_done:
            res = (da[:, cols(j)] + nn(dz[:, high], gw[high, cols(j)])).astype(BF16)
        else:
            res = nn(dz[...], gw[:, cols(j)]).astype(BF16)
        zd[0:ROWS, cols(j)] = res
        sv[pl.ds(j, 1)] = jnp.sum(res.astype(F32), axis=0, keepdims=True)

    def z_blocks(first, part_done):
        def step(j, carry):
            z_block(first + j, part_done)
            return carry
        lax.fori_loop(0, 2, step, 0)

    z_blocks(0, True)
    red0 = SmallReduce(me, sv, odd_land, sa, sb)
    red2 = SmallReduce(me, s2, even_land, sa2, sb2)
    red1 = SmallReduce(me, s1, odd_land, sa1, sb1)
    sc = Scatter(me, part, (r1, r2, r3, r4), ssem, rsem)

    def compute(u, w):
        p = lax.rem(u, SLOTS)
        if w == GRAM:
            for k in range(2):
                i, j = block_of(2 * u + k)
                part[p, k] = tn(zd[0:ROWS, cols(i)], zd[0:ROWS, cols(j)])
            return
        q = grad_unit(u)[1]
        if w == 2:
            rc = pl.ds(pl.multiple_of(q * 512, 512), 512)
            res = tn(hh[...], dz[:, rc]) + tn(ho[...], dzo[:, rc])
            part[p, 0] = res[:, 0:BLK]
            part[p, 1] = res[:, BLK:2 * BLK]
            return
        la, lb, ra, rb = ((x2h, x2o, dz, dzo), (x1h, x1o, zd, zod))[w]
        lc = pl.ds(pl.multiple_of(lax.rem(q, 2) * 512, 512), 512)
        rc = cols(q // 2)
        res = tn(la[:, lc], ra[0:ROWS, rc]) + tn(lb[:, lc], rb[:, rc])
        part[p, 0] = res[0:BLK]
        part[p, 1] = res[BLK:2 * BLK]

    def grad_unit(u):
        v = jnp.maximum(u - GRAM_UNITS, 0)
        return v // 16, lax.rem(v, 16)

    def region(u, w, k, off, n):
        q = grad_unit(u)[1]
        if w == 2:
            r0, c0 = c * 256, q * 512 + k * BLK
        else:
            r0, c0 = c * 1024 + lax.rem(q, 2) * 512 + k * BLK, (q // 2) * BLK
        return rows_at(r0 + off, n), cols_at(c0)

    grads = (g3_o, g2v, g1v)

    def keep_copy(u, k):
        own = region(u, 0, k, me.own[k], 32)
        return pltpu.make_async_copy(stage.at[lax.rem(u, 3), k], g3_o.at[own], lsem.at[k, lax.rem(u, RING)])

    def hop(e, k, inward):
        if e == 3 and inward:
            return me.keep[k], 128, me.p1
        return ((me.own[k], 32, me.last[k]), (me.near[k], 64, me.p1), (me.near[k], 64, me.p3),
                (me.far[k], 64, me.p1), (me.keep[k], 128, me.first[k]))[e]

    def spread(u, w, e, k, inward=False):
        r = lax.rem(u, RING)
        off, n, dev = hop(e, k, inward)
        if w == GRAM:
            i, j = block_of(2 * u + k)
            src = dst = gw.at[rows_at(i * BLK + off, n), cols(j)]
        else:
            dst = grads[w].at[region(u, w, k, off, n)]
            src = stage.at[lax.rem(u, 3), k] if e == 0 and w == 0 else dst
        g = 0 if w == GRAM else 1
        return rcopy(src, dst, asem.at[g, e, k, r], bsem.at[g, e, k, r], dev)

    def cross(u, w):
        r = lax.rem(u, RING)
        q = grad_unit(u)[1]
        buf = grads[w].at[unit_region(q, w, c)]
        return rcopy(buf, buf, asem.at[1, 5, 0, r], bsem.at[1, 5, 0, r], me.pc)

    def unit_region(q, w, core):
        if w == 2:
            return rows_at(core * 256, 256), pl.ds(pl.multiple_of(q * 512, 512), 512)
        return rows_at(core * 1024 + lax.rem(q, 2) * 512, 512), cols(q // 2)

    def put(u, w, own):
        reg = unit_region(grad_unit(u)[1], w, c if own else 1 - c)
        out = (None, g2_o, g1_o)[w]
        return pltpu.make_async_copy(grads[w].at[reg], out.at[reg], psem.at[0 if own else 1, lax.rem(u, RING)])

    def final(u, w):
        if w < 3:
            for k in range(2):
                piece = part[lax.rem(u, SLOTS), k, rows_at(me.own[k], 32)]
                if w == 0:
                    stage[lax.rem(u, 3), k] = piece
                    keep_copy(u, k).start()
                else:
                    rr, cc = region(u, w, k, me.own[k], 32)
                    grads[w][rr, cc] = piece
                spread(u, w, 0, k).start()
            return
        for k in range(2):
            i, j = block_of(2 * u + k)
            own = rows_at(me.own[k], 32)
            row0 = rows_at(i * BLK + me.own[k], 32)
            mu_r = g1v[rows_at(lax.rem(i, 2) * BLK + me.own[k], 32), lanes_at((i // 2) * 128)]
            mu_c = sv[pl.ds(j, 1)]
            mm = ALL_ROWS * jnp.concatenate([mu_r, mu_r], axis=1) * mu_c
            cov = (part[lax.rem(u, SLOTS), k, own] - mm) * (1.0 / (ALL_ROWS - 1))
            row = lax.broadcasted_iota(jnp.int32, (32, BLK), 0) + (i * BLK + me.own[k])
            col = lax.broadcasted_iota(jnp.int32, (32, BLK), 1) + j * BLK
            diag = row == col
            std = jnp.sqrt(jnp.where(diag, cov, 1.0) + STD_EPS)
            hinge = jnp.where(std < 1.0, VAR_WEIGHT / (2.0 * std), 0.0)
            weight = jnp.where(i == j, COV_WEIGHT, 2.0 * COV_WEIGHT)
            term = jnp.where(diag, VAR_WEIGHT * jnp.maximum(1.0 - std, 0.0), weight * cov * cov)
            lacc[...] = lacc[...] + ((term[0:8] + term[8:16]) + (term[16:24] + term[24:32]))
            gw[row0, cols(j)] = jnp.where(diag, -hinge, (2.0 * COV_WEIGHT) * cov).astype(BF16)
            spread(u, GRAM, 0, k).start()

    def diff_block(j):
        diff = zd[0:ROWS, cols(j)].astype(F32) - zod[:, cols(j)].astype(F32)
        sq = jnp.sum((diff * diff).reshape(ROWS // 8, 8, BLK), axis=0)
        lacc[...] = lacc[...] + (0.5 * INV_WEIGHT / ALL_ROWS) * sq
        da[:, cols(j)] = (2.0 * INV_WEIGHT / ALL_ROWS) * diff

    def dz_block(j):
        acc = nn(zd[...], gw[:, cols(j)])
        mean = acc[ROWS:ROWS + 1] + acc[ROWS + 1:ROWS + 2] + acc[ROWS + 2:ROWS + 3]
        dz[:, cols(j)] = (da[:, cols(j)] + (2.0 / (ALL_ROWS - 1)) * (acc[0:ROWS] - mean)).astype(BF16)

    def back_block(j, grad, st, layer):
        dx = nt(grad[0:ROWS, :], gw[cols(j)])
        nrm = nv[:, cols(j)]
        act = gains[layer][:, cols(j)] * nrm + biases[layer][:, cols(j)]
        d_act = jnp.where(act > 0.0, dx, 0.0)
        da[:, cols(j)] = d_act
        st[pl.ds(j, 1)] = jnp.sum(d_act, axis=0, keepdims=True)
        st[pl.ds(NB + j, 1)] = jnp.sum(d_act * nrm, axis=0, keepdims=True)

    def back_pre(dst, st, layer, after):
        def step(j, carry):
            scale = gains[layer][:, cols(j)] * rs[pl.ds(NB * layer + j, 1)]
            m0 = st[pl.ds(j, 1)] * (1.0 / ALL_ROWS)
            m1 = st[pl.ds(NB + j, 1)] * (1.0 / ALL_ROWS)
            dst[0:ROWS, cols(j)] = (scale * (da[:, cols(j)] - m0 - nv[:, cols(j)] * m1)).astype(BF16)
            after(j)
            return carry
        lax.fori_loop(0, NB, step, 0)

    def gather_step(e, u, w, inward):
        def each(f):
            for k in range(2):
                f(k)

        def wait_send(k):
            spread(u, w, e - 1, k, inward).wait_send()

        def wait_recv(k):
            spread(u, w, e - 1, k, inward).wait_recv()

        def begin(k):
            spread(u, w, e, k, inward).start()

        def run(sends, recvs, begins):
            if e == 1 and w == 0:
                each(lambda k: keep_copy(u, k).wait())
            if e in sends:
                each(wait_send)
            if e in recvs:
                each(wait_recv)
            if e in begins:
                each(begin)

        def at_end():
            if inward:
                run((), (4,), (4,))
            else:
                run((1, 2, 5), (1, 4, 5), (1, 4))

        def at_inner():
            if inward:
                run((1, 3, 4), (1, 3), (2, 3, 4))
            else:
                run((3, 4), (2, 3), (2, 3, 4))

        if e == 5:
            at_end()
        else:
            if e == 4 or not inward:
                pl.when(me.end)(at_end)
            if e > 1 or inward:
                pl.when(jnp.logical_not(me.end))(at_inner)
        if e == 5 and w < 3:
            cross(u, w).start()
            if w > 0:
                put(u, w, True).start()
        if e == 5 and w == GRAM:
            for k in range(2):
                i, j = block_of(2 * u + k)

                @pl.when(i != j)
                def _():
                    gw[rows_at(j * BLK, BLK), cols(i)] = gw[rows_at(i * BLK, BLK), cols(j)].T

    compute(jnp.int32(0), GRAM)

    def gather(e, u, w):
        if w == GRAM or e == 5:
            gather_step(e, u, w, False)
            return
        inward = is_inward(u)
        pl.when(jnp.logical_not(inward))(lambda: gather_step(e, u, w, False))
        pl.when(inward)(lambda: gather_step(e, u, w, True))

    def put_end(u, w):
        if w in (1, 2):
            put(u, w, False).wait()

    def cross_end(u, w):
        if w < 3:
            cross(u, w).wait()
        if w in (1, 2):
            put(u, w, True).wait()
            put(u, w, False).start()

    def means():
        mean = sv[...] * (1.0 / ALL_ROWS)
        sv[...] = mean
        hi = mean.astype(BF16)
        mid = (mean - hi.astype(F32)).astype(BF16)
        low = (mean - hi.astype(F32) - mid.astype(F32)).astype(BF16)
        for j in range(NB):
            for h in range(2):
                lanes = slice(128 * h, 128 * h + 128)
                r0, c0 = (j % 2) * BLK + 128 * h, (j // 2) * 128
                g1v[r0:r0 + 128, c0:c0 + 128] = jnp.broadcast_to(mean[j:j + 1, lanes], (128, 128)).T
            zd[ROWS:ROWS + 8, j * BLK:(j + 1) * BLK] = jnp.concatenate(
                [hi[j:j + 1], mid[j:j + 1], low[j:j + 1], jnp.zeros((5, BLK), BF16)], axis=0)

    def slots(lo, hi):
        def slot(t, carry):
            run_slot(Span(lo, hi, t), t)
            return carry
        lax.fori_loop(lo, hi, slot, 0)

    def run_slot(span, t):
        span.units(11 * LAG + 1, put_end)
        span.units(11 * LAG, cross_end)
        for e in (5, 4, 3, 2, 1):
            span.units((5 + e) * LAG, functools.partial(gather, e))
        reds = ((2, red0), (PASS_2 + SPAN_2 - 1, red2), (PASS_1 + SPAN_1 - 1, red1))
        for first, red in reds:
            @functools.partial(span.at, first + 1)
            def _(red=red):
                red.finish(0)
                red.start(1)

            @functools.partial(span.at, first + 2)
            def _(red=red):
                red.finish(1)

        @functools.partial(span.at, PASS_2 + SPAN_2)
        def _():
            load_w2.start()

        @functools.partial(span.at, PASS_2 + SPAN_2 + 1)
        def _():
            back_pre(zd, s2, 1, lambda j: swap_du2(j).start())
            load_n1.start()
            swap_s2.start()

        @functools.partial(span.at, PASS_1 + SPAN_1 + 1)
        def _():
            back_pre(dz, s1, 0, lambda j: None)
            swap_du1.start()
            swap_s1.start()

        for j, first in enumerate(DZ_SLOTS):
            span.at(first + 1, lambda j=j: swap_dz(j).wait())
        mine_now = jnp.int32(-1)
        for j, first in enumerate(DZ_SLOTS):
            if span.lo <= first < span.hi:
                mine_now = jnp.where(t == first, j, mine_now)
        if any(span.lo <= first < span.hi for first in DZ_SLOTS):
            @pl.when(mine_now >= 0)
            def _():
                dz_block(mine_now)
                swap_dz(mine_now).start()

        @functools.partial(span.at, DZ_SLOTS[-1])
        def _():
            for j in range(NB):
                load_w3(j).start()

        for e in (5, 4, 3, 2, 1):
            span.units(e * LAG, lambda u, w, e=e: sc.step(e, u, w == GRAM, lambda v: final(v, w)))
        span.units(0, lambda u, w: sc.start(u, 0))
        span.at(4, means)
        span.at(0, lambda: z_blocks(2, True))
        span.within(1, 3, lambda: z_blocks(2 * t + 2, False))

        @functools.partial(span.at, 3)
        def _():
            keep_x1.wait()
            keep_x2.wait()
            swap_x2.wait()
            swap_z.start()

        span.at(7, swap_z.wait)
        span.within(8, 8 + NB, lambda: diff_block(t - 8))
        @functools.partial(span.at, PASS_2)
        def _():
            s2[2 * NB:3 * NB] = lacc[...]

        @functools.partial(span.at, PASS_1)
        def _():
            load_w2.wait()
            load_n1.wait()

        @functools.partial(span.within, START_2 - 1, START_2 + 15)
        def _():
            block = (t - (START_2 - 1)) // 2

            @pl.when(t == START_2 - 1 + 2 * block)
            def _():
                swap_du2(block).wait()

        @functools.partial(span.at, START_2 + 8)
        def _():
            for cp in load_h2:
                cp.start()

        @functools.partial(span.at, START_2 + 14)
        def _():
            swap_du1.wait()
            for cp in load_h2:
                cp.wait()

        for first, width, grad, st, layer in ((PASS_2, SPAN_2, dz, s2, 1), (PASS_1, SPAN_1, zd, s1, 0)):
            @functools.partial(span.within, first, first + width)
            def _(first=first, n=-(-NB // width), grad=grad, st=st, layer=layer):
                def step(j, carry):
                    if layer == 1:
                        load_w3(j).wait()
                    back_block(j, grad, st, layer)
                    return carry
                lo = n * (t - first)
                lax.fori_loop(lo, jnp.minimum(lo + n, NB), step, 0)

        for last, red in reds:
            span.at(last, lambda red=red: red.start(0))
        span.units(-1, compute)

    for lo, hi in zip(LOOPS, LOOPS[1:]):
        slots(lo, hi)
    swap_s2.wait()
    swap_s1.wait()
    sum2, sum1 = s2[...] + e2[...], s1[...] + e1[...]
    for j in range(NB):
        lanes = slice(j * BLK, (j + 1) * BLK)
        st_o[0:1, lanes] = sum1[NB + j:NB + j + 1]
        st_o[1:2, lanes] = sum1[j:j + 1]
        st_o[2:3, lanes] = sum2[NB + j:NB + j + 1]
        st_o[3:4, lanes] = sum2[j:j + 1]
    loss_o[0, 0] = jnp.sum(sum2[2 * NB:])


def train_step(ha, hb, w1, w2, w3, g1, b1, g2, b2):
    act = pltpu.VMEM((ROWS, DIM), BF16)
    piece = pltpu.VMEM((ROWS, 1024), BF16)
    dma = pltpu.SemaphoreType.DMA
    return pl.pallas_call(
        step_kernel,
        out_shape=(sds((DIM, DIM), F32), sds((DIM, DIM), F32), sds((FEAT, DIM), F32), sds((ROWS, DIM), F32),
                   sds((ROWS, 256), BF16), sds((ROWS, 256), BF16), sds((4, DIM), F32), sds((1, 1), F32)),
        in_specs=[ANY] * 5 + [INV] * 4,
        out_specs=(ANY,) * 6 + (INV, pl.BlockSpec(memory_space=pltpu.SMEM)),
        scratch_shapes=[pltpu.VMEM((ROWS + 8, DIM), BF16), act, act, act, pltpu.VMEM((DIM, DIM), BF16),
                        piece, piece, piece, piece,
                        pltpu.VMEM((DIM, DIM), F32), pltpu.VMEM((FEAT, DIM), F32),
                        pltpu.VMEM((NB, BLK), F32), pltpu.VMEM((2 * NB, BLK), F32),
                        pltpu.VMEM((3, 2, 32, BLK), F32)]
        + scatter_scratch(SLOTS) + small_scratch(NB) + [dma((2, 2, 3))] * 4
        + small_scratch(3 * NB) + small_scratch(2 * NB)
        + [pltpu.VMEM((2, 3, 2 * NB, BLK), F32), pltpu.VMEM((2, 3, 3 * NB, BLK), F32),
           pltpu.VMEM((3 * NB, BLK), F32), pltpu.VMEM((2 * NB, BLK), F32),
           dma((2, 6, 2, RING)), dma((2, 6, 2, RING)), dma((2, RING)),
           dma((2, RING)), dma((11,)), dma((25,)), dma((25,)), dma((NB,))],
        compiler_params=pltpu.CompilerParams(collective_id=0, has_side_effects=True, vmem_limit_bytes=VMEM_LIMIT),
        name='train_step',
    )(ha, hb, w1, w2, w3, g1, b1, g2, b2)


CHUNK = 128
BUFS = 8


def finish_kernel(g3, g2, g1, st, loss, o3, o2, o1, gain1, bias1, gain2, bias2, loss_o, buf, isem, osem, rsem):
    jobs = [(src, dst, r) for src, dst, n in ((g3, o3, DIM), (g2, o2, DIM), (g1, o1, FEAT)) for r in range(0, n, CHUNK)]

    def take(i):
        src, _, r = jobs[i]
        return pltpu.make_async_copy(src.at[pl.ds(r, CHUNK)], buf.at[i % BUFS], isem.at[i % BUFS])

    def give(i):
        _, dst, r = jobs[i]
        return pltpu.make_async_copy(buf.at[i % BUFS], dst.at[pl.ds(r, CHUNK)], osem.at[i % BUFS])

    for i in range(BUFS - 1):
        take(i).start()
    rows = [pltpu.make_async_copy(st.at[pl.ds(row, 1)], out, rsem.at[row])
            for row, out in enumerate((gain1, bias1, gain2, bias2))]
    for cp in rows:
        cp.start()
    loss_o[0, 0] = loss[0, 0]
    for i in range(len(jobs)):
        take(i).wait()
        give(i).start()
        if i + BUFS - 1 < len(jobs):
            if i > 0:
                give(i - 1).wait()
            take(i + BUFS - 1).start()
    for i in range(len(jobs) - BUFS, len(jobs)):
        give(i).wait()
    for cp in rows:
        cp.wait()


def finish(g3, g2, g1, st, loss):
    smem = pl.BlockSpec(memory_space=pltpu.SMEM)
    dma = pltpu.SemaphoreType.DMA
    return pl.pallas_call(
        finish_kernel,
        out_shape=(sds((DIM, DIM), F32), sds((DIM, DIM), F32), sds((FEAT, DIM), F32)) + (sds((1, DIM), F32),) * 4
        + (sds((1, 1), F32),),
        in_specs=[ANY] * 4 + [smem],
        out_specs=(ANY,) * 7 + (smem,),
        scratch_shapes=[pltpu.VMEM((BUFS, CHUNK, DIM), F32), dma((BUFS,)), dma((BUFS,)), dma((4,))],
        name='finish',
    )(g3, g2, g1, st, loss)


def solution(mesh):
    def local_step(h_a, h_b, w_one, w_two, w_three, gain_one, bias_one, gain_two, bias_two):
        vecs = [v.reshape(1, DIM) for v in (gain_one, bias_one, gain_two, bias_two)]
        g_three, g_two, g_one, _, _, _, st, part_loss = train_step(h_a, h_b, w_one, w_two, w_three, *vecs)
        d_three, d_two, d_one, *small, loss = finish(g_three, g_two, g_one, st, part_loss)
        return (loss.reshape(()), d_one, d_two, d_three, *[v.reshape(DIM) for v in small])

    row_spec = P('data', None)
    return jax.shard_map(local_step, mesh=mesh,
                         in_specs=(row_spec, row_spec, P(), P(), P(), P(), P(), P(), P()),
                         out_specs=(P(), P(), P(), P(), P(), P(), P(), P()),
                         check_vma=False)
```

```python
import functools

import jax
import jax.numpy as jnp
from jax import lax
from jax.experimental import pallas as pl
from jax.experimental.pallas import tpu as pltpu
from jax.sharding import PartitionSpec as P

BN_EPS = 1e-5
STD_EPS = 1e-4
INV_WEIGHT = 2.0
VAR_WEIGHT = 1.0
COV_WEIGHT = 2.0

F32 = jnp.float32
BF16 = jnp.bfloat16
MESH = pl.DeviceIdType.MESH
VMEM_LIMIT = 67043328

ROWS = 1024
HALF = 512
FEAT = 512
DIM = 2048
NB = 8
BLK = 256
LAG = 2
RING = 8
ALL_ROWS = 16384


def sds(shape, dtype):
    return jax.ShapeDtypeStruct(shape, dtype)


ANY = pl.BlockSpec(memory_space=pl.ANY)
INV = pl.BlockSpec(memory_space=pltpu.VMEM)


class Place:
    def __init__(self):
        i = lax.axis_index('data')
        self.c = lax.rem(i, 2)
        x = lax.rem(i // 2, 2)
        y = lax.rem(i // 4, 2)
        z = i // 8
        zl = lax.rem(z, 2)
        zh = z // 2
        self.pc = i + 1 - 2 * self.c
        px = i + 2 - 4 * x
        py = i + 4 - 8 * y
        p1 = i + 8 - 16 * zl
        p2 = i + 16 - 32 * zh
        pd = px + py - i
        p3 = p1 + p2 - i
        self.phases = ((px, py, pd), (p1, p2, p3))
        self.end = zl == zh
        self.p1, self.p3 = p1, p3
        self.first, self.last = (px, py), (py, px)
        self.keep = [b * 128 for b in (x, y)]
        self.send = [(1 - b) * 128 for b in (x, y)]
        self.near = [k + zh * 64 for k in self.keep]
        self.far = [k + (1 - zh) * 64 for k in self.keep]
        self.own = [n + b * 32 for n, b in zip(self.near, (y, x))]
        self.give = [n + (1 - b) * 32 for n, b in zip(self.near, (y, x))]

    def announce(self):
        sem = pltpu.get_barrier_semaphore()
        for p in (self.pc,) + self.phases[0] + self.phases[1]:
            pl.semaphore_signal(sem, inc=1, device_id=(p,), device_id_type=MESH)

    def await_all(self):
        pl.semaphore_wait(pltpu.get_barrier_semaphore(), 7)


def rcopy(src, dst, ssem, rsem, dev):
    return pltpu.make_async_remote_copy(src_ref=src, dst_ref=dst, send_sem=ssem, recv_sem=rsem,
                                        device_id=(dev,), device_id_type=MESH)


def rows_at(off, n):
    return pl.ds(pl.multiple_of(off, n), n)


def nn(a, b):
    return jnp.dot(a, b, preferred_element_type=F32)


def nt(a, b):
    return lax.dot_general(a, b, (((1,), (1,)), ((), ())), preferred_element_type=F32)


def tn(a, b):
    return lax.dot_general(a, b, (((0,), (0,)), ((), ())), preferred_element_type=F32)


def lanes_at(off):
    return pl.ds(pl.multiple_of(off, 128), 128)


def cols_at(off):
    return pl.ds(pl.multiple_of(off, BLK), BLK)


def cols(j):
    return pl.ds(pl.multiple_of(j * BLK, BLK), BLK)


def is_inward(u):
    return (u >= GRAM_UNITS) & (lax.rem(jnp.maximum(u - GRAM_UNITS, 0), 4) == 0)


class Scatter:
    def __init__(self, place, part, lands, ssem, rsem):
        self.pl, self.part, self.lands, self.ssem, self.rsem = place, part, lands, ssem, rsem

    def landing(self, u, e, k, n):
        v = jnp.maximum(u - GRAM_UNITS, 0)
        q, r = v // 4, lax.rem(v, 4)
        gram = u < GRAM_UNITS
        if e in (0, 2):
            return self.lands[e].at[lax.rem(u, 4), k]
        if e == 4:
            turn = jnp.where(gram, u, jnp.where(r == 0, q, v - 1 - q))
            return self.lands[3].at[lax.rem(turn, 4), k]
        off = jnp.where(gram, lax.rem(u, 8) * 64, lax.rem(q, 2) * 320 + jnp.where(r == 0, 0, 64 + r * 64))
        return self.lands[1].at[k, pl.ds(pl.multiple_of(off, 64), n)]

    def copy(self, u, e, k, inward=False):
        me = self.pl
        off, n, dev = ((me.send[k], 128, me.first[k]), (me.far[k], 64, me.p1), (me.far[k], 64, me.p3),
                       (me.near[k], 64, me.p1), (me.give[k], 32, me.last[k]))[e]
        if e == 1 and inward:
            off, n = me.keep[k], 128
        r = lax.rem(u, RING)
        return rcopy(self.part.at[lax.rem(u, SLOTS), k, pl.ds(pl.multiple_of(off, 32), n)], self.landing(u, e, k, n),
                     self.ssem.at[e, k, r], self.rsem.at[e, k, r], dev)

    def start(self, u, e, inward=False):
        for k in range(2):
            self.copy(u, e, k, inward).start()

    def sent(self, u, e, inward=False):
        for k in range(2):
            self.copy(u, e, k, inward).wait_send()

    def add(self, u, e, off, inward=False):
        p, n = lax.rem(u, SLOTS), 128 if inward else (128, 64, 64, 64, 32)[e]
        for k in range(2):
            self.copy(u, e, k, inward).wait_recv()
            rr = pl.ds(pl.multiple_of(off[k], 32), n)
            self.part[p, k, rr] = self.part[p, k, rr] + self.landing(u, e, k, n)[...]

    def step(self, e, u, gram, final):
        me = self.pl
        if gram:
            owner, passes = me.end, jnp.logical_not(me.end)
        else:
            inward = is_inward(u)
            owner, passes = me.end != inward, jnp.logical_not(me.end) & jnp.logical_not(inward)
        variants = (False,) if gram else (False, True)

        def of(variant):
            return me.end if gram else me.end & (inward if variant else jnp.logical_not(inward))

        if e == 1:
            self.sent(u, 0)
            self.add(u, 0, me.keep)
            for v in variants:
                pl.when(of(v))(functools.partial(self.start, u, 1, v))
        if e == 2:
            for v in variants:
                pl.when(of(v))(functools.partial(self.sent, u, 1, v))

            @pl.when(jnp.logical_not(me.end))
            def _():
                for v in variants:
                    def gather(v=v):
                        self.add(u, 1, me.keep if v else me.far, v)
                    if gram:
                        gather()
                    else:
                        pl.when(inward if v else jnp.logical_not(inward))(gather)
                self.start(u, 2)
        if e == 3:
            @pl.when(jnp.logical_not(me.end))
            def _():
                self.sent(u, 2)
                self.add(u, 2, me.near)

            pl.when(passes)(functools.partial(self.start, u, 3))
        if e == 4:
            pl.when(of(False))(functools.partial(self.add, u, 3, me.near))
            pl.when(owner)(functools.partial(self.start, u, 4))
            pl.when(passes)(functools.partial(self.sent, u, 3))
        if e == 5:
            @pl.when(owner)
            def _():
                self.sent(u, 4)
                self.add(u, 4, me.own)
                final(u)


class Span:
    def __init__(self, lo, hi, t):
        self.lo, self.hi, self.t = lo, hi, t

    def at(self, slot, f):
        if self.lo <= slot < self.hi:
            pl.when(self.t == slot)(f)

    def within(self, first, stop, f):
        if max(first, self.lo) >= min(stop, self.hi):
            return
        conds = ([] if first <= self.lo else [self.t >= first]) + ([] if stop >= self.hi else [self.t < stop])
        if not conds:
            f()
        else:
            pl.when(conds[0] if len(conds) == 1 else conds[0] & conds[1])(f)

    def units(self, lag, f):
        for w, first, stop, base in ((GRAM, 0, GRAM_UNITS, 0), (0, START_3, START_3 + 16, 18),
                                     (1, START_2, START_2 + 16, 34), (2, START_2 + 16, START_2 + 20, 50)):
            u = self.t - (lag + first - base)
            self.within(first + lag, stop + lag, functools.partial(f, u, w))


def scatter_scratch(slots):
    return [pltpu.VMEM((slots, 2, BLK, BLK), F32), pltpu.VMEM((4, 2, 128, BLK), F32),
            pltpu.VMEM((2, 640, BLK), F32), pltpu.VMEM((4, 2, 64, BLK), F32), pltpu.VMEM((4, 2, 32, BLK), F32),
            pltpu.SemaphoreType.DMA((5, 2, RING)), pltpu.SemaphoreType.DMA((5, 2, RING))]


class SmallReduce:
    def __init__(self, place, val, land, ssem, rsem, row=0):
        self.pl, self.val, self.ssem, self.rsem = place, val, ssem, rsem
        self.land = land.at[:, :, pl.ds(row, val.shape[0])]

    def copies(self, ph):
        return [rcopy(self.val, self.land.at[ph, k], self.ssem.at[ph, k], self.rsem.at[ph, k], p)
                for k, p in enumerate(self.pl.phases[ph])]

    def start(self, ph):
        for cp in self.copies(ph):
            cp.start()

    def finish(self, ph):
        for cp in self.copies(ph):
            cp.wait()
        land = self.land
        self.val[...] = (self.val[...] + land[ph, 0]) + (land[ph, 1] + land[ph, 2])


def small_scratch(n):
    return [pltpu.VMEM((n, BLK), F32), pltpu.SemaphoreType.DMA((2, 3)), pltpu.SemaphoreType.DMA((2, 3))]


GRAM_UNITS = 18
GRAM = 3
UNITS = 54
SLOTS = 5 * LAG + 1
START_3 = 28
START_2 = 44
END = START_2 + 21 + 11 * LAG
LOOPS = (0, 18, 39, 54, 66, END)
DZ_SLOTS = (23, 27, 30, 32, 34, 36, 37, 38)
PASS_2 = 39
PASS_1 = 45
SPAN_2, SPAN_1 = 3, 4


def block_of(q):
    i = jnp.int32(0)
    for first in (8, 15, 21, 26, 30, 33, 35):
        i = i + jnp.where(q >= first, 1, 0)
    return i, i + q - (17 * i - i * i) // 2


def step_kernel(ha, hb, w1, w2, w3, g1, b1, g2, b2, g3_o, g2_o, g1_o, n1_o, h_o, ho_o, st_o, loss_o,
                zd, zod, dz, dzo, gw, x2h, x2o, x1h, x1o, g2v, g1v, lacc, rs, stage, st_v,
                part, r1, r2, r3, r4, ssem, rsem, sv, sa, sb, fa1, fb1, fa2, fb2,
                s2, sa2, sb2, s1, sa1, sb1, odd_land, even_land, e2, e1,
                asem, bsem, lsem, psem, csem, dsem, esem, wsem):
    me = Place()
    me.announce()
    c = me.c
    nv, da = g2v.at[pl.ds(0, ROWS)], g2v.at[pl.ds(ROWS, ROWS)]
    hv = x2o.at[:, pl.ds(0, FEAT)]
    f1, f2 = [[st.at[pl.ds(h * NB, NB)] for h in range(2)] for st in (s1, s2)]
    gains, biases = (g1, g2), (b1, b2)
    half = pl.ds(pl.multiple_of(c * 1024, 1024), 1024)
    ohalf = pl.ds(pl.multiple_of((1 - c) * 1024, 1024), 1024)
    hhalf = pl.ds(pl.multiple_of(c * 256, 256), 256)
    hohalf = pl.ds(pl.multiple_of((1 - c) * 256, 256), 256)
    mine = pl.ds(pl.multiple_of(c * HALF, HALF), HALF)
    theirs = pl.ds(pl.multiple_of((1 - c) * HALF, HALF), HALF)
    body = pl.ds(0, ROWS)
    w1v = zod.at[pl.ds(0, FEAT)]
    load_w1 = pltpu.make_async_copy(w1, w1v, csem.at[0])
    load_w2a = pltpu.make_async_copy(w2, gw, csem.at[1])
    load_w3a = [pltpu.make_async_copy(w3.at[pl.ds(r, 1024)], gw.at[pl.ds(r, 1024)], csem.at[k])
                for r, k in ((0, 2), (1024, 4))]
    load_w2 = pltpu.make_async_copy(w2, gw, csem.at[6])
    load_n1 = pltpu.make_async_copy(n1_o, nv, csem.at[7])
    save_n1 = pltpu.make_async_copy(da, n1_o, csem.at[8])
    keep_x1 = pltpu.make_async_copy(dzo.at[:, half], x1h, csem.at[3])
    keep_h = pltpu.make_async_copy(hv.at[:, hhalf], h_o, csem.at[5])
    hh, ho = x2h.at[:, pl.ds(0, 256)], x2o.at[:, pl.ds(0, 256)]
    load_h2 = [pltpu.make_async_copy(h_o, hh, csem.at[5]), pltpu.make_async_copy(ho_o, ho, csem.at[2])]
    keep_x2 = pltpu.make_async_copy(dz.at[:, half], x2h, csem.at[10])
    swap_z = rcopy(zd.at[body], zod, dsem.at[0], esem.at[0], me.pc)
    swap_x2 = rcopy(dz.at[:, ohalf], x2o, dsem.at[1], esem.at[1], me.pc)
    swap_x1 = rcopy(dzo.at[:, ohalf], x1o, dsem.at[2], esem.at[2], me.pc)
    swap_h = rcopy(hv.at[:, hohalf], ho_o, dsem.at[3], esem.at[3], me.pc)
    swap_du1 = rcopy(dz, dzo, dsem.at[5], esem.at[5], me.pc)
    swap_s2 = rcopy(s2, e2, dsem.at[6], esem.at[6], me.pc)
    swap_s1 = rcopy(s1, e1, dsem.at[7], esem.at[7], me.pc)

    def load_h(src):
        return pltpu.make_async_copy(src, hv.at[mine], csem.at[9])

    def give_h(src):
        return rcopy(src, hv.at[mine], dsem.at[16], esem.at[16], me.pc)

    def load_w3(j):
        return pltpu.make_async_copy(w3.at[cols(j)], gw.at[cols(j)], wsem.at[j])

    def swap_du2(j):
        return rcopy(zd.at[body, cols(j)], zod.at[:, cols(j)], dsem.at[17 + j], esem.at[17 + j], me.pc)

    def swap_dz(j):
        return rcopy(dz.at[:, cols(j)], dzo.at[:, cols(j)], dsem.at[8 + j], esem.at[8 + j], me.pc)

    for k, own in ((0, ha), (1, hb)):
        @pl.when(c == k)
        def _(own=own):
            load_h(own).start()
    load_w1.start()
    me.await_all()
    for k, other in ((0, hb), (1, ha)):
        @pl.when(c == k)
        def _(other=other):
            give_h(other).start()
    load_w2a.start()
    lacc[...] = jnp.zeros_like(lacc)

    def matmul(src, w, dst, rows, depth, first, stop, st=None, add=False):
        def step(j, carry):
            res = nn(src[rows, depth], w[depth, cols(j)])
            if add == 'depth':
                res = res + dst[rows, cols(j)]
            dst[rows, cols(j)] = res
            if st is not None:
                one = jnp.sum(res, axis=0, keepdims=True)
                two = jnp.sum(res * res, axis=0, keepdims=True)
                k = lax.rem(j, 4)
                if add == 'rows':
                    one = one + st[pl.ds(k, 1)]
                    two = two + st[pl.ds(4 + k, 1)]
                st[pl.ds(k, 1)] = one
                st[pl.ds(4 + k, 1)] = two
            return carry
        lax.fori_loop(first, stop, step, 0)

    def norm(u, x, st, layer, h):
        mean = st[0:4] * (1.0 / ALL_ROWS)
        var = st[4:8] * (1.0 / ALL_ROWS) - mean * mean
        inv = lax.rsqrt(var + BN_EPS)
        st[0:4] = mean
        st[4:8] = inv
        rs[NB * layer + 4 * h:NB * layer + 4 * h + 4] = inv

        def step(j, carry):
            k = j - 4 * h
            nrm = (u[:, cols(j)] - st[pl.ds(k, 1)]) * st[pl.ds(4 + k, 1)]
            act = gains[layer][:, cols(j)] * nrm + biases[layer][:, cols(j)]
            u[:, cols(j)] = nrm
            x[:, cols(j)] = jnp.maximum(act, 0.0).astype(BF16)
            return carry
        lax.fori_loop(4 * h, 4 * h + 4, step, 0)

    low, high, full = pl.ds(0, 1024), pl.ds(1024, 1024), pl.ds(0, DIM)
    all_f = pl.ds(0, FEAT)
    red_f1 = [SmallReduce(me, f1[h], odd_land, fa1.at[h], fb1.at[h], h * NB) for h in range(2)]
    red_f2 = [SmallReduce(me, f2[h], even_land, fa2.at[h], fb2.at[h], h * NB) for h in range(2)]
    load_w1.wait()
    load_h(ha).wait()
    give_h(ha).wait()
    swap_h.start()
    keep_h.start()
    for h in range(2):
        matmul(hv, w1v, da, body, all_f, 4 * h, 4 * h + 4, f1[h])
        red_f1[h].start(0)
    for h in range(2):
        red_f1[h].finish(0)
        red_f1[h].start(1)
    red_f1[0].finish(1)
    norm(da, dzo, f1[0], 0, 0)
    load_w2a.wait()
    matmul(dzo, gw, nv, body, low, 0, NB)
    red_f1[1].finish(1)
    norm(da, dzo, f1[1], 0, 1)
    matmul(dzo, gw, nv, body, high, 0, 4, f2[0], 'depth')
    red_f2[0].start(0)
    save_n1.start()
    keep_h.wait()
    swap_h.wait()
    swap_x1.start()
    keep_x1.start()
    matmul(dzo, gw, nv, body, high, 4, 6, f2[1], 'depth')
    red_f2[0].finish(0)
    red_f2[0].start(1)
    matmul(dzo, gw, nv, body, high, 6, NB, f2[1], 'depth')
    red_f2[1].start(0)
    for cp in load_w3a:
        cp.start()
    red_f2[0].finish(1)
    norm(nv, dz, f2[0], 1, 0)
    red_f2[1].finish(0)
    red_f2[1].start(1)
    save_n1.wait()
    load_w3a[0].wait()
    matmul(dz, gw, da, body, low, 0, 4)
    red_f2[1].finish(1)
    norm(nv, dz, f2[1], 1, 1)
    swap_x1.wait()
    swap_x2.start()
    keep_x2.start()
    load_w3a[1].wait()

    def z_block(j, part_done):
        if part_done:
            res = (da[:, cols(j)] + nn(dz[:, high], gw[high, cols(j)])).astype(BF16)
        else:
            res = nn(dz[...], gw[:, cols(j)]).astype(BF16)
        zd[0:ROWS, cols(j)] = res
        sv[pl.ds(j, 1)] = jnp.sum(res.astype(F32), axis=0, keepdims=True)

    def z_blocks(first, part_done):
        def step(j, carry):
            z_block(first + j, part_done)
            return carry
        lax.fori_loop(0, 2, step, 0)

    z_blocks(0, True)
    red0 = SmallReduce(me, sv, odd_land, sa, sb)
    red2 = SmallReduce(me, s2, even_land, sa2, sb2)
    red1 = SmallReduce(me, s1, odd_land, sa1, sb1)
    sc = Scatter(me, part, (r1, r2, r3, r4), ssem, rsem)

    def compute(u, w):
        p = lax.rem(u, SLOTS)
        if w == GRAM:
            i, j = block_of(2 * u)
            i1, j1 = block_of(2 * u + 1)

            @pl.when(i == i1)
            def _():
                res = tn(zd[0:ROWS, cols(i)], zd[0:ROWS, pl.ds(pl.multiple_of(j * BLK, BLK), 2 * BLK)])
                part[p, 0] = res[:, 0:BLK]
                part[p, 1] = res[:, BLK:2 * BLK]

            @pl.when(i != i1)
            def _():
                part[p, 0] = tn(zd[0:ROWS, cols(i)], zd[0:ROWS, cols(j)])
                part[p, 1] = tn(zd[0:ROWS, cols(i1)], zd[0:ROWS, cols(j1)])
            return
        q = grad_unit(u)[1]
        if w == 2:
            rc = pl.ds(pl.multiple_of(q * 512, 512), 512)
            res = tn(hh[...], dz[:, rc]) + tn(ho[...], dzo[:, rc])
            part[p, 0] = res[:, 0:BLK]
            part[p, 1] = res[:, BLK:2 * BLK]
            return
        la, lb, ra, rb = ((x2h, x2o, dz, dzo), (x1h, x1o, zd, zod))[w]
        lc = pl.ds(pl.multiple_of(lax.rem(q, 2) * 512, 512), 512)
        rc = cols(q // 2)
        res = tn(la[:, lc], ra[0:ROWS, rc]) + tn(lb[:, lc], rb[:, rc])
        part[p, 0] = res[0:BLK]
        part[p, 1] = res[BLK:2 * BLK]

    def grad_unit(u):
        v = jnp.maximum(u - GRAM_UNITS, 0)
        return v // 16, lax.rem(v, 16)

    def region(u, w, k, off, n):
        q = grad_unit(u)[1]
        if w == 2:
            r0, c0 = c * 256, q * 512 + k * BLK
        else:
            r0, c0 = c * 1024 + lax.rem(q, 2) * 512 + k * BLK, (q // 2) * BLK
        return rows_at(r0 + off, n), cols_at(c0)

    grads = (g3_o, g2v, g1v)

    def keep_copy(u, k):
        own = region(u, 0, k, me.own[k], 32)
        return pltpu.make_async_copy(stage.at[lax.rem(u, 3), k], g3_o.at[own], lsem.at[k, lax.rem(u, RING)])

    def hop(e, k, inward):
        if e == 3 and inward:
            return me.keep[k], 128, me.p1
        return ((me.own[k], 32, me.last[k]), (me.near[k], 64, me.p1), (me.near[k], 64, me.p3),
                (me.far[k], 64, me.p1), (me.keep[k], 128, me.first[k]))[e]

    def spread(u, w, e, k, inward=False):
        r = lax.rem(u, RING)
        off, n, dev = hop(e, k, inward)
        if w == GRAM:
            i, j = block_of(2 * u + k)
            src = dst = gw.at[rows_at(i * BLK + off, n), cols(j)]
        else:
            dst = grads[w].at[region(u, w, k, off, n)]
            src = stage.at[lax.rem(u, 3), k] if e == 0 and w == 0 else dst
        g = 0 if w == GRAM else 1
        return rcopy(src, dst, asem.at[g, e, k, r], bsem.at[g, e, k, r], dev)

    def cross(u, w):
        r = lax.rem(u, RING)
        q = grad_unit(u)[1]
        buf = grads[w].at[unit_region(q, w, c)]
        return rcopy(buf, buf, asem.at[1, 5, 0, r], bsem.at[1, 5, 0, r], me.pc)

    def unit_region(q, w, core):
        if w == 2:
            return rows_at(core * 256, 256), pl.ds(pl.multiple_of(q * 512, 512), 512)
        return rows_at(core * 1024 + lax.rem(q, 2) * 512, 512), cols(q // 2)

    def put(u, w, own):
        reg = unit_region(grad_unit(u)[1], w, c if own else 1 - c)
        out = (None, g2_o, g1_o)[w]
        return pltpu.make_async_copy(grads[w].at[reg], out.at[reg], psem.at[0 if own else 1, lax.rem(u, RING)])

    def final(u, w):
        if w < 3:
            for k in range(2):
                piece = part[lax.rem(u, SLOTS), k, rows_at(me.own[k], 32)]
                if w == 0:
                    stage[lax.rem(u, 3), k] = piece
                    keep_copy(u, k).start()
                else:
                    rr, cc = region(u, w, k, me.own[k], 32)
                    grads[w][rr, cc] = piece
                spread(u, w, 0, k).start()
            return
        for k in range(2):
            i, j = block_of(2 * u + k)
            own = rows_at(me.own[k], 32)
            row0 = rows_at(i * BLK + me.own[k], 32)
            mu_r = g1v[rows_at(lax.rem(i, 2) * BLK + me.own[k], 32), lanes_at((i // 2) * 128)]
            mu_c = sv[pl.ds(j, 1)]
            mm = ALL_ROWS * jnp.concatenate([mu_r, mu_r], axis=1) * mu_c
            cov = (part[lax.rem(u, SLOTS), k, own] - mm) * (1.0 / (ALL_ROWS - 1))
            row = lax.broadcasted_iota(jnp.int32, (32, BLK), 0) + (i * BLK + me.own[k])
            col = lax.broadcasted_iota(jnp.int32, (32, BLK), 1) + j * BLK
            diag = row == col
            std = jnp.sqrt(jnp.where(diag, cov, 1.0) + STD_EPS)
            hinge = jnp.where(std < 1.0, VAR_WEIGHT / (2.0 * std), 0.0)
            weight = jnp.where(i == j, COV_WEIGHT, 2.0 * COV_WEIGHT)
            term = jnp.where(diag, VAR_WEIGHT * jnp.maximum(1.0 - std, 0.0), weight * cov * cov)
            lacc[...] = lacc[...] + ((term[0:8] + term[8:16]) + (term[16:24] + term[24:32]))
            gw[row0, cols(j)] = jnp.where(diag, -hinge, (2.0 * COV_WEIGHT) * cov).astype(BF16)
            spread(u, GRAM, 0, k).start()

    def diff_block(j):
        diff = zd[0:ROWS, cols(j)].astype(F32) - zod[:, cols(j)].astype(F32)
        sq = jnp.sum((diff * diff).reshape(ROWS // 8, 8, BLK), axis=0)
        lacc[...] = lacc[...] + (0.5 * INV_WEIGHT / ALL_ROWS) * sq
        da[:, cols(j)] = (2.0 * INV_WEIGHT / ALL_ROWS) * diff

    def dz_block(j):
        acc = nn(zd[...], gw[:, cols(j)])
        mean = acc[ROWS:ROWS + 1] + acc[ROWS + 1:ROWS + 2] + acc[ROWS + 2:ROWS + 3]
        dz[:, cols(j)] = (da[:, cols(j)] + (2.0 / (ALL_ROWS - 1)) * (acc[0:ROWS] - mean)).astype(BF16)

    def back_block(j, grad, st, layer):
        dx = nt(grad[0:ROWS, :], gw[cols(j)])
        nrm = nv[:, cols(j)]
        act = gains[layer][:, cols(j)] * nrm + biases[layer][:, cols(j)]
        d_act = jnp.where(act > 0.0, dx, 0.0)
        da[:, cols(j)] = d_act
        st[pl.ds(j, 1)] = jnp.sum(d_act, axis=0, keepdims=True)
        st[pl.ds(NB + j, 1)] = jnp.sum(d_act * nrm, axis=0, keepdims=True)

    def back_pre(dst, st, layer, after):
        def step(j, carry):
            scale = gains[layer][:, cols(j)] * rs[pl.ds(NB * layer + j, 1)]
            m0 = st[pl.ds(j, 1)] * (1.0 / ALL_ROWS)
            m1 = st[pl.ds(NB + j, 1)] * (1.0 / ALL_ROWS)
            dst[0:ROWS, cols(j)] = (scale * (da[:, cols(j)] - m0 - nv[:, cols(j)] * m1)).astype(BF16)
            after(j)
            return carry
        lax.fori_loop(0, NB, step, 0)

    def gather_step(e, u, w, inward):
        def each(f):
            for k in range(2):
                f(k)

        def wait_send(k):
            spread(u, w, e - 1, k, inward).wait_send()

        def wait_recv(k):
            spread(u, w, e - 1, k, inward).wait_recv()

        def begin(k):
            spread(u, w, e, k, inward).start()

        def run(sends, recvs, begins):
            if e == 1 and w == 0:
                each(lambda k: keep_copy(u, k).wait())
            if e in sends:
                each(wait_send)
            if e in recvs:
                each(wait_recv)
            if e in begins:
                each(begin)

        def at_end():
            if inward:
                run((), (4,), (4,))
            else:
                run((1, 2, 5), (1, 4, 5), (1, 4))

        def at_inner():
            if inward:
                run((1, 3, 4), (1, 3), (2, 3, 4))
            else:
                run((3, 4), (2, 3), (2, 3, 4))

        if e == 5:
            at_end()
        else:
            if e == 4 or not inward:
                pl.when(me.end)(at_end)
            if e > 1 or inward:
                pl.when(jnp.logical_not(me.end))(at_inner)
        if e == 5 and w < 3:
            cross(u, w).start()
            if w > 0:
                put(u, w, True).start()
        if e == 5 and w == GRAM:
            for k in range(2):
                i, j = block_of(2 * u + k)

                @pl.when(i != j)
                def _():
                    gw[rows_at(j * BLK, BLK), cols(i)] = gw[rows_at(i * BLK, BLK), cols(j)].T

    compute(jnp.int32(0), GRAM)

    def gather(e, u, w):
        if w == GRAM or e == 5:
            gather_step(e, u, w, False)
            return
        inward = is_inward(u)
        pl.when(jnp.logical_not(inward))(lambda: gather_step(e, u, w, False))
        pl.when(inward)(lambda: gather_step(e, u, w, True))

    def put_end(u, w):
        if w in (1, 2):
            put(u, w, False).wait()

    def cross_end(u, w):
        if w < 3:
            cross(u, w).wait()
        if w in (1, 2):
            put(u, w, True).wait()
            put(u, w, False).start()

    def means():
        mean = sv[...] * (1.0 / ALL_ROWS)
        sv[...] = mean
        hi = mean.astype(BF16)
        mid = (mean - hi.astype(F32)).astype(BF16)
        low = (mean - hi.astype(F32) - mid.astype(F32)).astype(BF16)
        for j in range(NB):
            for h in range(2):
                lanes = slice(128 * h, 128 * h + 128)
                r0, c0 = (j % 2) * BLK + 128 * h, (j // 2) * 128
                g1v[r0:r0 + 128, c0:c0 + 128] = jnp.broadcast_to(mean[j:j + 1, lanes], (128, 128)).T
            zd[ROWS:ROWS + 8, j * BLK:(j + 1) * BLK] = jnp.concatenate(
                [hi[j:j + 1], mid[j:j + 1], low[j:j + 1], jnp.zeros((5, BLK), BF16)], axis=0)

    def slots(lo, hi):
        def slot(t, carry):
            run_slot(Span(lo, hi, t), t)
            return carry
        lax.fori_loop(lo, hi, slot, 0)

    out_st = pltpu.make_async_copy(st_v, st_o, csem.at[9])

    def small_results():
        swap_s2.wait()
        swap_s1.wait()
        sum2, sum1 = s2[...] + e2[...], s1[...] + e1[...]
        for j in range(NB):
            lanes = slice(j * BLK, (j + 1) * BLK)
            st_v[0:1, lanes] = sum1[NB + j:NB + j + 1]
            st_v[1:2, lanes] = sum1[j:j + 1]
            st_v[2:3, lanes] = sum2[NB + j:NB + j + 1]
            st_v[3:4, lanes] = sum2[j:j + 1]
        loss_o[0, 0] = jnp.sum(sum2[2 * NB:])
        out_st.start()

    def run_slot(span, t):
        span.units(11 * LAG + 1, put_end)
        span.units(11 * LAG, cross_end)
        for e in (5, 4, 3, 2, 1):
            span.units((5 + e) * LAG, functools.partial(gather, e))
        reds = ((2, red0), (PASS_2 + SPAN_2 - 1, red2), (PASS_1 + SPAN_1 - 1, red1))
        for first, red in reds:
            @functools.partial(span.at, first + 1)
            def _(red=red):
                red.finish(0)
                red.start(1)

            @functools.partial(span.at, first + 2)
            def _(red=red):
                red.finish(1)

        @functools.partial(span.at, PASS_2 + SPAN_2)
        def _():
            load_w2.start()

        @functools.partial(span.at, PASS_2 + SPAN_2 + 1)
        def _():
            back_pre(zd, s2, 1, lambda j: swap_du2(j).start())
            load_n1.start()
            swap_s2.start()

        @functools.partial(span.at, PASS_1 + SPAN_1 + 1)
        def _():
            back_pre(dz, s1, 0, lambda j: None)
            swap_du1.start()
            swap_s1.start()

        for j, first in enumerate(DZ_SLOTS):
            span.at(first + 1, lambda j=j: swap_dz(j).wait())
        mine_now = jnp.int32(-1)
        for j, first in enumerate(DZ_SLOTS):
            if span.lo <= first < span.hi:
                mine_now = jnp.where(t == first, j, mine_now)
        if any(span.lo <= first < span.hi for first in DZ_SLOTS):
            @pl.when(mine_now >= 0)
            def _():
                dz_block(mine_now)
                swap_dz(mine_now).start()

        @functools.partial(span.at, DZ_SLOTS[-1])
        def _():
            for j in range(NB):
                load_w3(j).start()

        span.at(START_2 + 24, small_results)
        for e in (5, 4, 3, 2, 1):
            span.units(e * LAG, lambda u, w, e=e: sc.step(e, u, w == GRAM, lambda v: final(v, w)))
        span.units(0, lambda u, w: sc.start(u, 0))
        span.at(4, means)
        span.at(0, lambda: z_blocks(2, True))
        span.within(1, 3, lambda: z_blocks(2 * t + 2, False))

        @functools.partial(span.at, 3)
        def _():
            keep_x1.wait()
            keep_x2.wait()
            swap_x2.wait()
            swap_z.start()

        span.at(7, swap_z.wait)
        span.within(8, 8 + NB, lambda: diff_block(t - 8))
        @functools.partial(span.at, PASS_2)
        def _():
            s2[2 * NB:3 * NB] = lacc[...]

        @functools.partial(span.at, PASS_1)
        def _():
            load_w2.wait()
            load_n1.wait()

        @functools.partial(span.within, START_2 - 1, START_2 + 15)
        def _():
            block = (t - (START_2 - 1)) // 2

            @pl.when(t == START_2 - 1 + 2 * block)
            def _():
                swap_du2(block).wait()

        @functools.partial(span.at, START_2 + 8)
        def _():
            for cp in load_h2:
                cp.start()

        @functools.partial(span.at, START_2 + 14)
        def _():
            swap_du1.wait()
            for cp in load_h2:
                cp.wait()

        for first, width, grad, st, layer in ((PASS_2, SPAN_2, dz, s2, 1), (PASS_1, SPAN_1, zd, s1, 0)):
            @functools.partial(span.within, first, first + width)
            def _(first=first, n=-(-NB // width), grad=grad, st=st, layer=layer):
                def step(j, carry):
                    if layer == 1:
                        load_w3(j).wait()
                    back_block(j, grad, st, layer)
                    return carry
                lo = n * (t - first)
                lax.fori_loop(lo, jnp.minimum(lo + n, NB), step, 0)

        for last, red in reds:
            span.at(last, lambda red=red: red.start(0))
        span.units(-1, compute)

    for lo, hi in zip(LOOPS, LOOPS[1:]):
        slots(lo, hi)
    out_st.wait()


def train_step(ha, hb, w1, w2, w3, g1, b1, g2, b2):
    act = pltpu.VMEM((ROWS, DIM), BF16)
    piece = pltpu.VMEM((ROWS, 1024), BF16)
    dma = pltpu.SemaphoreType.DMA
    return pl.pallas_call(
        step_kernel,
        out_shape=(sds((DIM, DIM), F32), sds((DIM, DIM), F32), sds((FEAT, DIM), F32), sds((ROWS, DIM), F32),
                   sds((ROWS, 256), BF16), sds((ROWS, 256), BF16), sds((4, DIM), F32), sds((1, 1), F32)),
        in_specs=[ANY] * 5 + [INV] * 4,
        out_specs=(ANY,) * 7 + (pl.BlockSpec(memory_space=pltpu.SMEM),),
        scratch_shapes=[pltpu.VMEM((ROWS + 8, DIM), BF16), act, act, act, pltpu.VMEM((DIM, DIM), BF16),
                        piece, piece, piece, piece,
                        pltpu.VMEM((DIM, DIM), F32), pltpu.VMEM((FEAT, DIM), F32),
                        pltpu.VMEM((NB, BLK), F32), pltpu.VMEM((2 * NB, BLK), F32),
                        pltpu.VMEM((3, 2, 32, BLK), F32), pltpu.VMEM((4, DIM), F32)]
        + scatter_scratch(SLOTS) + small_scratch(NB) + [dma((2, 2, 3))] * 4
        + small_scratch(3 * NB) + small_scratch(2 * NB)
        + [pltpu.VMEM((2, 3, 2 * NB, BLK), F32), pltpu.VMEM((2, 3, 3 * NB, BLK), F32),
           pltpu.VMEM((3 * NB, BLK), F32), pltpu.VMEM((2 * NB, BLK), F32),
           dma((2, 6, 2, RING)), dma((2, 6, 2, RING)), dma((2, RING)),
           dma((2, RING)), dma((11,)), dma((25,)), dma((25,)), dma((NB,))],
        compiler_params=pltpu.CompilerParams(collective_id=0, has_side_effects=True, vmem_limit_bytes=VMEM_LIMIT),
        name='train_step',
    )(ha, hb, w1, w2, w3, g1, b1, g2, b2)


CHUNK = 128
BUFS = 8


def finish_kernel(g3, g2, g1, st, loss, o3, o2, o1, gain1, bias1, gain2, bias2, loss_o, buf, isem, osem, rsem):
    jobs = [(src, dst, r) for src, dst, n in ((g3, o3, DIM), (g2, o2, DIM), (g1, o1, FEAT)) for r in range(0, n, CHUNK)]

    def take(i):
        src, _, r = jobs[i]
        return pltpu.make_async_copy(src.at[pl.ds(r, CHUNK)], buf.at[i % BUFS], isem.at[i % BUFS])

    def give(i):
        _, dst, r = jobs[i]
        return pltpu.make_async_copy(buf.at[i % BUFS], dst.at[pl.ds(r, CHUNK)], osem.at[i % BUFS])

    for i in range(BUFS - 1):
        take(i).start()
    rows = [pltpu.make_async_copy(st.at[pl.ds(row, 1)], out, rsem.at[row])
            for row, out in enumerate((gain1, bias1, gain2, bias2))]
    for cp in rows:
        cp.start()
    loss_o[0, 0] = loss[0, 0]
    for i in range(len(jobs)):
        take(i).wait()
        give(i).start()
        if i + BUFS - 1 < len(jobs):
            if i > 0:
                give(i - 1).wait()
            take(i + BUFS - 1).start()
    for i in range(len(jobs) - BUFS, len(jobs)):
        give(i).wait()
    for cp in rows:
        cp.wait()


def finish(g3, g2, g1, st, loss):
    smem = pl.BlockSpec(memory_space=pltpu.SMEM)
    dma = pltpu.SemaphoreType.DMA
    return pl.pallas_call(
        finish_kernel,
        out_shape=(sds((DIM, DIM), F32), sds((DIM, DIM), F32), sds((FEAT, DIM), F32)) + (sds((1, DIM), F32),) * 4
        + (sds((1, 1), F32),),
        in_specs=[ANY] * 4 + [smem],
        out_specs=(ANY,) * 7 + (smem,),
        scratch_shapes=[pltpu.VMEM((BUFS, CHUNK, DIM), F32), dma((BUFS,)), dma((BUFS,)), dma((4,))],
        name='finish',
    )(g3, g2, g1, st, loss)


def solution(mesh):
    def local_step(h_a, h_b, w_one, w_two, w_three, gain_one, bias_one, gain_two, bias_two):
        vecs = [v.reshape(1, DIM) for v in (gain_one, bias_one, gain_two, bias_two)]
        g_three, g_two, g_one, _, _, _, st, part_loss = train_step(h_a, h_b, w_one, w_two, w_three, *vecs)
        d_three, d_two, d_one, *small, loss = finish(g_three, g_two, g_one, st, part_loss)
        return (loss.reshape(()), d_one, d_two, d_three, *[v.reshape(DIM) for v in small])

    row_spec = P('data', None)
    return jax.shard_map(local_step, mesh=mesh,
                         in_specs=(row_spec, row_spec, P(), P(), P(), P(), P(), P(), P()),
                         out_specs=(P(), P(), P(), P(), P(), P(), P(), P()),
                         check_vma=False)
```

```python
import functools

import jax
import jax.numpy as jnp
from jax import lax
from jax.experimental import pallas as pl
from jax.experimental.pallas import tpu as pltpu
from jax.sharding import PartitionSpec as P

BN_EPS = 1e-5
STD_EPS = 1e-4
INV_WEIGHT = 2.0
VAR_WEIGHT = 1.0
COV_WEIGHT = 2.0

F32 = jnp.float32
BF16 = jnp.bfloat16
MESH = pl.DeviceIdType.MESH
VMEM_LIMIT = 67043328

ROWS = 1024
HALF = 512
FEAT = 512
DIM = 2048
NB = 8
BLK = 256
LAG = 2
RING = 8
ALL_ROWS = 16384


def sds(shape, dtype):
    return jax.ShapeDtypeStruct(shape, dtype)


ANY = pl.BlockSpec(memory_space=pl.ANY)
INV = pl.BlockSpec(memory_space=pltpu.VMEM)


class Place:
    def __init__(self):
        i = lax.axis_index('data')
        self.c = lax.rem(i, 2)
        x = lax.rem(i // 2, 2)
        y = lax.rem(i // 4, 2)
        z = i // 8
        zl = lax.rem(z, 2)
        zh = z // 2
        self.pc = i + 1 - 2 * self.c
        px = i + 2 - 4 * x
        py = i + 4 - 8 * y
        p1 = i + 8 - 16 * zl
        p2 = i + 16 - 32 * zh
        pd = px + py - i
        p3 = p1 + p2 - i
        self.phases = ((px, py, pd), (p1, p2, p3))
        self.end = zl == zh
        self.p1, self.p3 = p1, p3
        self.first, self.last = (px, py), (py, px)
        self.keep = [b * 128 for b in (x, y)]
        self.send = [(1 - b) * 128 for b in (x, y)]
        self.near = [k + zh * 64 for k in self.keep]
        self.far = [k + (1 - zh) * 64 for k in self.keep]
        self.own = [n + b * 32 for n, b in zip(self.near, (y, x))]
        self.give = [n + (1 - b) * 32 for n, b in zip(self.near, (y, x))]

    def announce(self):
        sem = pltpu.get_barrier_semaphore()
        for p in (self.pc,) + self.phases[0] + self.phases[1]:
            pl.semaphore_signal(sem, inc=1, device_id=(p,), device_id_type=MESH)

    def await_all(self):
        pl.semaphore_wait(pltpu.get_barrier_semaphore(), 7)


def rcopy(src, dst, ssem, rsem, dev):
    return pltpu.make_async_remote_copy(src_ref=src, dst_ref=dst, send_sem=ssem, recv_sem=rsem,
                                        device_id=(dev,), device_id_type=MESH)


def rows_at(off, n):
    return pl.ds(pl.multiple_of(off, n), n)


def nn(a, b):
    return jnp.dot(a, b, preferred_element_type=F32)


def nt(a, b):
    return lax.dot_general(a, b, (((1,), (1,)), ((), ())), preferred_element_type=F32)


def tn(a, b):
    return lax.dot_general(a, b, (((0,), (0,)), ((), ())), preferred_element_type=F32)


def lanes_at(off):
    return pl.ds(pl.multiple_of(off, 128), 128)


def cols_at(off):
    return pl.ds(pl.multiple_of(off, BLK), BLK)


def cols(j):
    return pl.ds(pl.multiple_of(j * BLK, BLK), BLK)


def is_inward(u):
    return (u >= GRAM_UNITS) & (lax.rem(jnp.maximum(u - GRAM_UNITS, 0), 4) == 0)


class Scatter:
    def __init__(self, place, part, lands, ssem, rsem):
        self.pl, self.part, self.lands, self.ssem, self.rsem = place, part, lands, ssem, rsem

    def landing(self, u, e, k, n):
        v = jnp.maximum(u - GRAM_UNITS, 0)
        q, r = v // 4, lax.rem(v, 4)
        gram = u < GRAM_UNITS
        if e in (0, 2):
            return self.lands[e].at[lax.rem(u, 4), k]
        if e == 4:
            turn = jnp.where(gram, u, jnp.where(r == 0, q, v - 1 - q))
            return self.lands[3].at[lax.rem(turn, 4), k]
        off = jnp.where(gram, lax.rem(u, 8) * 64, lax.rem(q, 2) * 320 + jnp.where(r == 0, 0, 64 + r * 64))
        return self.lands[1].at[k, pl.ds(pl.multiple_of(off, 64), n)]

    def copy(self, u, e, k, inward=False):
        me = self.pl
        off, n, dev = ((me.send[k], 128, me.first[k]), (me.far[k], 64, me.p1), (me.far[k], 64, me.p3),
                       (me.near[k], 64, me.p1), (me.give[k], 32, me.last[k]))[e]
        if e == 1 and inward:
            off, n = me.keep[k], 128
        r = lax.rem(u, RING)
        return rcopy(self.part.at[lax.rem(u, SLOTS), k, pl.ds(pl.multiple_of(off, 32), n)], self.landing(u, e, k, n),
                     self.ssem.at[e, k, r], self.rsem.at[e, k, r], dev)

    def start(self, u, e, inward=False):
        for k in range(2):
            self.copy(u, e, k, inward).start()

    def sent(self, u, e, inward=False):
        for k in range(2):
            self.copy(u, e, k, inward).wait_send()

    def add(self, u, e, off, inward=False):
        p, n = lax.rem(u, SLOTS), 128 if inward else (128, 64, 64, 64, 32)[e]
        for k in range(2):
            self.copy(u, e, k, inward).wait_recv()
            rr = pl.ds(pl.multiple_of(off[k], 32), n)
            self.part[p, k, rr] = self.part[p, k, rr] + self.landing(u, e, k, n)[...]

    def step(self, e, u, gram, final):
        me = self.pl
        if gram:
            owner, passes = me.end, jnp.logical_not(me.end)
        else:
            inward = is_inward(u)
            owner, passes = me.end != inward, jnp.logical_not(me.end) & jnp.logical_not(inward)
        variants = (False,) if gram else (False, True)

        def of(variant):
            return me.end if gram else me.end & (inward if variant else jnp.logical_not(inward))

        if e == 1:
            self.sent(u, 0)
            self.add(u, 0, me.keep)
            for v in variants:
                pl.when(of(v))(functools.partial(self.start, u, 1, v))
        if e == 2:
            for v in variants:
                pl.when(of(v))(functools.partial(self.sent, u, 1, v))

            @pl.when(jnp.logical_not(me.end))
            def _():
                for v in variants:
                    def gather(v=v):
                        self.add(u, 1, me.keep if v else me.far, v)
                    if gram:
                        gather()
                    else:
                        pl.when(inward if v else jnp.logical_not(inward))(gather)
                self.start(u, 2)
        if e == 3:
            @pl.when(jnp.logical_not(me.end))
            def _():
                self.sent(u, 2)
                self.add(u, 2, me.near)

            pl.when(passes)(functools.partial(self.start, u, 3))
        if e == 4:
            pl.when(of(False))(functools.partial(self.add, u, 3, me.near))
            pl.when(owner)(functools.partial(self.start, u, 4))
            pl.when(passes)(functools.partial(self.sent, u, 3))
        if e == 5:
            @pl.when(owner)
            def _():
                self.sent(u, 4)
                self.add(u, 4, me.own)
                final(u)


class Span:
    def __init__(self, lo, hi, t):
        self.lo, self.hi, self.t = lo, hi, t

    def at(self, slot, f):
        if self.lo <= slot < self.hi:
            pl.when(self.t == slot)(f)

    def within(self, first, stop, f):
        if max(first, self.lo) >= min(stop, self.hi):
            return
        conds = ([] if first <= self.lo else [self.t >= first]) + ([] if stop >= self.hi else [self.t < stop])
        if not conds:
            f()
        else:
            pl.when(conds[0] if len(conds) == 1 else conds[0] & conds[1])(f)

    def units(self, lag, f):
        for w, first, stop, base in ((GRAM, 0, GRAM_UNITS, 0), (0, START_3, START_3 + 16, 18),
                                     (1, START_2, START_2 + 16, 34), (2, START_2 + 16, START_2 + 20, 50)):
            u = self.t - (lag + first - base)
            self.within(first + lag, stop + lag, functools.partial(f, u, w))


def scatter_scratch(slots):
    return [pltpu.VMEM((slots, 2, BLK, BLK), F32), pltpu.VMEM((4, 2, 128, BLK), F32),
            pltpu.VMEM((2, 640, BLK), F32), pltpu.VMEM((4, 2, 64, BLK), F32), pltpu.VMEM((4, 2, 32, BLK), F32),
            pltpu.SemaphoreType.DMA((5, 2, RING)), pltpu.SemaphoreType.DMA((5, 2, RING))]


class SmallReduce:
    def __init__(self, place, val, land, ssem, rsem, row=0):
        self.pl, self.val, self.ssem, self.rsem = place, val, ssem, rsem
        self.land = land.at[:, :, pl.ds(row, val.shape[0])]

    def copies(self, ph):
        return [rcopy(self.val, self.land.at[ph, k], self.ssem.at[ph, k], self.rsem.at[ph, k], p)
                for k, p in enumerate(self.pl.phases[ph])]

    def start(self, ph):
        for cp in self.copies(ph):
            cp.start()

    def finish(self, ph):
        for cp in self.copies(ph):
            cp.wait()
        land = self.land
        self.val[...] = (self.val[...] + land[ph, 0]) + (land[ph, 1] + land[ph, 2])


def small_scratch(n):
    return [pltpu.VMEM((n, BLK), F32), pltpu.SemaphoreType.DMA((2, 3)), pltpu.SemaphoreType.DMA((2, 3))]


GRAM_UNITS = 18
GRAM = 3
UNITS = 54
SLOTS = 5 * LAG + 1
START_3 = 28
START_2 = 44
END = START_2 + 21 + 11 * LAG
LOOPS = (0, 18, 39, 54, 66, END)
DZ_SLOTS = (23, 27, 30, 32, 34, 36, 37, 38)
PASS_2 = 39
PASS_1 = 45
SPAN_2, SPAN_1 = 3, 4


def block_of(q):
    i = jnp.int32(0)
    for first in (8, 15, 21, 26, 30, 33, 35):
        i = i + jnp.where(q >= first, 1, 0)
    return i, i + q - (17 * i - i * i) // 2


def step_kernel(ha, hb, w1, w2, w3, g1, b1, g2, b2, g3_o, g2_o, g1_o, n1_o, h_o, ho_o, st_o, loss_o,
                zd, zod, dz, dzo, gw, x2h, x2o, x1h, x1o, g2v, g1v, lacc, rs, stage, st_v,
                part, r1, r2, r3, r4, ssem, rsem, sv, sa, sb, fa1, fb1, fa2, fb2,
                s2, sa2, sb2, s1, sa1, sb1, odd_land, even_land, e2, e1,
                asem, bsem, lsem, psem, csem, dsem, esem, wsem):
    me = Place()
    me.announce()
    c = me.c
    nv, da = g2v.at[pl.ds(0, ROWS)], g2v.at[pl.ds(ROWS, ROWS)]
    hv = x2o.at[:, pl.ds(0, FEAT)]
    f1, f2 = [[st.at[pl.ds(h * NB, NB)] for h in range(2)] for st in (s1, s2)]
    gains, biases = (g1, g2), (b1, b2)
    half = pl.ds(pl.multiple_of(c * 1024, 1024), 1024)
    ohalf = pl.ds(pl.multiple_of((1 - c) * 1024, 1024), 1024)
    hhalf = pl.ds(pl.multiple_of(c * 256, 256), 256)
    hohalf = pl.ds(pl.multiple_of((1 - c) * 256, 256), 256)
    mine = pl.ds(pl.multiple_of(c * HALF, HALF), HALF)
    theirs = pl.ds(pl.multiple_of((1 - c) * HALF, HALF), HALF)
    body = pl.ds(0, ROWS)
    w1v = zod.at[pl.ds(0, FEAT)]
    load_w1 = pltpu.make_async_copy(w1, w1v, csem.at[0])
    load_w2a = pltpu.make_async_copy(w2, gw, csem.at[1])
    load_w3a = [pltpu.make_async_copy(w3.at[pl.ds(r, 1024)], gw.at[pl.ds(r, 1024)], csem.at[k])
                for r, k in ((0, 2), (1024, 4))]
    load_w2 = pltpu.make_async_copy(w2, gw, csem.at[6])
    load_n1 = pltpu.make_async_copy(n1_o, nv, csem.at[7])
    save_n1 = pltpu.make_async_copy(da, n1_o, csem.at[8])
    keep_x1 = pltpu.make_async_copy(dzo.at[:, half], x1h, csem.at[3])
    keep_h = pltpu.make_async_copy(hv.at[:, hhalf], h_o, csem.at[5])
    hh, ho = x2h.at[:, pl.ds(0, 256)], x2o.at[:, pl.ds(0, 256)]
    load_h2 = [pltpu.make_async_copy(h_o, hh, csem.at[5]), pltpu.make_async_copy(ho_o, ho, csem.at[2])]
    keep_x2 = pltpu.make_async_copy(dz.at[:, half], x2h, csem.at[10])
    swap_z = rcopy(zd.at[body], zod, dsem.at[0], esem.at[0], me.pc)
    swap_x2 = rcopy(dz.at[:, ohalf], x2o, dsem.at[1], esem.at[1], me.pc)
    swap_x1 = rcopy(dzo.at[:, ohalf], x1o, dsem.at[2], esem.at[2], me.pc)
    swap_h = rcopy(hv.at[:, hohalf], ho_o, dsem.at[3], esem.at[3], me.pc)
    swap_du1 = rcopy(dz, dzo, dsem.at[5], esem.at[5], me.pc)
    swap_s2 = rcopy(s2, e2, dsem.at[6], esem.at[6], me.pc)
    swap_s1 = rcopy(s1, e1, dsem.at[7], esem.at[7], me.pc)

    def load_h(src):
        return pltpu.make_async_copy(src, hv.at[mine], csem.at[9])

    def give_h(src):
        return rcopy(src, hv.at[mine], dsem.at[16], esem.at[16], me.pc)

    def load_w3(j):
        return pltpu.make_async_copy(w3.at[cols(j)], gw.at[cols(j)], wsem.at[j])

    def swap_du2(j):
        return rcopy(zd.at[body, cols(j)], zod.at[:, cols(j)], dsem.at[17 + j], esem.at[17 + j], me.pc)

    def swap_dz(j):
        return rcopy(dz.at[:, cols(j)], dzo.at[:, cols(j)], dsem.at[8 + j], esem.at[8 + j], me.pc)

    for k, own in ((0, ha), (1, hb)):
        @pl.when(c == k)
        def _(own=own):
            load_h(own).start()
    load_w1.start()
    me.await_all()
    for k, other in ((0, hb), (1, ha)):
        @pl.when(c == k)
        def _(other=other):
            give_h(other).start()
    load_w2a.start()
    lacc[...] = jnp.zeros_like(lacc)

    def matmul(src, w, dst, rows, depth, first, stop, st=None, add=False):
        def step(j, carry):
            res = nn(src[rows, depth], w[depth, cols(j)])
            if add == 'depth':
                res = res + dst[rows, cols(j)]
            dst[rows, cols(j)] = res
            if st is not None:
                one = jnp.sum(res, axis=0, keepdims=True)
                two = jnp.sum(res * res, axis=0, keepdims=True)
                k = lax.rem(j, 4)
                if add == 'rows':
                    one = one + st[pl.ds(k, 1)]
                    two = two + st[pl.ds(4 + k, 1)]
                st[pl.ds(k, 1)] = one
                st[pl.ds(4 + k, 1)] = two
            return carry
        lax.fori_loop(first, stop, step, 0)

    def norm(u, x, st, layer, h):
        mean = st[0:4] * (1.0 / ALL_ROWS)
        var = st[4:8] * (1.0 / ALL_ROWS) - mean * mean
        inv = lax.rsqrt(var + BN_EPS)
        st[0:4] = mean
        st[4:8] = inv
        rs[NB * layer + 4 * h:NB * layer + 4 * h + 4] = inv

        def step(j, carry):
            k = j - 4 * h
            nrm = (u[:, cols(j)] - st[pl.ds(k, 1)]) * st[pl.ds(4 + k, 1)]
            act = gains[layer][:, cols(j)] * nrm + biases[layer][:, cols(j)]
            u[:, cols(j)] = nrm
            x[:, cols(j)] = jnp.maximum(act, 0.0).astype(BF16)
            return carry
        lax.fori_loop(4 * h, 4 * h + 4, step, 0)

    low, high, full = pl.ds(0, 1024), pl.ds(1024, 1024), pl.ds(0, DIM)
    all_f = pl.ds(0, FEAT)
    red_f1 = [SmallReduce(me, f1[h], odd_land, fa1.at[h], fb1.at[h], h * NB) for h in range(2)]
    red_f2 = [SmallReduce(me, f2[h], even_land, fa2.at[h], fb2.at[h], h * NB) for h in range(2)]
    load_w1.wait()
    load_h(ha).wait()
    give_h(ha).wait()
    swap_h.start()
    keep_h.start()
    for h in range(2):
        matmul(hv, w1v, da, body, all_f, 4 * h, 4 * h + 4, f1[h])
        red_f1[h].start(0)
    for h in range(2):
        red_f1[h].finish(0)
        red_f1[h].start(1)
    red_f1[0].finish(1)
    norm(da, dzo, f1[0], 0, 0)
    load_w2a.wait()
    matmul(dzo, gw, nv, body, low, 0, NB)
    red_f1[1].finish(1)
    norm(da, dzo, f1[1], 0, 1)
    matmul(dzo, gw, nv, body, high, 0, 4, f2[0], 'depth')
    red_f2[0].start(0)
    save_n1.start()
    keep_h.wait()
    swap_h.wait()
    swap_x1.start()
    keep_x1.start()
    matmul(dzo, gw, nv, body, high, 4, 6, f2[1], 'depth')
    red_f2[0].finish(0)
    red_f2[0].start(1)
    matmul(dzo, gw, nv, body, high, 6, NB, f2[1], 'depth')
    red_f2[1].start(0)
    for cp in load_w3a:
        cp.start()
    red_f2[0].finish(1)
    norm(nv, dz, f2[0], 1, 0)
    red_f2[1].finish(0)
    red_f2[1].start(1)
    save_n1.wait()
    load_w3a[0].wait()
    matmul(dz, gw, da, body, low, 0, 4)
    red_f2[1].finish(1)
    norm(nv, dz, f2[1], 1, 1)
    swap_x1.wait()
    swap_x2.start()
    keep_x2.start()
    load_w3a[1].wait()

    def z_block(j, part_done):
        if part_done:
            res = (da[:, cols(j)] + nn(dz[:, high], gw[high, cols(j)])).astype(BF16)
        else:
            res = nn(dz[...], gw[:, cols(j)]).astype(BF16)
        zd[0:ROWS, cols(j)] = res
        sv[pl.ds(j, 1)] = jnp.sum(res.astype(F32), axis=0, keepdims=True)

    def z_blocks(first, part_done):
        def step(j, carry):
            z_block(first + j, part_done)
            return carry
        lax.fori_loop(0, 2, step, 0)

    z_blocks(0, True)
    red0 = SmallReduce(me, sv, odd_land, sa, sb)
    red2 = SmallReduce(me, s2, even_land, sa2, sb2)
    red1 = SmallReduce(me, s1, odd_land, sa1, sb1)
    sc = Scatter(me, part, (r1, r2, r3, r4), ssem, rsem)

    def compute(u, w):
        p = lax.rem(u, SLOTS)
        if w == GRAM:
            i, j = block_of(2 * u)
            i1, j1 = block_of(2 * u + 1)

            @pl.when(i == i1)
            def _():
                res = tn(zd[0:ROWS, cols(i)], zd[0:ROWS, pl.ds(pl.multiple_of(j * BLK, BLK), 2 * BLK)])
                part[p, 0] = res[:, 0:BLK]
                part[p, 1] = res[:, BLK:2 * BLK]

            @pl.when(i != i1)
            def _():
                part[p, 0] = tn(zd[0:ROWS, cols(i)], zd[0:ROWS, cols(j)])
                part[p, 1] = tn(zd[0:ROWS, cols(i1)], zd[0:ROWS, cols(j1)])
            return
        q = grad_unit(u)[1]
        if w == 2:
            rc = pl.ds(pl.multiple_of(q * 512, 512), 512)
            res = tn(hh[...], dz[:, rc]) + tn(ho[...], dzo[:, rc])
            part[p, 0] = res[:, 0:BLK]
            part[p, 1] = res[:, BLK:2 * BLK]
            return
        la, lb, ra, rb = ((x2h, x2o, dz, dzo), (x1h, x1o, zd, zod))[w]
        lc = pl.ds(pl.multiple_of(lax.rem(q, 2) * 512, 512), 512)
        rc = cols(q // 2)
        res = tn(la[:, lc], ra[0:ROWS, rc]) + tn(lb[:, lc], rb[:, rc])
        part[p, 0] = res[0:BLK]
        part[p, 1] = res[BLK:2 * BLK]

    def grad_unit(u):
        v = jnp.maximum(u - GRAM_UNITS, 0)
        return v // 16, lax.rem(v, 16)

    def region(u, w, k, off, n):
        q = grad_unit(u)[1]
        if w == 2:
            r0, c0 = c * 256, q * 512 + k * BLK
        else:
            r0, c0 = c * 1024 + lax.rem(q, 2) * 512 + k * BLK, (q // 2) * BLK
        return rows_at(r0 + off, n), cols_at(c0)

    grads = (g3_o, g2v, g1v)

    def keep_copy(u, k):
        own = region(u, 0, k, me.own[k], 32)
        return pltpu.make_async_copy(stage.at[lax.rem(u, 3), k], g3_o.at[own], lsem.at[k, lax.rem(u, RING)])

    def hop(e, k, inward):
        if e == 3 and inward:
            return me.keep[k], 128, me.p1
        return ((me.own[k], 32, me.last[k]), (me.near[k], 64, me.p1), (me.near[k], 64, me.p3),
                (me.far[k], 64, me.p1), (me.keep[k], 128, me.first[k]))[e]

    def spread(u, w, e, k, inward=False):
        r = lax.rem(u, RING)
        off, n, dev = hop(e, k, inward)
        if w == GRAM:
            i, j = block_of(2 * u + k)
            src = dst = gw.at[rows_at(i * BLK + off, n), cols(j)]
        else:
            dst = grads[w].at[region(u, w, k, off, n)]
            src = stage.at[lax.rem(u, 3), k] if e == 0 and w == 0 else dst
        g = 0 if w == GRAM else 1
        return rcopy(src, dst, asem.at[g, e, k, r], bsem.at[g, e, k, r], dev)

    def cross(u, w):
        r = lax.rem(u, RING)
        q = grad_unit(u)[1]
        buf = grads[w].at[unit_region(q, w, c)]
        return rcopy(buf, buf, asem.at[1, 5, 0, r], bsem.at[1, 5, 0, r], me.pc)

    def unit_region(q, w, core):
        if w == 2:
            return rows_at(core * 256, 256), pl.ds(pl.multiple_of(q * 512, 512), 512)
        return rows_at(core * 1024 + lax.rem(q, 2) * 512, 512), cols(q // 2)

    def put(u, w, own):
        reg = unit_region(grad_unit(u)[1], w, c if own else 1 - c)
        out = (None, g2_o, g1_o)[w]
        return pltpu.make_async_copy(grads[w].at[reg], out.at[reg], psem.at[0 if own else 1, lax.rem(u, RING)])

    def final(u, w):
        if w < 3:
            for k in range(2):
                piece = part[lax.rem(u, SLOTS), k, rows_at(me.own[k], 32)]
                if w == 0:
                    stage[lax.rem(u, 3), k] = piece
                    keep_copy(u, k).start()
                else:
                    rr, cc = region(u, w, k, me.own[k], 32)
                    grads[w][rr, cc] = piece
                spread(u, w, 0, k).start()
            return
        for k in range(2):
            i, j = block_of(2 * u + k)
            own = rows_at(me.own[k], 32)
            row0 = rows_at(i * BLK + me.own[k], 32)
            mu_r = g1v[rows_at(lax.rem(i, 2) * BLK + me.own[k], 32), lanes_at((i // 2) * 128)]
            mu_c = sv[pl.ds(j, 1)]
            mm = ALL_ROWS * jnp.concatenate([mu_r, mu_r], axis=1) * mu_c
            cov = (part[lax.rem(u, SLOTS), k, own] - mm) * (1.0 / (ALL_ROWS - 1))
            row = lax.broadcasted_iota(jnp.int32, (32, BLK), 0) + (i * BLK + me.own[k])
            col = lax.broadcasted_iota(jnp.int32, (32, BLK), 1) + j * BLK
            diag = row == col
            std = jnp.sqrt(jnp.where(diag, cov, 1.0) + STD_EPS)
            hinge = jnp.where(std < 1.0, VAR_WEIGHT / (2.0 * std), 0.0)
            weight = jnp.where(i == j, COV_WEIGHT, 2.0 * COV_WEIGHT)
            term = jnp.where(diag, VAR_WEIGHT * jnp.maximum(1.0 - std, 0.0), weight * cov * cov)
            lacc[...] = lacc[...] + ((term[0:8] + term[8:16]) + (term[16:24] + term[24:32]))
            gw[row0, cols(j)] = jnp.where(diag, -hinge, (2.0 * COV_WEIGHT) * cov).astype(BF16)
            spread(u, GRAM, 0, k).start()

    def diff_block(j):
        diff = zd[0:ROWS, cols(j)].astype(F32) - zod[:, cols(j)].astype(F32)
        sq = jnp.sum((diff * diff).reshape(ROWS // 8, 8, BLK), axis=0)
        lacc[...] = lacc[...] + (0.5 * INV_WEIGHT / ALL_ROWS) * sq
        da[:, cols(j)] = (2.0 * INV_WEIGHT / ALL_ROWS) * diff

    def dz_block(j):
        acc = nn(zd[...], gw[:, cols(j)])
        mean = acc[ROWS:ROWS + 1] + acc[ROWS + 1:ROWS + 2] + acc[ROWS + 2:ROWS + 3]
        dz[:, cols(j)] = (da[:, cols(j)] + (2.0 / (ALL_ROWS - 1)) * (acc[0:ROWS] - mean)).astype(BF16)

    def back_block(j, grad, st, layer):
        dx = nt(grad[0:ROWS, :], gw[cols(j)])
        nrm = nv[:, cols(j)]
        act = gains[layer][:, cols(j)] * nrm + biases[layer][:, cols(j)]
        d_act = jnp.where(act > 0.0, dx, 0.0)
        da[:, cols(j)] = d_act
        st[pl.ds(j, 1)] = jnp.sum(d_act, axis=0, keepdims=True)
        st[pl.ds(NB + j, 1)] = jnp.sum(d_act * nrm, axis=0, keepdims=True)

    def back_pre(dst, st, layer, after):
        def step(j, carry):
            scale = gains[layer][:, cols(j)] * rs[pl.ds(NB * layer + j, 1)]
            m0 = st[pl.ds(j, 1)] * (1.0 / ALL_ROWS)
            m1 = st[pl.ds(NB + j, 1)] * (1.0 / ALL_ROWS)
            dst[0:ROWS, cols(j)] = (scale * (da[:, cols(j)] - m0 - nv[:, cols(j)] * m1)).astype(BF16)
            after(j)
            return carry
        lax.fori_loop(0, NB, step, 0)

    def gather_step(e, u, w, inward):
        def each(f):
            for k in range(2):
                f(k)

        def wait_send(k):
            spread(u, w, e - 1, k, inward).wait_send()

        def wait_recv(k):
            spread(u, w, e - 1, k, inward).wait_recv()

        def begin(k):
            spread(u, w, e, k, inward).start()

        def run(sends, recvs, begins):
            if e == 1 and w == 0:
                each(lambda k: keep_copy(u, k).wait())
            if e in sends:
                each(wait_send)
            if e in recvs:
                each(wait_recv)
            if e in begins:
                each(begin)

        def at_end():
            if inward:
                run((), (4,), (4,))
            else:
                run((1, 2, 5), (1, 4, 5), (1, 4))

        def at_inner():
            if inward:
                run((1, 3, 4), (1, 3), (2, 3, 4))
            else:
                run((3, 4), (2, 3), (2, 3, 4))

        if e == 5:
            at_end()
        else:
            if e == 4 or not inward:
                pl.when(me.end)(at_end)
            if e > 1 or inward:
                pl.when(jnp.logical_not(me.end))(at_inner)
        if e == 5 and w < 3:
            cross(u, w).start()
            if w > 0:
                put(u, w, True).start()
        if e == 5 and w == GRAM:
            for k in range(2):
                i, j = block_of(2 * u + k)

                @pl.when(i != j)
                def _():
                    gw[rows_at(j * BLK, BLK), cols(i)] = gw[rows_at(i * BLK, BLK), cols(j)].T

    compute(jnp.int32(0), GRAM)

    def gather(e, u, w):
        if w == GRAM or e == 5:
            gather_step(e, u, w, False)
            return
        inward = is_inward(u)
        pl.when(jnp.logical_not(inward))(lambda: gather_step(e, u, w, False))
        pl.when(inward)(lambda: gather_step(e, u, w, True))

    def put_end(u, w):
        if w in (1, 2):
            put(u, w, False).wait()

    def cross_end(u, w):
        if w < 3:
            cross(u, w).wait()
        if w in (1, 2):
            put(u, w, True).wait()
            put(u, w, False).start()

    def means():
        mean = sv[...] * (1.0 / ALL_ROWS)
        sv[...] = mean
        hi = mean.astype(BF16)
        mid = (mean - hi.astype(F32)).astype(BF16)
        low = (mean - hi.astype(F32) - mid.astype(F32)).astype(BF16)
        for j in range(NB):
            for h in range(2):
                lanes = slice(128 * h, 128 * h + 128)
                r0, c0 = (j % 2) * BLK + 128 * h, (j // 2) * 128
                g1v[r0:r0 + 128, c0:c0 + 128] = jnp.broadcast_to(mean[j:j + 1, lanes], (128, 128)).T
            zd[ROWS:ROWS + 8, j * BLK:(j + 1) * BLK] = jnp.concatenate(
                [hi[j:j + 1], mid[j:j + 1], low[j:j + 1], jnp.zeros((5, BLK), BF16)], axis=0)

    def slots(lo, hi):
        def slot(t, carry):
            run_slot(Span(lo, hi, t), t)
            return carry
        lax.fori_loop(lo, hi, slot, 0)

    out_st = pltpu.make_async_copy(st_v, st_o, csem.at[9])

    def small_results():
        swap_s2.wait()
        swap_s1.wait()
        sum2, sum1 = s2[...] + e2[...], s1[...] + e1[...]
        for j in range(NB):
            lanes = slice(j * BLK, (j + 1) * BLK)
            st_v[0:1, lanes] = sum1[NB + j:NB + j + 1]
            st_v[1:2, lanes] = sum1[j:j + 1]
            st_v[2:3, lanes] = sum2[NB + j:NB + j + 1]
            st_v[3:4, lanes] = sum2[j:j + 1]
        loss_o[0, 0] = jnp.sum(sum2[2 * NB:])
        out_st.start()

    def run_slot(span, t):
        span.units(11 * LAG + 1, put_end)
        span.units(11 * LAG, cross_end)
        for e in (5, 4, 3, 2, 1):
            span.units((5 + e) * LAG, functools.partial(gather, e))
        reds = ((2, red0), (PASS_2 + SPAN_2 - 1, red2), (PASS_1 + SPAN_1 - 1, red1))
        for first, red in reds[:2]:
            @functools.partial(span.at, first + 1)
            def _(red=red):
                red.finish(0)
                red.start(1)

            @functools.partial(span.at, first + 2)
            def _(red=red):
                red.finish(1)

        @functools.partial(span.at, PASS_2 + SPAN_2)
        def _():
            load_w2.start()

        @functools.partial(span.at, PASS_2 + SPAN_2 + 1)
        def _():
            back_pre(zd, s2, 1, lambda j: swap_du2(j).start())
            load_n1.start()
            swap_s2.start()

        for j, first in enumerate(DZ_SLOTS):
            span.at(first + 1, lambda j=j: swap_dz(j).wait())
        mine_now = jnp.int32(-1)
        for j, first in enumerate(DZ_SLOTS):
            if span.lo <= first < span.hi:
                mine_now = jnp.where(t == first, j, mine_now)
        if any(span.lo <= first < span.hi for first in DZ_SLOTS):
            @pl.when(mine_now >= 0)
            def _():
                dz_block(mine_now)
                swap_dz(mine_now).start()

        @functools.partial(span.at, DZ_SLOTS[-1])
        def _():
            for j in range(NB):
                load_w3(j).start()

        span.at(START_2 + 24, small_results)
        for e in (5, 4, 3, 2, 1):
            span.units(e * LAG, lambda u, w, e=e: sc.step(e, u, w == GRAM, lambda v: final(v, w)))
        span.units(0, lambda u, w: sc.start(u, 0))
        first, red = reds[2]

        @functools.partial(span.at, first + 1)
        def _():
            red.finish(0)
            red.start(1)

        span.at(first + 2, lambda: red.finish(1))

        @functools.partial(span.at, PASS_1 + SPAN_1 + 1)
        def _():
            back_pre(dz, s1, 0, lambda j: None)
            swap_du1.start()
            swap_s1.start()

        span.at(4, means)
        span.at(0, lambda: z_blocks(2, True))
        span.within(1, 3, lambda: z_blocks(2 * t + 2, False))

        @functools.partial(span.at, 3)
        def _():
            keep_x1.wait()
            keep_x2.wait()
            swap_x2.wait()
            swap_z.start()

        span.at(7, swap_z.wait)
        span.within(8, 8 + NB, lambda: diff_block(t - 8))
        @functools.partial(span.at, PASS_2)
        def _():
            s2[2 * NB:3 * NB] = lacc[...]

        @functools.partial(span.at, PASS_1)
        def _():
            load_w2.wait()
            load_n1.wait()

        @functools.partial(span.within, START_2 - 1, START_2 + 15)
        def _():
            block = (t - (START_2 - 1)) // 2

            @pl.when(t == START_2 - 1 + 2 * block)
            def _():
                swap_du2(block).wait()

        @functools.partial(span.at, START_2 + 8)
        def _():
            for cp in load_h2:
                cp.start()

        @functools.partial(span.at, START_2 + 14)
        def _():
            swap_du1.wait()
            for cp in load_h2:
                cp.wait()

        for first, width, grad, st, layer in ((PASS_2, SPAN_2, dz, s2, 1), (PASS_1, SPAN_1, zd, s1, 0)):
            @functools.partial(span.within, first, first + width)
            def _(first=first, n=-(-NB // width), grad=grad, st=st, layer=layer):
                def step(j, carry):
                    if layer == 1:
                        load_w3(j).wait()
                    back_block(j, grad, st, layer)
                    return carry
                lo = n * (t - first)
                lax.fori_loop(lo, jnp.minimum(lo + n, NB), step, 0)

        for last, red in reds:
            span.at(last, lambda red=red: red.start(0))
        span.units(-1, compute)

    for lo, hi in zip(LOOPS, LOOPS[1:]):
        slots(lo, hi)
    out_st.wait()


def train_step(ha, hb, w1, w2, w3, g1, b1, g2, b2):
    act = pltpu.VMEM((ROWS, DIM), BF16)
    piece = pltpu.VMEM((ROWS, 1024), BF16)
    dma = pltpu.SemaphoreType.DMA
    return pl.pallas_call(
        step_kernel,
        out_shape=(sds((DIM, DIM), F32), sds((DIM, DIM), F32), sds((FEAT, DIM), F32), sds((ROWS, DIM), F32),
                   sds((ROWS, 256), BF16), sds((ROWS, 256), BF16), sds((4, DIM), F32), sds((1, 1), F32)),
        in_specs=[ANY] * 5 + [INV] * 4,
        out_specs=(ANY,) * 7 + (pl.BlockSpec(memory_space=pltpu.SMEM),),
        scratch_shapes=[pltpu.VMEM((ROWS + 8, DIM), BF16), act, act, act, pltpu.VMEM((DIM, DIM), BF16),
                        piece, piece, piece, piece,
                        pltpu.VMEM((DIM, DIM), F32), pltpu.VMEM((FEAT, DIM), F32),
                        pltpu.VMEM((NB, BLK), F32), pltpu.VMEM((2 * NB, BLK), F32),
                        pltpu.VMEM((3, 2, 32, BLK), F32), pltpu.VMEM((4, DIM), F32)]
        + scatter_scratch(SLOTS) + small_scratch(NB) + [dma((2, 2, 3))] * 4
        + small_scratch(3 * NB) + small_scratch(2 * NB)
        + [pltpu.VMEM((2, 3, 2 * NB, BLK), F32), pltpu.VMEM((2, 3, 3 * NB, BLK), F32),
           pltpu.VMEM((3 * NB, BLK), F32), pltpu.VMEM((2 * NB, BLK), F32),
           dma((2, 6, 2, RING)), dma((2, 6, 2, RING)), dma((2, RING)),
           dma((2, RING)), dma((11,)), dma((25,)), dma((25,)), dma((NB,))],
        compiler_params=pltpu.CompilerParams(collective_id=0, has_side_effects=True, vmem_limit_bytes=VMEM_LIMIT),
        name='train_step',
    )(ha, hb, w1, w2, w3, g1, b1, g2, b2)


CHUNK = 128
BUFS = 8


def finish_kernel(g3, g2, g1, st, loss, o3, o2, o1, gain1, bias1, gain2, bias2, loss_o, buf, isem, osem, rsem):
    jobs = [(src, dst, r) for src, dst, n in ((g3, o3, DIM), (g2, o2, DIM), (g1, o1, FEAT)) for r in range(0, n, CHUNK)]

    def take(i):
        src, _, r = jobs[i]
        return pltpu.make_async_copy(src.at[pl.ds(r, CHUNK)], buf.at[i % BUFS], isem.at[i % BUFS])

    def give(i):
        _, dst, r = jobs[i]
        return pltpu.make_async_copy(buf.at[i % BUFS], dst.at[pl.ds(r, CHUNK)], osem.at[i % BUFS])

    for i in range(BUFS - 1):
        take(i).start()
    rows = [pltpu.make_async_copy(st.at[pl.ds(row, 1)], out, rsem.at[row])
            for row, out in enumerate((gain1, bias1, gain2, bias2))]
    for cp in rows:
        cp.start()
    loss_o[0, 0] = loss[0, 0]
    for i in range(len(jobs)):
        take(i).wait()
        give(i).start()
        if i + BUFS - 1 < len(jobs):
            if i > 0:
                give(i - 1).wait()
            take(i + BUFS - 1).start()
    for i in range(len(jobs) - BUFS, len(jobs)):
        give(i).wait()
    for cp in rows:
        cp.wait()


def finish(g3, g2, g1, st, loss):
    smem = pl.BlockSpec(memory_space=pltpu.SMEM)
    dma = pltpu.SemaphoreType.DMA
    return pl.pallas_call(
        finish_kernel,
        out_shape=(sds((DIM, DIM), F32), sds((DIM, DIM), F32), sds((FEAT, DIM), F32)) + (sds((1, DIM), F32),) * 4
        + (sds((1, 1), F32),),
        in_specs=[ANY] * 4 + [smem],
        out_specs=(ANY,) * 7 + (smem,),
        scratch_shapes=[pltpu.VMEM((BUFS, CHUNK, DIM), F32), dma((BUFS,)), dma((BUFS,)), dma((4,))],
        name='finish',
    )(g3, g2, g1, st, loss)


def solution(mesh):
    def local_step(h_a, h_b, w_one, w_two, w_three, gain_one, bias_one, gain_two, bias_two):
        vecs = [v.reshape(1, DIM) for v in (gain_one, bias_one, gain_two, bias_two)]
        g_three, g_two, g_one, _, _, _, st, part_loss = train_step(h_a, h_b, w_one, w_two, w_three, *vecs)
        d_three, d_two, d_one, *small, loss = finish(g_three, g_two, g_one, st, part_loss)
        return (loss.reshape(()), d_one, d_two, d_three, *[v.reshape(DIM) for v in small])

    row_spec = P('data', None)
    return jax.shard_map(local_step, mesh=mesh,
                         in_specs=(row_spec, row_spec, P(), P(), P(), P(), P(), P(), P()),
                         out_specs=(P(), P(), P(), P(), P(), P(), P(), P()),
                         check_vma=False)
```
